128 devices in a mesh: gx: 16 (over y, x), gy: 8 (over z, core).
Axes of the slice: x: 4, y: 4, z: 4, core: 2. Of those that a mesh axis runs over, the one named last changes fastest.
Arguments:
- probes: bfloat16 [512, 2048, 256], P('gx', 'gy'), may hold values from -6 to 6
- blk_rows: int32 [16384, 128], P(('gx', 'gy')), may hold values from 0 to 8191
- blk_sensor: int32 [16384], P(('gx', 'gy')), may hold values from 0 to 1023, as said below
- blk_count: int32 [128], P(('gx', 'gy')), may hold values from 64 to 128, as said below
- coef: bfloat16 [16384, 128], P(('gx', 'gy')), may hold values from -5 to 5
- owner: int32 [1024], replicated, may hold values from 0 to 127, as said below
- weights: float32 [1024], replicated, may hold values from 0.1 to 1
Outputs:
- sensitivity: float32 [1024], P(('gx', 'gy'))
- new_weights: float32 [1024], replicated
- density: float32 [512, 2048], P('gx', 'gy')
The draws below stay inside these ranges and needn't reach their ends.
Inputs may be any that keep to these rules, and one draw needn't show every extreme that they name: `owner`: every device owns exactly 8 sensors. `blk_sensor`: among the live slots of one tile, at most 2 belong to sensors of one owner; in every draw some owner receives 2 live blocks from every tile. `blk_count`: some tile has all 128 slots live.
All inputs are finite; a program needn't handle non-finite values.
Results may differ from the reference program's by a relative error of at most 0.0008.
Values may be sent and summed in bfloat16 or wider, within the bound.
No kernel may reach another device: no remote copies, remote signals or barrier semaphores. Data moves between devices by JAX's collectives and lax.ppermute only.
A program may use at most 128 MiB of HBM per device.

```python
import math
import jax
import jax.numpy as jnp
from jax import lax

P_SIZE = 256
FOOT = 128
TR = 32
TC = 256
SPD = 8
CAP = 2
SENSORS = 1024
NBLK = 128
GR = 512
GC = 2048
N_GX = 16
N_GY = 8
DEVICES = 128


def layout(key):
    perm = jax.random.permutation(jax.random.fold_in(key, 11), SENSORS).astype(jnp.int32)
    owners = perm // SPD
    inverse = jnp.argsort(perm, stable=True).astype(jnp.int32)
    hot = jax.random.permutation(jax.random.fold_in(key, 12), DEVICES)[:2].astype(jnp.int32)
    entries = jnp.arange(DEVICES * CAP, dtype=jnp.int32)
    is_hot = jnp.any((entries // CAP)[:, None] == hot[None, :], axis=1).astype(jnp.int32)
    score = jax.random.randint(jax.random.fold_in(key, 13), (DEVICES, DEVICES * CAP), 0, 2 ** 20, dtype=jnp.int32)
    score = (score + is_hot[None, :] * 2 ** 21) * (DEVICES * CAP) + entries[None, :]
    chosen = lax.top_k(score, NBLK)[1].astype(jnp.int32)
    dest = chosen // CAP
    within = jax.random.randint(jax.random.fold_in(key, 14), (DEVICES, NBLK), 0, SPD, dtype=jnp.int32)
    sensor = inverse[dest * SPD + within]
    count = jax.random.randint(jax.random.fold_in(key, 15), (DEVICES,), NBLK // 2, NBLK + 1, dtype=jnp.int32)
    full_tile = jax.random.randint(jax.random.fold_in(key, 16), (), 0, DEVICES, dtype=jnp.int32)
    count = jnp.where(jnp.arange(DEVICES, dtype=jnp.int32) == full_tile, NBLK, count)
    return (owners, sensor.reshape(-1), count)


def draw_owner(key, part):
    return layout(key)[0]


def draw_blk_sensor(key, part):
    return layout(key)[1]


def draw_blk_count(key, part):
    return layout(key)[2]


def touch_ends(values, own_key, least, top_value):
    longest = values.shape.index(max(values.shape))
    spots = []
    for shift in (0, 1):
        where = [jax.random.randint(jax.random.fold_in(own_key, axis), (), 0, length) for axis, length in enumerate(values.shape)]
        where[longest] = (where[longest] + shift) % values.shape[longest]
        spots.append(tuple(where))
    return values.at[spots[0]].set(least).at[spots[1]].set(top_value)


def block_levels(key, dims, shards, smallest, high):
    loudness = 1.0
    for position, blocks in shards:
        steps = jax.random.uniform(jax.random.fold_in(jax.random.fold_in(key, 6), position), (blocks,), jnp.float32, smallest / len(shards), high / len(shards))
        loudness = loudness * jnp.repeat(jnp.exp(steps), dims[position] // blocks).reshape((-1,) + (1,) * (len(dims) - 1 - position))
    return loudness


def normal_values(key, extent, deviation, limit, cuts=(), kind=jnp.bfloat16):
    values = deviation * jax.random.normal(key, extent, jnp.float32)
    if cuts:
        values = values * block_levels(key, extent, cuts, -0.22, 0.18)
    return jnp.clip(values, -limit, limit).astype(kind)


def setup_inputs(seed: int = 0) -> dict:
    keys = jax.random.split(jax.random.key(seed), 8)
    return {
        "probes": normal_values(keys[0], (GR, GC, P_SIZE), 1.0, 6.0, ((0, 16), (1, 8))),
        "blk_rows": touch_ends(jax.random.randint(keys[1], (DEVICES * NBLK, FOOT), 0, TR * TC), jax.random.fold_in(keys[1], 1), 0, (TR * TC) - 1).astype(jnp.int32),
        "blk_sensor": draw_blk_sensor(jax.random.fold_in(keys[7], 71), 0),
        "blk_count": draw_blk_count(jax.random.fold_in(keys[7], 71), 0),
        "coef": normal_values(keys[4], (DEVICES * NBLK, FOOT), 1.0, 5.0, ((0, 128),)),
        "owner": draw_owner(jax.random.fold_in(keys[7], 71), 0),
        "weights": jnp.clip(jnp.exp(jax.random.uniform(keys[6], (SENSORS,), jnp.float32, math.log(0.1), math.log(1.0))), 0.1, 1.0),
    }


def reference(probes, blk_rows, blk_sensor, blk_count, coef, owner, weights):
    tiles = probes.reshape(N_GX, TR, N_GY, TC, P_SIZE).transpose(0, 2, 1, 3, 4).reshape(N_GX * N_GY, TR * TC, P_SIZE)
    rows = blk_rows.reshape(DEVICES, NBLK, FOOT)
    sensors = blk_sensor.reshape(DEVICES, NBLK)
    coefs = coef.reshape(DEVICES, NBLK, FOOT)
    live = (jnp.arange(NBLK, dtype=jnp.int32)[None, :] < blk_count[:, None]).astype(jnp.float32)

    def accumulate(obs, inputs):
        tile, row_ids, sens, weight, alive = inputs
        picked = tile[row_ids.reshape(-1)].reshape(NBLK, FOOT, P_SIZE).astype(jnp.float32)
        contrib = weight.astype(jnp.float32)[:, :, None] * picked * alive[:, None, None]
        return (obs.at[sens].add(contrib), None)
    obs = lax.scan(accumulate, jnp.zeros((SENSORS, FOOT, P_SIZE), jnp.float32), (tiles, rows, sensors, coefs, live))[0]
    sens_h = lax.optimization_barrier(jnp.sum(obs * obs, axis=(1, 2))) / (FOOT * P_SIZE)
    order = jnp.argsort(owner * SENSORS + jnp.arange(SENSORS, dtype=jnp.int32))
    sensitivity = sens_h[order]
    gain = weights * jnp.sqrt(1.0 + sens_h)
    new_weights = SENSORS * gain / jnp.sum(gain)
    values = live[:, :, None] * new_weights[sensors][:, :, None] * jnp.square(coefs.astype(jnp.float32))
    tile_ids = jnp.broadcast_to(jnp.arange(DEVICES, dtype=jnp.int32)[:, None, None], rows.shape)
    dens = jnp.zeros((DEVICES, TR * TC), jnp.float32).at[tile_ids, rows].add(values)
    density = dens.reshape(N_GX, N_GY, TR, TC).transpose(0, 2, 1, 3).reshape(N_GX * TR, N_GY * TC)
    return (sensitivity, new_weights, density)
```

```python
import jax
import jax.numpy as jnp
from jax import lax
from jax.experimental import pallas as pl
from jax.experimental.pallas import tpu as pltpu
from jax.sharding import PartitionSpec as P

SPD = 8
AXES = ("gx", "gy")
CHUNKS = (32, 32, 32, 32)
F32 = jnp.float32
BF16 = jnp.bfloat16
I32 = jnp.int32


def gather_rows(flat, index, slot0, ns, rb=8):
    n, pn = flat.shape
    foot = nblk = 128
    half = pn // 2

    def body(idx, x_ref, out_ref, tab, stage):
        g = pl.program_id(0)

        @pl.when(g == 0)
        def _():
            ch = 512

            def conv(i, c):
                x = x_ref[pl.ds(i * ch, ch), :].astype(F32)
                tab[pl.ds(i * 2 * ch, ch, stride=2), :] = x[:, :half]
                tab[pl.ds(i * 2 * ch + 1, ch, stride=2), :] = x[:, half:]
                return c

            lax.fori_loop(0, n // ch, conv, 0)

        def channel(q, c):
            base = (g * rb + q) * nblk + slot0
            for j in range(ns):
                at = pl.multiple_of(idx[base + j], 2)
                stage[q, pl.ds(2 * j, 2), :] = tab[pl.ds(at, 2), :]
            return c

        lax.fori_loop(0, rb, channel, 0)
        for q in range(rb):
            out_ref[q, :, :half] = stage[q, pl.ds(0, ns, stride=2), :].astype(BF16)
            out_ref[q, :, half:] = stage[q, pl.ds(1, ns, stride=2), :].astype(BF16)

    return pl.pallas_call(
        body,
        grid_spec=pltpu.PrefetchScalarGridSpec(
            num_scalar_prefetch=1,
            grid=(foot // rb,),
            in_specs=[pl.BlockSpec((n, pn), lambda g, idx: (0, 0))],
            out_specs=pl.BlockSpec((rb, ns, pn), lambda g, idx: (g, 0, 0)),
            scratch_shapes=[
                pltpu.VMEM((2 * n, half), F32),
                pltpu.VMEM((rb, 2 * ns, half), F32),
            ],
        ),
        out_shape=jax.ShapeDtypeStruct((foot, ns, pn), BF16),
        compiler_params=pltpu.CompilerParams(
            dimension_semantics=("arbitrary",), vmem_limit_bytes=24 * 1024 * 1024
        ),
        name="gather_rows",
    )(index, flat)


def mix_chunk(data, ids, coef, acc, n_sens, last, n_dev, kb=512, mb=256):
    k, pn = data.shape

    def body(*refs):
        data_ref, ids_ref, coef_ref = refs[:3]
        acc_ref = None if acc is None else refs[3]
        out_ref, sum_ref = refs[-2:]
        g = pl.program_id(0)

        @pl.when(g == 0)
        def _():
            if acc_ref is None:
                sum_ref[...] = jnp.zeros((n_sens, pn), F32)
            else:
                sum_ref[...] = acc_ref[...]

        rows = data_ref[...]
        wanted = ids_ref[...]
        weight = coef_ref[...]
        sub = lax.broadcasted_iota(I32, (mb, kb), 0)
        for m in range(n_sens // mb):
            hit = sub == (wanted - m * mb)
            mixer = jnp.where(hit, weight, 0.0).astype(BF16)
            sum_ref[pl.ds(m * mb, mb), :] += jnp.dot(mixer, rows, preferred_element_type=F32)

        @pl.when(g == pl.num_programs(0) - 1)
        def _():
            if not last:
                out_ref[...] = sum_ref[...]
            else:
                for m in range(n_sens // 128):
                    x = sum_ref[pl.ds(m * 128, 128), :]
                    x = x * x
                    x = x[:, : pn // 2] + x[:, pn // 2 :]
                    row = jnp.sum(x.T, axis=0, keepdims=True)
                    out_ref[:, :, pl.ds(m * 128, 128)] = jnp.broadcast_to(row[None], (n_dev, 1, 128))

    specs = [
        pl.BlockSpec((kb, pn), lambda g: (g, 0)),
        pl.BlockSpec((1, kb), lambda g: (0, g)),
        pl.BlockSpec((1, kb), lambda g: (0, g)),
    ]
    args = [data, ids, coef]
    if acc is not None:
        specs.append(pl.BlockSpec((n_sens, pn), lambda g: (0, 0)))
        args.append(acc)
    shape = (n_dev, 1, n_sens) if last else (n_sens, pn)
    return pl.pallas_call(
        body,
        grid=(k // kb,),
        in_specs=specs,
        out_specs=pl.BlockSpec(shape, lambda g: (0,) * len(shape)),
        scratch_shapes=[pltpu.VMEM((n_sens, pn), F32)],
        out_shape=jax.ShapeDtypeStruct(shape, F32),
        compiler_params=pltpu.CompilerParams(
            dimension_semantics=("arbitrary",), vmem_limit_bytes=24 * 1024 * 1024
        ),
        name="mix_last" if last else "mix_chunk",
    )(*args)


def spread_squares(rows, coef, owner, me, tile_r, tile_c, sb=8):
    nblk, foot = rows.shape
    n_sens = owner.shape[1]

    def body(me_ref, rows_ref, coef_ref, owner_ref, map_ref, pos_ref):
        g = pl.program_id(0)

        @pl.when(g == 0)
        def _():
            mine = owner_ref[...] == me_ref[0]
            flag = jnp.broadcast_to(jnp.where(mine, 1.0, 0.0), (8, n_sens)).astype(BF16)
            row = lax.broadcasted_iota(I32, (n_sens, n_sens), 0)
            col = lax.broadcasted_iota(I32, (n_sens, n_sens), 1)
            before = jnp.where(row < col, 1.0, 0.0).astype(BF16)
            rank = jnp.dot(flag, before, preferred_element_type=F32)[0:1, :]
            pos_ref[...] = jnp.where(mine, rank.astype(I32), -1)

        sub_r = lax.broadcasted_iota(I32, (tile_r, foot), 0)
        sub_c = lax.broadcasted_iota(I32, (tile_c, foot), 0)
        point = rows_ref[...]
        high = point // tile_c
        low = point - high * tile_c
        c = coef_ref[...].astype(F32)
        sq = c * c
        sq_top = sq.astype(BF16).astype(F32)
        sq_rest = sq - sq_top
        for s in range(sb):
            at_r = sub_r == high[s : s + 1, :]
            left = jnp.concatenate(
                [jnp.where(at_r, sq_top[s : s + 1, :], 0.0), jnp.where(at_r, sq_rest[s : s + 1, :], 0.0)], axis=0
            ).astype(BF16)
            right = jnp.where(sub_c == low[s : s + 1, :], 1.0, 0.0).astype(BF16)
            both = lax.dot_general(left, right, (((1,), (1,)), ((), ())), preferred_element_type=F32)
            map_ref[s] = both[:tile_r] + both[tile_r:]

    return pl.pallas_call(
        body,
        grid=(nblk // sb,),
        in_specs=[
            pl.BlockSpec(memory_space=pltpu.SMEM),
            pl.BlockSpec((sb, foot), lambda g: (g, 0)),
            pl.BlockSpec((sb, foot), lambda g: (g, 0)),
            pl.BlockSpec((1, n_sens), lambda g: (0, 0)),
        ],
        out_specs=[
            pl.BlockSpec((sb, tile_r, tile_c), lambda g: (g, 0, 0)),
            pl.BlockSpec((1, n_sens), lambda g: (0, 0)),
        ],
        out_shape=[
            jax.ShapeDtypeStruct((nblk, tile_r, tile_c), F32),
            jax.ShapeDtypeStruct((1, n_sens), I32),
        ],
        compiler_params=pltpu.CompilerParams(
            dimension_semantics=("arbitrary",), vmem_limit_bytes=24 * 1024 * 1024
        ),
        name="spread_squares",
    )(me, rows, coef, owner)


def finish(parts, weights, sensor, count, maps, pos, scale, sb=32):
    n_dev = parts.shape[0]
    n_sens = weights.shape[1]
    nblk, tile_r, tile_c = maps.shape

    def body(count_ref, parts_ref, weights_ref, sensor_ref, pos_ref, maps_ref, sens_ref, new_ref, dens_ref, slot_w):
        g = pl.program_id(0)

        @pl.when(g == 0)
        def _():
            h = jnp.sum(parts_ref[...], axis=0) * scale
            gain = weights_ref[...] * jnp.sqrt(1.0 + h)
            new = n_sens * gain / jnp.sum(gain)
            new_ref[...] = new
            k = lax.broadcasted_iota(I32, (SPD, n_sens), 0)
            own = jnp.sum(jnp.where(pos_ref[...] == k, h, 0.0), axis=1, keepdims=True)
            diag = lax.broadcasted_iota(I32, (SPD, 128), 0) == lax.broadcasted_iota(I32, (SPD, 128), 1)
            sens_ref[...] = jnp.sum(jnp.where(diag, own, 0.0), axis=0, keepdims=True)
            which = lax.broadcasted_iota(I32, (nblk, n_sens), 1)
            w = jnp.sum(jnp.where(which == sensor_ref[...], new, 0.0), axis=1, keepdims=True)
            alive = lax.broadcasted_iota(I32, (nblk, 1), 0) < count_ref[0]
            slot_w[...] = jnp.broadcast_to(jnp.where(alive, w, 0.0), (nblk, tile_c))
            dens_ref[...] = jnp.zeros((tile_r, tile_c), F32)

        total = dens_ref[...]
        for s in range(sb):
            total += slot_w[pl.ds(g * sb + s, 1), :] * maps_ref[s]
        dens_ref[...] = total

    whole = lambda *shape: pl.BlockSpec(shape, lambda g: (0,) * len(shape))
    return pl.pallas_call(
        body,
        grid=(nblk // sb,),
        in_specs=[
            pl.BlockSpec(memory_space=pltpu.SMEM),
            whole(n_dev, 1, n_sens),
            whole(1, n_sens),
            whole(nblk, 1),
            whole(1, n_sens),
            pl.BlockSpec((sb, tile_r, tile_c), lambda g: (g, 0, 0)),
        ],
        out_specs=[whole(1, 128), whole(1, n_sens), whole(tile_r, tile_c)],
        out_shape=[
            jax.ShapeDtypeStruct((1, 128), F32),
            jax.ShapeDtypeStruct((1, n_sens), F32),
            jax.ShapeDtypeStruct((tile_r, tile_c), F32),
        ],
        scratch_shapes=[pltpu.VMEM((nblk, tile_c), F32)],
        compiler_params=pltpu.CompilerParams(
            dimension_semantics=("arbitrary",), vmem_limit_bytes=24 * 1024 * 1024
        ),
        name="finish",
    )(count, parts, weights, sensor, pos, maps)


def exchange(x):
    return lax.all_to_all(x, AXES, split_axis=0, concat_axis=0, tiled=True)


def local(probes, blk_rows, blk_sensor, blk_count, coef, owner, weights):
    n_dev = lax.axis_size("gx") * lax.axis_size("gy")
    me = (lax.axis_index("gx") * lax.axis_size("gy") + lax.axis_index("gy")).astype(I32).reshape(1)
    tile_r, tile_c, probe_n = probes.shape
    nblk, foot = blk_rows.shape
    n_sens = owner.shape[0]
    flat = probes.reshape(tile_r * tile_c, probe_n)
    index = (blk_rows.T * 2).reshape(-1)
    alive = jnp.arange(nblk, dtype=I32) < blk_count[0]
    side = jnp.stack(
        [
            jnp.where(alive[:, None], coef.astype(F32), 0.0).T,
            jnp.broadcast_to(blk_sensor.astype(F32)[None, :], (foot, nblk)),
        ],
        axis=1,
    )
    side = exchange(side)
    acc = None
    slot0 = 0
    for c, ns in enumerate(CHUNKS):
        sent = gather_rows(flat, index, slot0, ns)
        got = exchange(sent).reshape(n_dev * ns, probe_n)
        w = side[:, 0, slot0 : slot0 + ns].reshape(1, n_dev * ns)
        ids = side[:, 1, slot0 : slot0 + ns].astype(I32).reshape(1, n_dev * ns)
        acc = mix_chunk(got, ids, w, acc, n_sens, c == len(CHUNKS) - 1, n_dev)
        slot0 += ns
    maps, pos = spread_squares(blk_rows, coef, owner.reshape(1, n_sens), me, tile_r, tile_c)
    parts = exchange(acc)
    sens, new, density = finish(
        parts, weights.reshape(1, n_sens), blk_sensor.reshape(nblk, 1), blk_count, maps, pos, 1.0 / (foot * probe_n)
    )
    return (sens[0, :SPD], new.reshape(n_sens), density)


def solution(mesh):
    in_specs = (
        P("gx", "gy", None),
        P(("gx", "gy"), None),
        P(("gx", "gy")),
        P(("gx", "gy")),
        P(("gx", "gy"), None),
        P(),
        P(),
    )
    out_specs = (P(("gx", "gy")), P(), P("gx", "gy"))
    return jax.shard_map(local, mesh=mesh, in_specs=in_specs, out_specs=out_specs, check_vma=False)
```

```python
import jax
import jax.numpy as jnp
from jax import lax
from jax.experimental import pallas as pl
from jax.experimental.pallas import tpu as pltpu
from jax.sharding import PartitionSpec as P

SPD = 8
AXES = ("gx", "gy")
CHUNKS = (32, 96)
SIDE = 8
VMEM = 60 * 1024 * 1024
MB = 256
TILES = {16: 64, 32: 32, 48: 16, 64: 16, 80: 16, 96: 16, 112: 8}
F32 = jnp.float32
BF16 = jnp.bfloat16
I32 = jnp.int32


def gather_rows(probes, index, slot0, ns, side=None, rb=16):
    n, pn = probes.shape
    foot = nblk = 128
    half = pn // 2
    extra = 0 if side is None else SIDE
    parts = 8
    step = n // parts

    def body(*refs):
        idx, x_hbm = refs[:2]
        side_refs = refs[2:-6]
        out_ref, raw, tab, stage, coef_t, sem = refs[-6:]
        g = pl.program_id(0)

        @pl.when(g == 0)
        def _():
            def fetch(i):
                return pltpu.make_async_copy(x_hbm.at[pl.ds(i * step, step), :], raw.at[pl.ds(i * step, step), :], sem.at[i])

            for i in range(parts):
                fetch(i).start()
            if side is not None:
                coef_ref, _, count_ref = side_refs
                alive = lax.broadcasted_iota(I32, (nblk, foot), 0) < count_ref[0]
                coef_t[...] = jnp.where(alive, coef_ref[...].astype(F32), 0.0).T
            ch = 512
            for i in range(parts):
                fetch(i).wait()

                def conv(q, c):
                    at = i * step + q * ch
                    x = raw[pl.ds(at, ch), :].astype(F32)
                    tab[pl.ds(at * 2, ch, stride=2), :] = x[:, :half]
                    tab[pl.ds(at * 2 + 1, ch, stride=2), :] = x[:, half:]
                    return c

                lax.fori_loop(0, step // ch, conv, 0)

        def channels(q2, c):
            for u in range(2):
                q = q2 * 2 + u
                base = slot0 * foot + g * rb + q
                for j in range(ns):
                    at = pl.multiple_of(idx[base + j * foot], 2)
                    stage[u, pl.ds(2 * j, 2), :] = tab[pl.ds(at, 2), :]
                out_ref[q, pl.ds(0, ns), :] = stage[u, pl.ds(0, ns, stride=2), :].astype(BF16)
                out_ref[q, pl.ds(ns, ns), :] = stage[u, pl.ds(1, ns, stride=2), :].astype(BF16)
                if side is not None:
                    sensor = side_refs[1][...]
                    high = sensor // MB
                    low = sensor - high * MB
                    row = lax.broadcasted_iota(I32, (SIDE, nblk), 0)
                    tail = jnp.where(row == 1, high, jnp.where(row == 2, low, 0)).astype(F32)
                    tail = jnp.where(row == 0, coef_t[pl.ds(g * rb + q, 1), :], tail)
                    out_ref[q, pl.ds(2 * ns, SIDE), :] = tail.astype(BF16)
            return c

        lax.fori_loop(0, rb // 2, channels, 0)

    specs = [pl.BlockSpec(memory_space=pltpu.HBM)]
    args = [probes]
    if side is not None:
        specs += [
            pl.BlockSpec((nblk, foot), lambda g, idx: (0, 0)),
            pl.BlockSpec((1, nblk), lambda g, idx: (0, 0)),
            pl.BlockSpec(memory_space=pltpu.SMEM),
        ]
        args += list(side)
    return pl.pallas_call(
        body,
        grid_spec=pltpu.PrefetchScalarGridSpec(
            num_scalar_prefetch=1,
            grid=(foot // rb,),
            in_specs=specs,
            out_specs=pl.BlockSpec((rb, 2 * ns + extra, half), lambda g, idx: (g, 0, 0)),
            scratch_shapes=[
                pltpu.VMEM((n, pn), BF16),
                pltpu.VMEM((2 * n, half), F32),
                pltpu.VMEM((2, 2 * ns, half), F32),
                pltpu.VMEM((foot, nblk), F32),
                pltpu.SemaphoreType.DMA((parts,)),
            ],
        ),
        out_shape=jax.ShapeDtypeStruct((foot, 2 * ns + extra, half), BF16),
        compiler_params=pltpu.CompilerParams(
            dimension_semantics=("arbitrary",), vmem_limit_bytes=VMEM
        ),
        name="gather_rows",
    )(index, *args)


def mix_chunk(data, high, low, coef, acc, ns, n_sens, last, kb_tiles):
    n_dev, rows, half = data.shape
    kb = kb_tiles * ns
    n_m = n_sens // MB

    def body(*refs):
        data_ref, high_ref, low_ref, coef_ref = refs[:4]
        acc_ref = None if acc is None else refs[4]
        out_ref, sum_ref = refs[-2:]
        g = pl.program_id(0)

        @pl.when(g == 0)
        def _():
            if acc_ref is None:
                sum_ref[...] = jnp.zeros((n_sens, 2 * half), F32)
            else:
                sum_ref[...] = acc_ref[...]

        x = data_ref[...]
        x = jnp.concatenate([x[:, :ns].reshape(kb, half), x[:, ns : 2 * ns].reshape(kb, half)], axis=1)
        weight = coef_ref[...]
        sub = lax.broadcasted_iota(I32, (MB, kb), 0).astype(F32).astype(BF16)
        for m in range(n_m):
            wanted = jnp.where(high_ref[...] == m, low_ref[...], -1.0).astype(BF16)
            mixer = jnp.where(sub == wanted, weight, jnp.zeros((), BF16))
            sum_ref[pl.ds(m * MB, MB), :] += jnp.dot(mixer, x, preferred_element_type=F32)

        @pl.when(g == pl.num_programs(0) - 1)
        def _():
            if not last:
                out_ref[...] = sum_ref[...]
            else:
                for m in range(n_sens // 128):
                    y = sum_ref[pl.ds(m * 128, 128), :]
                    y = y * y
                    y = y[:, :half] + y[:, half:]
                    row = jnp.sum(y.T, axis=0, keepdims=True)
                    out_ref[:, :, pl.ds(m * 128, 128)] = jnp.broadcast_to(row[None], (n_dev, 1, 128))

    specs = [pl.BlockSpec((kb_tiles, rows, half), lambda g: (g, 0, 0))]
    specs += [pl.BlockSpec((1, kb), lambda g: (0, g))] * 3
    args = [data, high, low, coef]
    if acc is not None:
        specs.append(pl.BlockSpec((n_sens, 2 * half), lambda g: (0, 0)))
        args.append(acc)
    shape = (n_dev, 1, n_sens) if last else (n_sens, 2 * half)
    return pl.pallas_call(
        body,
        grid=(n_dev // kb_tiles,),
        in_specs=specs,
        out_specs=pl.BlockSpec(shape, lambda g: (0,) * len(shape)),
        scratch_shapes=[pltpu.VMEM((n_sens, 2 * half), F32)],
        out_shape=jax.ShapeDtypeStruct(shape, F32),
        compiler_params=pltpu.CompilerParams(
            dimension_semantics=("arbitrary",), vmem_limit_bytes=VMEM
        ),
        name="mix_last" if last else "mix_chunk",
    )(*args)


def spread_squares(rows, coef, owner, me, tile_r, tile_c, sb=8):
    nblk, foot = rows.shape
    n_sens = owner.shape[1]

    def body(me_ref, rows_ref, coef_ref, owner_ref, map_ref, pos_ref):
        g = pl.program_id(0)

        @pl.when(g == 0)
        def _():
            mine = owner_ref[...] == me_ref[0]
            flag = jnp.broadcast_to(jnp.where(mine, 1.0, 0.0), (8, n_sens)).astype(BF16)
            row = lax.broadcasted_iota(I32, (n_sens, n_sens), 0)
            col = lax.broadcasted_iota(I32, (n_sens, n_sens), 1)
            before = jnp.where(row < col, 1.0, 0.0).astype(BF16)
            rank = jnp.dot(flag, before, preferred_element_type=F32)[0:1, :]
            pos_ref[...] = jnp.where(mine, rank.astype(I32), -1)

        sub_r = lax.broadcasted_iota(I32, (tile_r, foot), 0)
        sub_c = lax.broadcasted_iota(I32, (tile_c, foot), 0)
        point = rows_ref[...]
        high = point // tile_c
        low = point - high * tile_c
        c = coef_ref[...].astype(F32)
        sq = c * c
        sq_top = sq.astype(BF16).astype(F32)
        sq_rest = sq - sq_top
        for s in range(sb):
            at_r = sub_r == high[s : s + 1, :]
            left = jnp.concatenate(
                [jnp.where(at_r, sq_top[s : s + 1, :], 0.0), jnp.where(at_r, sq_rest[s : s + 1, :], 0.0)], axis=0
            ).astype(BF16)
            right = jnp.where(sub_c == low[s : s + 1, :], 1.0, 0.0).astype(BF16)
            both = lax.dot_general(left, right, (((1,), (1,)), ((), ())), preferred_element_type=F32)
            map_ref[s] = both[:tile_r] + both[tile_r:]

    return pl.pallas_call(
        body,
        grid=(nblk // sb,),
        in_specs=[
            pl.BlockSpec(memory_space=pltpu.SMEM),
            pl.BlockSpec((sb, foot), lambda g: (g, 0)),
            pl.BlockSpec((sb, foot), lambda g: (g, 0)),
            pl.BlockSpec((1, n_sens), lambda g: (0, 0)),
        ],
        out_specs=[
            pl.BlockSpec((sb, tile_r, tile_c), lambda g: (g, 0, 0)),
            pl.BlockSpec((1, n_sens), lambda g: (0, 0)),
        ],
        out_shape=[
            jax.ShapeDtypeStruct((nblk, tile_r, tile_c), F32),
            jax.ShapeDtypeStruct((1, n_sens), I32),
        ],
        compiler_params=pltpu.CompilerParams(
            dimension_semantics=("arbitrary",), vmem_limit_bytes=VMEM
        ),
        name="spread_squares",
    )(me, rows, coef, owner)


def finish(parts, weights, sensor, count, maps, pos, scale, sb=32):
    n_dev = parts.shape[0]
    n_sens = weights.shape[1]
    nblk, tile_r, tile_c = maps.shape
    pieces = nblk // sb

    def body(count_ref, parts_ref, weights_ref, sensor_ref, pos_ref, maps_hbm, sens_ref, new_ref, dens_ref, slot_w, maps_ref, sem):
        def fetch(i):
            return pltpu.make_async_copy(maps_hbm.at[pl.ds(i * sb, sb)], maps_ref.at[pl.ds(i * sb, sb)], sem.at[i])

        for i in range(pieces):
            fetch(i).start()
        h = jnp.sum(parts_ref[...], axis=0) * scale
        gain = weights_ref[...] * jnp.sqrt(1.0 + h)
        new = n_sens * gain / jnp.sum(gain)
        new_ref[...] = new
        k = lax.broadcasted_iota(I32, (SPD, n_sens), 0)
        own = jnp.sum(jnp.where(pos_ref[...] == k, h, 0.0), axis=1, keepdims=True)
        diag = lax.broadcasted_iota(I32, (SPD, 128), 0) == lax.broadcasted_iota(I32, (SPD, 128), 1)
        sens_ref[...] = jnp.sum(jnp.where(diag, own, 0.0), axis=0, keepdims=True)
        which = lax.broadcasted_iota(I32, (nblk, n_sens), 1)
        w = jnp.sum(jnp.where(which == sensor_ref[...], new, 0.0), axis=1, keepdims=True)
        alive = lax.broadcasted_iota(I32, (nblk, 1), 0) < count_ref[0]
        slot_w[...] = jnp.broadcast_to(jnp.where(alive, w, 0.0), (nblk, tile_c))
        dens_ref[...] = jnp.zeros((tile_r, tile_c), F32)
        for i in range(pieces):
            fetch(i).wait()

            def add(q, c):
                total = dens_ref[...]
                for s in range(8):
                    at = i * sb + q * 8 + s
                    total += slot_w[pl.ds(at, 1), :] * maps_ref[at]
                dens_ref[...] = total
                return c

            lax.fori_loop(0, sb // 8, add, 0)

    vmem = pl.BlockSpec(memory_space=pltpu.VMEM)
    return pl.pallas_call(
        body,
        in_specs=[pl.BlockSpec(memory_space=pltpu.SMEM), vmem, vmem, vmem, vmem, pl.BlockSpec(memory_space=pltpu.HBM)],
        out_specs=[vmem, vmem, vmem],
        out_shape=[
            jax.ShapeDtypeStruct((1, 128), F32),
            jax.ShapeDtypeStruct((1, n_sens), F32),
            jax.ShapeDtypeStruct((tile_r, tile_c), F32),
        ],
        scratch_shapes=[
            pltpu.VMEM((nblk, tile_c), F32),
            pltpu.VMEM((nblk, tile_r, tile_c), F32),
            pltpu.SemaphoreType.DMA((pieces,)),
        ],
        compiler_params=pltpu.CompilerParams(vmem_limit_bytes=VMEM),
        name="finish",
    )(count, parts, weights, sensor, pos, maps)


def exchange(x):
    return lax.all_to_all(x, AXES, split_axis=0, concat_axis=0, tiled=True)


def local(probes, blk_rows, blk_sensor, blk_count, coef, owner, weights):
    n_dev = lax.axis_size("gx") * lax.axis_size("gy")
    me = (lax.axis_index("gx") * lax.axis_size("gy") + lax.axis_index("gy")).astype(I32).reshape(1)
    tile_r, tile_c, probe_n = probes.shape
    nblk, foot = blk_rows.shape
    n_sens = owner.shape[0]
    flat = probes.reshape(tile_r * tile_c, probe_n)
    index = (blk_rows * 2).reshape(-1)
    maps, pos = spread_squares(blk_rows, coef, owner.reshape(1, n_sens), me, tile_r, tile_c)
    acc = side = None
    slot0 = 0
    for c, ns in enumerate(CHUNKS):
        last = c == len(CHUNKS) - 1
        got = exchange(gather_rows(flat, index, slot0, ns, (coef, blk_sensor.reshape(1, nblk), blk_count) if c == 0 else None))
        if c == 0:
            side = got[:, 2 * ns : 2 * ns + 3, :]
        if last:
            got, maps, pos = lax.optimization_barrier((got, maps, pos))
        w, high, low = (side[:, i, slot0 : slot0 + ns].reshape(1, n_dev * ns) for i in range(3))
        acc = mix_chunk(got, high, low, w, acc, ns, n_sens, last, TILES[ns])
        slot0 += ns
    parts = exchange(acc)
    sens, new, density = finish(
        parts, weights.reshape(1, n_sens), blk_sensor.reshape(nblk, 1), blk_count, maps, pos, 1.0 / (foot * probe_n)
    )
    return (sens[0, :SPD], new.reshape(n_sens), density)


def solution(mesh):
    in_specs = (
        P("gx", "gy", None),
        P(("gx", "gy"), None),
        P(("gx", "gy")),
        P(("gx", "gy")),
        P(("gx", "gy"), None),
        P(),
        P(),
    )
    out_specs = (P(("gx", "gy")), P(), P("gx", "gy"))
    return jax.shard_map(local, mesh=mesh, in_specs=in_specs, out_specs=out_specs, check_vma=False)
```

```python
import jax
import jax.numpy as jnp
from jax import lax
from jax.experimental import pallas as pl
from jax.experimental.pallas import tpu as pltpu
from jax.sharding import PartitionSpec as P

SPD = 8
AXES = ("gx", "gy")
CHUNKS = (32, 96)
SIDE = 8
ROOM = 5
VMEM = 60 * 1024 * 1024
MB = 256
TILES = {16: 128, 32: 64, 48: 64, 64: 32, 80: 32, 96: 32, 112: 32}
F32 = jnp.float32
BF16 = jnp.bfloat16
I32 = jnp.int32


def gather_rows(probes, rows, slot0, ns, side=None, rb=32, unroll=4):
    n, pn = probes.shape
    nblk, foot = rows.shape
    half = pn // 2
    extra = 0 if side is None else SIDE
    parts = 8
    step = n // parts
    n_side = 0 if side is None else 3

    def body(*refs):
        x_hbm, rows_hbm = refs[:2]
        side_refs = refs[2 : 2 + n_side]
        out_ref, idx, idx_v, raw, tab, stage, coef_t, sem = refs[2 + n_side :]
        g = pl.program_id(0)

        @pl.when(g == 0)
        def _():
            def fetch(i):
                return pltpu.make_async_copy(x_hbm.at[pl.ds(i * step, step), :], raw.at[pl.ds(i * step, step), :], sem.at[i])

            index = pltpu.make_async_copy(rows_hbm.at[pl.ds(slot0, ns), :], idx_v, sem.at[parts])
            index.start()
            for i in range(parts):
                fetch(i).start()
            index.wait()
            idx_v[...] = idx_v[...] * 2
            doubled = pltpu.make_async_copy(idx_v, idx, sem.at[parts + 1])
            doubled.start()
            if side is not None:
                coef_ref, _, count_ref = side_refs
                alive = lax.broadcasted_iota(I32, (nblk, foot), 0) < count_ref[0]
                coef_t[...] = jnp.where(alive, coef_ref[...].astype(F32), 0.0).T
            ch = 512
            for i in range(parts):
                fetch(i).wait()

                def conv(q, c):
                    at = i * step + q * ch
                    x = raw[pl.ds(at, ch), :].astype(F32)
                    tab[pl.ds(at * 2, ch, stride=2), :] = x[:, :half]
                    tab[pl.ds(at * 2 + 1, ch, stride=2), :] = x[:, half:]
                    return c

                lax.fori_loop(0, step // ch, conv, 0)
            doubled.wait()

        def channels(t, c):
            for u in range(unroll):
                r = g * rb + t * unroll + u
                for j in range(ns):
                    at = pl.multiple_of(idx.at[j][r], 2)
                    stage[u, pl.ds(2 * j, 2), :] = tab[pl.ds(at, 2), :]
            for u in range(unroll):
                q = t * unroll + u
                out_ref[q, pl.ds(0, ns), :] = stage[u, pl.ds(0, ns, stride=2), :].astype(BF16)
                out_ref[q, pl.ds(ns, ns), :] = stage[u, pl.ds(1, ns, stride=2), :].astype(BF16)
                if side is not None:
                    sensor = side_refs[1][...]
                    high = sensor // MB
                    low = sensor - high * MB
                    row = lax.broadcasted_iota(I32, (SIDE, nblk), 0)
                    tail = jnp.where(row == 1, high, jnp.where(row == 2, low, 0)).astype(F32)
                    tail = jnp.where(row == 0, coef_t[pl.ds(g * rb + q, 1), :], tail)
                    out_ref[q, pl.ds(2 * ns, SIDE), :] = tail.astype(BF16)
            return c

        lax.fori_loop(0, rb // unroll, channels, 0)

    specs = [pl.BlockSpec(memory_space=pltpu.HBM)] * 2
    args = [probes, rows]
    if side is not None:
        specs += [
            pl.BlockSpec((nblk, foot), lambda g: (0, 0)),
            pl.BlockSpec((1, nblk), lambda g: (0, 0)),
            pl.BlockSpec(memory_space=pltpu.SMEM),
        ]
        args += list(side)
    return pl.pallas_call(
        body,
        grid=(foot // rb,),
        in_specs=specs,
        out_specs=pl.BlockSpec((rb, 2 * ns + extra, half), lambda g: (g, 0, 0)),
        scratch_shapes=[
            pltpu.SMEM((ns, foot), I32),
            pltpu.VMEM((ns, foot), I32),
            pltpu.VMEM((n, pn), BF16),
            pltpu.VMEM((2 * n, half), F32),
            pltpu.VMEM((unroll, 2 * ns, half), F32),
            pltpu.VMEM((foot, nblk), F32),
            pltpu.SemaphoreType.DMA((parts + 2,)),
        ],
        out_shape=jax.ShapeDtypeStruct((foot, 2 * ns + extra, half), BF16),
        compiler_params=pltpu.CompilerParams(dimension_semantics=("arbitrary",), vmem_limit_bytes=VMEM),
        name="gather_rows",
    )(*args)


def mix_chunk(data, high, low, coef, acc, ns, n_sens, last, kb_tiles):
    n_dev, rows, half = data.shape
    kb = kb_tiles * ns
    n_m = n_sens // MB

    def body(*refs):
        data_ref, high_ref, low_ref, coef_ref = refs[:4]
        acc_ref = None if acc is None else refs[4]
        out_ref, sum_ref = refs[-2:]
        g = pl.program_id(0)

        @pl.when(g == 0)
        def _():
            if acc_ref is None:
                sum_ref[...] = jnp.zeros((n_sens, 2 * half), F32)
            else:
                sum_ref[...] = acc_ref[...]

        x = data_ref[...]
        x = jnp.concatenate([x[:, :ns].reshape(kb, half), x[:, ns : 2 * ns].reshape(kb, half)], axis=1)
        weight = coef_ref[...]
        sub = lax.broadcasted_iota(I32, (MB, kb), 0).astype(F32).astype(BF16)
        for m in range(n_m):
            wanted = jnp.where(high_ref[...] == m, low_ref[...], -1.0).astype(BF16)
            mixer = jnp.where(sub == wanted, weight, jnp.zeros((), BF16))
            sum_ref[pl.ds(m * MB, MB), :] += jnp.dot(mixer, x, preferred_element_type=F32)

        @pl.when(g == pl.num_programs(0) - 1)
        def _():
            if not last:
                out_ref[...] = sum_ref[...]
            else:
                for m in range(n_sens // 128):
                    y = sum_ref[pl.ds(m * 128, 128), :]
                    y = y * y
                    y = y[:, :half] + y[:, half:]
                    row = jnp.sum(y.T, axis=0, keepdims=True)
                    out_ref[:, :, pl.ds(m * 128, 128)] = jnp.broadcast_to(row[None], (n_dev, 1, 128))

    specs = [pl.BlockSpec((kb_tiles, rows, half), lambda g: (g, 0, 0))]
    specs += [pl.BlockSpec((1, kb), lambda g: (0, g))] * 3
    args = [data, high, low, coef]
    if acc is not None:
        specs.append(pl.BlockSpec((n_sens, 2 * half), lambda g: (0, 0)))
        args.append(acc)
    shape = (n_dev, 1, n_sens) if last else (n_sens, 2 * half)
    return pl.pallas_call(
        body,
        grid=(n_dev // kb_tiles,),
        in_specs=specs,
        out_specs=pl.BlockSpec(shape, lambda g: (0,) * len(shape)),
        scratch_shapes=[pltpu.VMEM((n_sens, 2 * half), F32)],
        out_shape=jax.ShapeDtypeStruct(shape, F32),
        compiler_params=pltpu.CompilerParams(
            dimension_semantics=("arbitrary",), vmem_limit_bytes=VMEM
        ),
        name="mix_last" if last else "mix_chunk",
    )(*args)


def spread_squares(rows, coef, owner, me, tile_r, tile_c, sb=8):
    nblk, foot = rows.shape
    n_sens = owner.shape[1]

    def body(me_ref, rows_ref, coef_ref, owner_ref, map_ref, pos_ref):
        g = pl.program_id(0)

        @pl.when(g == 0)
        def _():
            mine = owner_ref[...] == me_ref[0]
            flag = jnp.broadcast_to(jnp.where(mine, 1.0, 0.0), (8, n_sens)).astype(BF16)
            row = lax.broadcasted_iota(I32, (n_sens, n_sens), 0)
            col = lax.broadcasted_iota(I32, (n_sens, n_sens), 1)
            before = jnp.where(row < col, 1.0, 0.0).astype(BF16)
            rank = jnp.dot(flag, before, preferred_element_type=F32)[0:1, :]
            pos_ref[...] = jnp.where(mine, rank.astype(I32), -1)

        sub_r = lax.broadcasted_iota(I32, (tile_r, foot), 0)
        sub_c = lax.broadcasted_iota(I32, (tile_c, foot), 0)
        point = rows_ref[...]
        high = point // tile_c
        low = point - high * tile_c
        c = coef_ref[...].astype(F32)
        sq = c * c
        sq_top = sq.astype(BF16).astype(F32)
        sq_rest = sq - sq_top
        for s in range(sb):
            at_r = sub_r == high[s : s + 1, :]
            left = jnp.concatenate(
                [jnp.where(at_r, sq_top[s : s + 1, :], 0.0), jnp.where(at_r, sq_rest[s : s + 1, :], 0.0)], axis=0
            ).astype(BF16)
            right = jnp.where(sub_c == low[s : s + 1, :], 1.0, 0.0).astype(BF16)
            both = lax.dot_general(left, right, (((1,), (1,)), ((), ())), preferred_element_type=F32)
            map_ref[s] = both[:tile_r] + both[tile_r:]

    return pl.pallas_call(
        body,
        grid=(nblk // sb,),
        in_specs=[
            pl.BlockSpec(memory_space=pltpu.SMEM),
            pl.BlockSpec((sb, foot), lambda g: (g, 0)),
            pl.BlockSpec((sb, foot), lambda g: (g, 0)),
            pl.BlockSpec((1, n_sens), lambda g: (0, 0)),
        ],
        out_specs=[
            pl.BlockSpec((sb, tile_r, tile_c), lambda g: (g, 0, 0)),
            pl.BlockSpec((1, n_sens), lambda g: (0, 0)),
        ],
        out_shape=[
            jax.ShapeDtypeStruct((ROOM * nblk, tile_r, tile_c), F32),
            jax.ShapeDtypeStruct((1, n_sens), I32),
        ],
        compiler_params=pltpu.CompilerParams(
            dimension_semantics=("arbitrary",), vmem_limit_bytes=VMEM
        ),
        name="spread_squares",
    )(me, rows, coef, owner)


def finish(parts, weights, sensor, count, maps, pos, scale, sb=32):
    n_dev = parts.shape[0]
    n_sens = weights.shape[1]
    nblk = sensor.shape[0]
    tile_r, tile_c = maps.shape[1:]
    pieces = nblk // sb

    def body(count_ref, parts_ref, weights_ref, sensor_ref, pos_ref, maps_hbm, sens_ref, new_ref, dens_ref, slot_w, maps_ref, sem):
        def fetch(i):
            return pltpu.make_async_copy(maps_hbm.at[pl.ds(i * sb, sb)], maps_ref.at[pl.ds(i * sb, sb)], sem.at[i])

        for i in range(pieces):
            fetch(i).start()
        h = jnp.sum(parts_ref[...], axis=0) * scale
        gain = weights_ref[...] * jnp.sqrt(1.0 + h)
        new = n_sens * gain / jnp.sum(gain)
        new_ref[...] = new
        k = lax.broadcasted_iota(I32, (SPD, n_sens), 0)
        own = jnp.sum(jnp.where(pos_ref[...] == k, h, 0.0), axis=1, keepdims=True)
        diag = lax.broadcasted_iota(I32, (SPD, SPD), 0) == lax.broadcasted_iota(I32, (SPD, SPD), 1)
        sens_ref[...] = jnp.sum(jnp.where(diag, own, 0.0), axis=0, keepdims=True)
        which = lax.broadcasted_iota(I32, (nblk, n_sens), 1)
        w = jnp.sum(jnp.where(which == sensor_ref[...], new, 0.0), axis=1, keepdims=True)
        alive = lax.broadcasted_iota(I32, (nblk, 1), 0) < count_ref[0]
        slot_w[...] = jnp.broadcast_to(jnp.where(alive, w, 0.0), (nblk, tile_c))
        dens_ref[...] = jnp.zeros((tile_r, tile_c), F32)
        for i in range(pieces):
            fetch(i).wait()

            def add(q, c):
                total = dens_ref[...]
                for s in range(8):
                    at = i * sb + q * 8 + s
                    total += slot_w[pl.ds(at, 1), :] * maps_ref[at]
                dens_ref[...] = total
                return c

            lax.fori_loop(0, sb // 8, add, 0)

    vmem = pl.BlockSpec(memory_space=pltpu.VMEM)
    return pl.pallas_call(
        body,
        in_specs=[pl.BlockSpec(memory_space=pltpu.SMEM), vmem, vmem, vmem, vmem, pl.BlockSpec(memory_space=pltpu.HBM)],
        out_specs=[vmem, vmem, vmem],
        out_shape=[
            jax.ShapeDtypeStruct((1, SPD), F32),
            jax.ShapeDtypeStruct((1, n_sens), F32),
            jax.ShapeDtypeStruct((tile_r, tile_c), F32),
        ],
        scratch_shapes=[
            pltpu.VMEM((nblk, tile_c), F32),
            pltpu.VMEM((nblk, tile_r, tile_c), F32),
            pltpu.SemaphoreType.DMA((pieces,)),
        ],
        compiler_params=pltpu.CompilerParams(vmem_limit_bytes=48 * 1024 * 1024),
        name="finish",
    )(count, parts, weights, sensor, pos, maps)


def exchange(x):
    return lax.all_to_all(x, AXES, split_axis=0, concat_axis=0, tiled=True)


def local(probes, blk_rows, blk_sensor, blk_count, coef, owner, weights):
    n_dev = lax.axis_size("gx") * lax.axis_size("gy")
    me = (lax.axis_index("gx") * lax.axis_size("gy") + lax.axis_index("gy")).astype(I32).reshape(1)
    tile_r, tile_c, probe_n = probes.shape
    nblk, foot = blk_rows.shape
    n_sens = owner.shape[0]
    flat = probes.reshape(tile_r * tile_c, probe_n)
    maps, pos = spread_squares(blk_rows, coef, owner.reshape(1, n_sens), me, tile_r, tile_c)
    acc = side = None
    slot0 = 0
    for c, ns in enumerate(CHUNKS):
        last = c == len(CHUNKS) - 1
        got = exchange(gather_rows(flat, blk_rows, slot0, ns, (coef, blk_sensor.reshape(1, nblk), blk_count) if c == 0 else None))
        if c == 0:
            side = got[:, 2 * ns : 2 * ns + 3, :]
        if last:
            got, maps, pos = lax.optimization_barrier((got, maps, pos))
        w, high, low = (side[:, i, slot0 : slot0 + ns].reshape(1, n_dev * ns) for i in range(3))
        acc = mix_chunk(got, high, low, w, acc, ns, n_sens, last, TILES[ns])
        slot0 += ns
    parts = exchange(acc)
    sens, new, density = finish(
        parts, weights.reshape(1, n_sens), blk_sensor.reshape(nblk, 1), blk_count, maps, pos, 1.0 / (foot * probe_n)
    )
    return (sens.reshape(SPD), new.reshape(n_sens), density)


def solution(mesh):
    in_specs = (
        P("gx", "gy", None),
        P(("gx", "gy"), None),
        P(("gx", "gy")),
        P(("gx", "gy")),
        P(("gx", "gy"), None),
        P(),
        P(),
    )
    out_specs = (P(("gx", "gy")), P(), P("gx", "gy"))
    return jax.shard_map(local, mesh=mesh, in_specs=in_specs, out_specs=out_specs, check_vma=False)
```

```python
import jax
import jax.numpy as jnp
from jax import lax
from jax.experimental import pallas as pl
from jax.experimental.pallas import tpu as pltpu
from jax.sharding import PartitionSpec as P

SPD = 8
AXES = ("gx", "gy")
CHUNKS = (112, 16)
SIDE = 8
ROOM = 5
VMEM = 60 * 1024 * 1024
MB = 256
TILES = {16: 64, 32: 64, 48: 64, 64: 32, 80: 32, 96: 32, 112: 32}
F32 = jnp.float32
BF16 = jnp.bfloat16
I32 = jnp.int32


def gather_rows(probes, rows, slot0, ns, side=None, rb=32, unroll=4):
    n, pn = probes.shape
    nblk, foot = rows.shape
    half = pn // 2
    extra = 0 if side is None else SIDE
    parts = 8
    step = n // parts
    n_side = 0 if side is None else 3

    def body(*refs):
        x_hbm, rows_hbm = refs[:2]
        side_refs = refs[2 : 2 + n_side]
        out_ref, idx, idx_v, raw, tab, stage, coef_t, sem = refs[2 + n_side :]
        g = pl.program_id(0)

        @pl.when(g == 0)
        def _():
            def fetch(i):
                return pltpu.make_async_copy(x_hbm.at[pl.ds(i * step, step), :], raw.at[pl.ds(i * step, step), :], sem.at[i])

            index = pltpu.make_async_copy(rows_hbm.at[pl.ds(slot0, ns), :], idx_v, sem.at[parts])
            index.start()
            for i in range(parts):
                fetch(i).start()
            index.wait()
            idx_v[...] = idx_v[...] * 2
            doubled = pltpu.make_async_copy(idx_v, idx, sem.at[parts + 1])
            doubled.start()
            if side is not None:
                coef_ref, _, count_ref = side_refs
                alive = lax.broadcasted_iota(I32, (nblk, foot), 0) < count_ref[0]
                coef_t[...] = jnp.where(alive, coef_ref[...].astype(F32), 0.0).T
            ch = 512
            for i in range(parts):
                fetch(i).wait()

                def conv(q, c):
                    at = i * step + q * ch
                    x = raw[pl.ds(at, ch), :].astype(F32)
                    tab[pl.ds(at * 2, ch, stride=2), :] = x[:, :half]
                    tab[pl.ds(at * 2 + 1, ch, stride=2), :] = x[:, half:]
                    return c

                lax.fori_loop(0, step // ch, conv, 0)
            doubled.wait()

        def channels(t, c):
            for u in range(unroll):
                r = g * rb + t * unroll + u
                for j in range(ns):
                    at = pl.multiple_of(idx.at[j][r], 2)
                    stage[u, pl.ds(2 * j, 2), :] = tab[pl.ds(at, 2), :]
            for u in range(unroll):
                q = t * unroll + u
                out_ref[q, pl.ds(0, ns), :] = stage[u, pl.ds(0, ns, stride=2), :].astype(BF16)
                out_ref[q, pl.ds(ns, ns), :] = stage[u, pl.ds(1, ns, stride=2), :].astype(BF16)
                if side is not None:
                    sensor = side_refs[1][...]
                    high = sensor // MB
                    low = sensor - high * MB
                    row = lax.broadcasted_iota(I32, (SIDE, nblk), 0)
                    tail = jnp.where(row == 1, high, jnp.where(row == 2, low, 0)).astype(F32)
                    tail = jnp.where(row == 0, coef_t[pl.ds(g * rb + q, 1), :], tail)
                    out_ref[q, pl.ds(2 * ns, SIDE), :] = tail.astype(BF16)
            return c

        lax.fori_loop(0, rb // unroll, channels, 0)

    specs = [pl.BlockSpec(memory_space=pltpu.HBM)] * 2
    args = [probes, rows]
    if side is not None:
        specs += [
            pl.BlockSpec((nblk, foot), lambda g: (0, 0)),
            pl.BlockSpec((1, nblk), lambda g: (0, 0)),
            pl.BlockSpec(memory_space=pltpu.SMEM),
        ]
        args += list(side)
    return pl.pallas_call(
        body,
        grid=(foot // rb,),
        in_specs=specs,
        out_specs=pl.BlockSpec((rb, 2 * ns + extra, half), lambda g: (g, 0, 0)),
        scratch_shapes=[
            pltpu.SMEM((ns, foot), I32),
            pltpu.VMEM((ns, foot), I32),
            pltpu.VMEM((n, pn), BF16),
            pltpu.VMEM((2 * n, half), F32),
            pltpu.VMEM((unroll, 2 * ns, half), F32),
            pltpu.VMEM((foot, nblk), F32),
            pltpu.SemaphoreType.DMA((parts + 2,)),
        ],
        out_shape=jax.ShapeDtypeStruct((foot, 2 * ns + extra, half), BF16),
        compiler_params=pltpu.CompilerParams(dimension_semantics=("arbitrary",), vmem_limit_bytes=VMEM),
        name="gather_rows",
    )(*args)


def mix_chunk(data, high, low, coef, acc, ns, n_sens, last, kb_tiles):
    n_dev, rows, half = data.shape
    kb = kb_tiles * ns
    n_m = n_sens // MB

    def body(*refs):
        data_ref, high_ref, low_ref, coef_ref = refs[:4]
        acc_ref = None if acc is None else refs[4]
        out_ref, sum_ref = refs[-2:]
        g = pl.program_id(0)

        @pl.when(g == 0)
        def _():
            if acc_ref is None:
                sum_ref[...] = jnp.zeros((n_sens, 2 * half), F32)
            else:
                sum_ref[...] = acc_ref[...]

        x = data_ref[...]
        x = jnp.concatenate([x[:, :ns].reshape(kb, half), x[:, ns : 2 * ns].reshape(kb, half)], axis=1)
        weight = coef_ref[...]
        sub = lax.broadcasted_iota(I32, (MB, kb), 0).astype(F32).astype(BF16)
        for m in range(n_m):
            wanted = jnp.where(high_ref[...] == m, low_ref[...], -1.0).astype(BF16)
            mixer = jnp.where(sub == wanted, weight, jnp.zeros((), BF16))
            sum_ref[pl.ds(m * MB, MB), :] += jnp.dot(mixer, x, preferred_element_type=F32)

        @pl.when(g == pl.num_programs(0) - 1)
        def _():
            if not last:
                out_ref[...] = sum_ref[...]
            else:
                for m in range(n_sens // 128):
                    y = sum_ref[pl.ds(m * 128, 128), :]
                    y = y * y
                    y = y[:, :half] + y[:, half:]
                    row = jnp.sum(y.T, axis=0, keepdims=True)
                    out_ref[:, :, pl.ds(m * 128, 128)] = jnp.broadcast_to(row[None], (n_dev, 1, 128))

    specs = [pl.BlockSpec((kb_tiles, rows, half), lambda g: (g, 0, 0))]
    specs += [pl.BlockSpec((1, kb), lambda g: (0, g))] * 3
    args = [data, high, low, coef]
    if acc is not None:
        specs.append(pl.BlockSpec((n_sens, 2 * half), lambda g: (0, 0)))
        args.append(acc)
    shape = (n_dev, 1, n_sens) if last else (n_sens, 2 * half)
    return pl.pallas_call(
        body,
        grid=(n_dev // kb_tiles,),
        in_specs=specs,
        out_specs=pl.BlockSpec(shape, lambda g: (0,) * len(shape)),
        scratch_shapes=[pltpu.VMEM((n_sens, 2 * half), F32)],
        out_shape=jax.ShapeDtypeStruct(shape, F32),
        compiler_params=pltpu.CompilerParams(
            dimension_semantics=("arbitrary",), vmem_limit_bytes=VMEM
        ),
        name="mix_last" if last else "mix_chunk",
    )(*args)


def spread_squares(rows, coef, owner, me, tile_r, tile_c, sb=8):
    nblk, foot = rows.shape
    n_sens = owner.shape[1]

    def body(me_ref, rows_ref, coef_ref, owner_ref, map_ref, pos_ref):
        g = pl.program_id(0)

        @pl.when(g == 0)
        def _():
            mine = owner_ref[...] == me_ref[0]
            flag = jnp.broadcast_to(jnp.where(mine, 1.0, 0.0), (8, n_sens)).astype(BF16)
            row = lax.broadcasted_iota(I32, (n_sens, n_sens), 0)
            col = lax.broadcasted_iota(I32, (n_sens, n_sens), 1)
            before = jnp.where(row < col, 1.0, 0.0).astype(BF16)
            rank = jnp.dot(flag, before, preferred_element_type=F32)[0:1, :]
            pos_ref[...] = jnp.where(mine, rank.astype(I32), -1)

        sub_r = lax.broadcasted_iota(I32, (tile_r, foot), 0)
        sub_c = lax.broadcasted_iota(I32, (tile_c, foot), 0)
        point = rows_ref[...]
        high = point // tile_c
        low = point - high * tile_c
        c = coef_ref[...].astype(F32)
        sq = c * c
        sq_top = sq.astype(BF16).astype(F32)
        sq_rest = sq - sq_top
        for s in range(sb):
            at_r = sub_r == high[s : s + 1, :]
            left = jnp.concatenate(
                [jnp.where(at_r, sq_top[s : s + 1, :], 0.0), jnp.where(at_r, sq_rest[s : s + 1, :], 0.0)], axis=0
            ).astype(BF16)
            right = jnp.where(sub_c == low[s : s + 1, :], 1.0, 0.0).astype(BF16)
            both = lax.dot_general(left, right, (((1,), (1,)), ((), ())), preferred_element_type=F32)
            map_ref[s] = both[:tile_r] + both[tile_r:]

    return pl.pallas_call(
        body,
        grid=(nblk // sb,),
        in_specs=[
            pl.BlockSpec(memory_space=pltpu.SMEM),
            pl.BlockSpec((sb, foot), lambda g: (g, 0)),
            pl.BlockSpec((sb, foot), lambda g: (g, 0)),
            pl.BlockSpec((1, n_sens), lambda g: (0, 0)),
        ],
        out_specs=[
            pl.BlockSpec((sb, tile_r, tile_c), lambda g: (g, 0, 0)),
            pl.BlockSpec((1, n_sens), lambda g: (0, 0)),
        ],
        out_shape=[
            jax.ShapeDtypeStruct((ROOM * nblk, tile_r, tile_c), F32),
            jax.ShapeDtypeStruct((1, n_sens), I32),
        ],
        compiler_params=pltpu.CompilerParams(
            dimension_semantics=("arbitrary",), vmem_limit_bytes=VMEM
        ),
        name="spread_squares",
    )(me, rows, coef, owner)


def finish(parts, weights, sensor, count, maps, pos, scale, sb=32):
    n_dev = parts.shape[0]
    n_sens = weights.shape[1]
    nblk = sensor.shape[0]
    tile_r, tile_c = maps.shape[1:]
    pieces = nblk // sb

    def body(count_ref, parts_ref, weights_ref, sensor_ref, pos_ref, maps_hbm, sens_ref, new_ref, dens_ref, slot_w, maps_ref, sem):
        def fetch(i):
            return pltpu.make_async_copy(maps_hbm.at[pl.ds(i * sb, sb)], maps_ref.at[pl.ds(i * sb, sb)], sem.at[i])

        for i in range(pieces):
            fetch(i).start()
        h = jnp.sum(parts_ref[...], axis=0) * scale
        gain = weights_ref[...] * jnp.sqrt(1.0 + h)
        new = n_sens * gain / jnp.sum(gain)
        new_ref[...] = new
        k = lax.broadcasted_iota(I32, (SPD, n_sens), 0)
        own = jnp.sum(jnp.where(pos_ref[...] == k, h, 0.0), axis=1, keepdims=True)
        diag = lax.broadcasted_iota(I32, (SPD, SPD), 0) == lax.broadcasted_iota(I32, (SPD, SPD), 1)
        sens_ref[...] = jnp.sum(jnp.where(diag, own, 0.0), axis=0, keepdims=True)
        which = lax.broadcasted_iota(I32, (nblk, n_sens), 1)
        w = jnp.sum(jnp.where(which == sensor_ref[...], new, 0.0), axis=1, keepdims=True)
        alive = lax.broadcasted_iota(I32, (nblk, 1), 0) < count_ref[0]
        slot_w[...] = jnp.broadcast_to(jnp.where(alive, w, 0.0), (nblk, tile_c))
        dens_ref[...] = jnp.zeros((tile_r, tile_c), F32)
        for i in range(pieces):
            fetch(i).wait()

            def add(q, c):
                total = dens_ref[...]
                for s in range(8):
                    at = i * sb + q * 8 + s
                    total += slot_w[pl.ds(at, 1), :] * maps_ref[at]
                dens_ref[...] = total
                return c

            lax.fori_loop(0, sb // 8, add, 0)

    vmem = pl.BlockSpec(memory_space=pltpu.VMEM)
    return pl.pallas_call(
        body,
        in_specs=[pl.BlockSpec(memory_space=pltpu.SMEM), vmem, vmem, vmem, vmem, pl.BlockSpec(memory_space=pltpu.HBM)],
        out_specs=[vmem, vmem, vmem],
        out_shape=[
            jax.ShapeDtypeStruct((1, SPD), F32),
            jax.ShapeDtypeStruct((1, n_sens), F32),
            jax.ShapeDtypeStruct((tile_r, tile_c), F32),
        ],
        scratch_shapes=[
            pltpu.VMEM((nblk, tile_c), F32),
            pltpu.VMEM((nblk, tile_r, tile_c), F32),
            pltpu.SemaphoreType.DMA((pieces,)),
        ],
        compiler_params=pltpu.CompilerParams(vmem_limit_bytes=48 * 1024 * 1024),
        name="finish",
    )(count, parts, weights, sensor, pos, maps)


def exchange(x):
    return lax.all_to_all(x, AXES, split_axis=0, concat_axis=0, tiled=True)


def local(probes, blk_rows, blk_sensor, blk_count, coef, owner, weights):
    n_dev = lax.axis_size("gx") * lax.axis_size("gy")
    me = (lax.axis_index("gx") * lax.axis_size("gy") + lax.axis_index("gy")).astype(I32).reshape(1)
    tile_r, tile_c, probe_n = probes.shape
    nblk, foot = blk_rows.shape
    n_sens = owner.shape[0]
    flat = probes.reshape(tile_r * tile_c, probe_n)
    maps, pos = spread_squares(blk_rows, coef, owner.reshape(1, n_sens), me, tile_r, tile_c)
    acc = side = None
    slot0 = 0
    for c, ns in enumerate(CHUNKS):
        last = c == len(CHUNKS) - 1
        got = exchange(gather_rows(flat, blk_rows, slot0, ns, (coef, blk_sensor.reshape(1, nblk), blk_count) if c == 0 else None))
        if c == 0:
            side = got[:, 2 * ns : 2 * ns + 3, :]
        if last:
            got, maps, pos = lax.optimization_barrier((got, maps, pos))
        w, high, low = (side[:, i, slot0 : slot0 + ns].reshape(1, n_dev * ns) for i in range(3))
        acc = mix_chunk(got, high, low, w, acc, ns, n_sens, last, TILES[ns])
        slot0 += ns
    parts = exchange(acc)
    sens, new, density = finish(
        parts, weights.reshape(1, n_sens), blk_sensor.reshape(nblk, 1), blk_count, maps, pos, 1.0 / (foot * probe_n)
    )
    return (sens.reshape(SPD), new.reshape(n_sens), density)


def solution(mesh):
    in_specs = (
        P("gx", "gy", None),
        P(("gx", "gy"), None),
        P(("gx", "gy")),
        P(("gx", "gy")),
        P(("gx", "gy"), None),
        P(),
        P(),
    )
    out_specs = (P(("gx", "gy")), P(), P("gx", "gy"))
    return jax.shard_map(local, mesh=mesh, in_specs=in_specs, out_specs=out_specs, check_vma=False)
```

```python
import jax
import jax.numpy as jnp
from jax import lax
from jax.experimental import pallas as pl
from jax.experimental.pallas import tpu as pltpu
from jax.sharding import Mesh
from jax.sharding import PartitionSpec as P

SPD = 8
AXES = ("gx", "z", "core")
SIDE = 8
ROOM = 5
VMEM = 60 * 1024 * 1024
MB = 256
F32 = jnp.float32
BF16 = jnp.bfloat16
I32 = jnp.int32


def gather_rows(probes, rows, coef, sensor, count, core, rb=16, unroll=4):
    n, pn = probes.shape
    nblk, foot = rows.shape
    half = pn // 2
    parts = 8
    step = n // parts

    def body(x_hbm, rows_hbm, coef_ref, sensor_ref, count_ref, core_ref, out_ref, idx, idx_v, raw, tab, stage, coef_t, sem):
        g = pl.program_id(0)

        @pl.when(g == 0)
        def _():
            def fetch(i):
                return pltpu.make_async_copy(x_hbm.at[pl.ds(i * step, step), :], raw.at[pl.ds(i * step, step), :], sem.at[i])

            index = pltpu.make_async_copy(rows_hbm, idx_v, sem.at[parts])
            index.start()
            for i in range(parts):
                fetch(i).start()
            index.wait()
            idx_v[...] = idx_v[...] * 2
            doubled = pltpu.make_async_copy(idx_v, idx, sem.at[parts + 1])
            doubled.start()
            alive = lax.broadcasted_iota(I32, (nblk, foot), 0) < count_ref[0]
            coef_t[...] = jnp.where(alive, coef_ref[...].astype(F32), 0.0).T
            ch = 512
            for i in range(parts):
                fetch(i).wait()

                def conv(q, c):
                    at = i * step + q * ch
                    x = raw[pl.ds(at, ch), :].astype(F32)
                    tab[pl.ds(at * 2, ch, stride=2), :] = x[:, :half]
                    tab[pl.ds(at * 2 + 1, ch, stride=2), :] = x[:, half:]
                    return c

                lax.fori_loop(0, step // ch, conv, 0)
            doubled.wait()

        def channels(t, c):
            for u in range(unroll):
                r = (g * rb + t * unroll + u) * 2 + core_ref[0]
                for j in range(nblk):
                    at = pl.multiple_of(idx.at[j][r], 2)
                    stage[u, pl.ds(2 * j, 2), :] = tab[pl.ds(at, 2), :]
            for u in range(unroll):
                q = t * unroll + u
                out_ref[q, pl.ds(0, nblk), :] = stage[u, pl.ds(0, nblk, stride=2), :].astype(BF16)
                out_ref[q, pl.ds(nblk, nblk), :] = stage[u, pl.ds(1, nblk, stride=2), :].astype(BF16)
                high = sensor_ref[...] // MB
                low = sensor_ref[...] - high * MB
                row = lax.broadcasted_iota(I32, (SIDE, nblk), 0)
                tail = jnp.where(row == 1, high, jnp.where(row == 2, low, 0)).astype(F32)
                tail = jnp.where(row == 0, coef_t[pl.ds((g * rb + q) * 2 + core_ref[0], 1), :], tail)
                out_ref[q, pl.ds(2 * nblk, SIDE), :] = tail.astype(BF16)
            return c

        lax.fori_loop(0, rb // unroll, channels, 0)

    hbm = pl.BlockSpec(memory_space=pltpu.HBM)
    smem = pl.BlockSpec(memory_space=pltpu.SMEM)
    shape = (foot // 2, 2 * nblk + SIDE, half)
    return pl.pallas_call(
        body,
        grid=(foot // 2 // rb,),
        in_specs=[
            hbm,
            hbm,
            pl.BlockSpec((nblk, foot), lambda g: (0, 0)),
            pl.BlockSpec((1, nblk), lambda g: (0, 0)),
            smem,
            smem,
        ],
        out_specs=pl.BlockSpec((rb,) + shape[1:], lambda g: (g, 0, 0)),
        scratch_shapes=[
            pltpu.SMEM((nblk, foot), I32),
            pltpu.VMEM((nblk, foot), I32),
            pltpu.VMEM((n, pn), BF16),
            pltpu.VMEM((2 * n, half), F32),
            pltpu.VMEM((unroll, 2 * nblk, half), F32),
            pltpu.VMEM((foot, nblk), F32),
            pltpu.SemaphoreType.DMA((parts + 2,)),
        ],
        out_shape=jax.ShapeDtypeStruct(shape, BF16),
        compiler_params=pltpu.CompilerParams(dimension_semantics=("arbitrary",), vmem_limit_bytes=VMEM),
        name="gather_rows",
    )(probes, rows, coef, sensor, count, core)


def mix_chunk(data, acc, n_sens, n_dev, last, tiles=16):
    n_tiles, rows, half = data.shape
    ns = half
    kb = tiles * ns
    n_m = n_sens // MB

    def body(*refs):
        data_ref = refs[0]
        acc_ref = None if acc is None else refs[1]
        out_ref, sum_ref = refs[-2:]
        g = pl.program_id(0)

        @pl.when(g == 0)
        def _():
            if acc_ref is None:
                sum_ref[...] = jnp.zeros((n_sens, 2 * half), F32)
            else:
                sum_ref[...] = acc_ref[...]

        x = jnp.concatenate([data_ref[:, :ns].reshape(kb, half), data_ref[:, ns : 2 * ns].reshape(kb, half)], axis=1)
        side = [data_ref[t, 2 * ns :].astype(F32) for t in range(tiles)]
        coef, high, low = (jnp.concatenate([s[i : i + 1] for s in side], axis=1) for i in range(3))
        coef = coef.astype(BF16)
        sub = lax.broadcasted_iota(I32, (MB, kb), 0).astype(F32).astype(BF16)
        for m in range(n_m):
            wanted = jnp.where(high == m, low, -1.0).astype(BF16)
            mixer = jnp.where(sub == wanted, coef, jnp.zeros((), BF16))
            sum_ref[pl.ds(m * MB, MB), :] += jnp.dot(mixer, x, preferred_element_type=F32)

        @pl.when(g == pl.num_programs(0) - 1)
        def _():
            if not last:
                out_ref[...] = sum_ref[...]
            else:
                lanes = []
                for m in range(n_sens // 128):
                    y = sum_ref[pl.ds(m * 128, 128), :]
                    y = y * y
                    y = y[:, :half] + y[:, half:]
                    lanes.append(jnp.sum(y.T, axis=0, keepdims=True))
                out_ref[...] = jnp.broadcast_to(jnp.concatenate(lanes, axis=0)[None], out_ref.shape)

    specs = [pl.BlockSpec((tiles, rows, half), lambda g: (g, 0, 0))]
    args = [data]
    if acc is not None:
        specs.append(pl.BlockSpec((n_sens, 2 * half), lambda g: (0, 0)))
        args.append(acc)
    shape = (n_dev, n_sens // 128, 128) if last else (n_sens, 2 * half)
    return pl.pallas_call(
        body,
        grid=(n_tiles // tiles,),
        in_specs=specs,
        out_specs=pl.BlockSpec(shape, lambda g: (0,) * len(shape)),
        scratch_shapes=[pltpu.VMEM((n_sens, 2 * half), F32)],
        out_shape=jax.ShapeDtypeStruct(shape, F32),
        compiler_params=pltpu.CompilerParams(dimension_semantics=("arbitrary",), vmem_limit_bytes=VMEM),
        name="mix_last" if last else "mix_chunk",
    )(*args)


def spread_squares(rows, coef, owner, me, tile_r, tile_c, sb=8):
    nblk, foot = rows.shape
    n_sens = owner.shape[1]

    def body(me_ref, rows_ref, coef_ref, owner_ref, map_ref, pos_ref):
        g = pl.program_id(0)

        @pl.when(g == 0)
        def _():
            mine = owner_ref[...] == me_ref[0]
            flag = jnp.broadcast_to(jnp.where(mine, 1.0, 0.0), (8, n_sens)).astype(BF16)
            row = lax.broadcasted_iota(I32, (n_sens, n_sens), 0)
            col = lax.broadcasted_iota(I32, (n_sens, n_sens), 1)
            before = jnp.where(row < col, 1.0, 0.0).astype(BF16)
            rank = jnp.dot(flag, before, preferred_element_type=F32)[0:1, :]
            pos_ref[...] = jnp.where(mine, rank.astype(I32), -1)

        sub_r = lax.broadcasted_iota(I32, (tile_r, foot), 0)
        sub_c = lax.broadcasted_iota(I32, (tile_c, foot), 0)
        point = rows_ref[...]
        high = point // tile_c
        low = point - high * tile_c
        c = coef_ref[...].astype(F32)
        sq = c * c
        sq_top = sq.astype(BF16).astype(F32)
        sq_rest = sq - sq_top
        for s in range(sb):
            at_r = sub_r == high[s : s + 1, :]
            left = jnp.concatenate(
                [jnp.where(at_r, sq_top[s : s + 1, :], 0.0), jnp.where(at_r, sq_rest[s : s + 1, :], 0.0)], axis=0
            ).astype(BF16)
            right = jnp.where(sub_c == low[s : s + 1, :], 1.0, 0.0).astype(BF16)
            both = lax.dot_general(left, right, (((1,), (1,)), ((), ())), preferred_element_type=F32)
            map_ref[s] = both[:tile_r] + both[tile_r:]

    return pl.pallas_call(
        body,
        grid=(nblk // sb,),
        in_specs=[
            pl.BlockSpec(memory_space=pltpu.SMEM),
            pl.BlockSpec((sb, foot), lambda g: (g, 0)),
            pl.BlockSpec((sb, foot), lambda g: (g, 0)),
            pl.BlockSpec((1, n_sens), lambda g: (0, 0)),
        ],
        out_specs=[
            pl.BlockSpec((sb, tile_r, tile_c), lambda g: (g, 0, 0)),
            pl.BlockSpec((1, n_sens), lambda g: (0, 0)),
        ],
        out_shape=[
            jax.ShapeDtypeStruct((ROOM * nblk, tile_r, tile_c), F32),
            jax.ShapeDtypeStruct((1, n_sens), I32),
        ],
        compiler_params=pltpu.CompilerParams(
            dimension_semantics=("arbitrary",), vmem_limit_bytes=VMEM
        ),
        name="spread_squares",
    )(me, rows, coef, owner)


def finish(parts, weights, sensor, count, maps, pos, scale, sb=32):
    n_sens = pos.shape[1]
    nblk = sensor.shape[0]
    tile_r, tile_c = maps.shape[1:]
    pieces = nblk // sb

    def body(count_ref, parts_ref, weights_ref, sensor_ref, pos_ref, maps_hbm, sens_ref, new_ref, dens_ref, slot_w, maps_ref, sem):
        def fetch(i):
            return pltpu.make_async_copy(maps_hbm.at[pl.ds(i * sb, sb)], maps_ref.at[pl.ds(i * sb, sb)], sem.at[i])

        for i in range(pieces):
            fetch(i).start()
        h8 = jnp.sum(parts_ref[...], axis=0) * scale
        gain = weights_ref[...] * jnp.sqrt(1.0 + h8)
        new8 = n_sens * gain / jnp.sum(gain)
        new_ref[...] = new8
        h, new = (jnp.concatenate([v[i : i + 1] for i in range(n_sens // 128)], axis=1) for v in (h8, new8))
        k = lax.broadcasted_iota(I32, (SPD, n_sens), 0)
        own = jnp.sum(jnp.where(pos_ref[...] == k, h, 0.0), axis=1, keepdims=True)
        diag = lax.broadcasted_iota(I32, (SPD, SPD), 0) == lax.broadcasted_iota(I32, (SPD, SPD), 1)
        sens_ref[...] = jnp.sum(jnp.where(diag, own, 0.0), axis=0, keepdims=True)
        which = lax.broadcasted_iota(I32, (nblk, n_sens), 1)
        w = jnp.sum(jnp.where(which == sensor_ref[...], new, 0.0), axis=1, keepdims=True)
        alive = lax.broadcasted_iota(I32, (nblk, 1), 0) < count_ref[0]
        slot_w[...] = jnp.broadcast_to(jnp.where(alive, w, 0.0), (nblk, tile_c))
        dens_ref[...] = jnp.zeros((tile_r, tile_c), F32)
        for i in range(pieces):
            fetch(i).wait()

            def add(q, c):
                total = dens_ref[...]
                for s in range(8):
                    at = i * sb + q * 8 + s
                    total += slot_w[pl.ds(at, 1), :] * maps_ref[at]
                dens_ref[...] = total
                return c

            lax.fori_loop(0, sb // 8, add, 0)

    vmem = pl.BlockSpec(memory_space=pltpu.VMEM)
    return pl.pallas_call(
        body,
        in_specs=[pl.BlockSpec(memory_space=pltpu.SMEM), vmem, vmem, vmem, vmem, pl.BlockSpec(memory_space=pltpu.HBM)],
        out_specs=[vmem, vmem, vmem],
        out_shape=[
            jax.ShapeDtypeStruct((1, SPD), F32),
            jax.ShapeDtypeStruct((n_sens // 128, 128), F32),
            jax.ShapeDtypeStruct((tile_r, tile_c), F32),
        ],
        scratch_shapes=[
            pltpu.VMEM((nblk, tile_c), F32),
            pltpu.VMEM((nblk, tile_r, tile_c), F32),
            pltpu.SemaphoreType.DMA((pieces,)),
        ],
        compiler_params=pltpu.CompilerParams(vmem_limit_bytes=48 * 1024 * 1024),
        name="finish",
    )(count, parts, weights, sensor, pos, maps)


def exchange(x, axes):
    return lax.all_to_all(x, axes, split_axis=0, concat_axis=0, tiled=True)


def local(probes, blk_rows, blk_sensor, blk_count, coef, owner, weights):
    n_dev = lax.axis_size(AXES)
    core = lax.axis_index("core").astype(I32).reshape(1)
    me = lax.axis_index(AXES).astype(I32).reshape(1)
    tile_r, tile_c, probe_n = probes.shape
    nblk, foot = blk_rows.shape
    n_sens = owner.shape[0]
    flat = probes.reshape(tile_r * tile_c, probe_n)
    tile = (blk_rows, coef, blk_sensor.reshape(1, nblk), blk_count)
    maps, pos = spread_squares(blk_rows, coef, owner.reshape(1, n_sens), me, tile_r, tile_c)
    own, flat = lax.optimization_barrier((gather_rows(flat, *tile, core), flat))
    own = exchange(own, AXES[:2])
    partner = gather_rows(flat, *tile, 1 - core)
    partner = lax.ppermute(partner, AXES[2], [(0, 1), (1, 0)])
    partner = exchange(partner, AXES[:2])
    acc = mix_chunk(own, None, n_sens, n_dev, False)
    partner, maps, pos = lax.optimization_barrier((partner, maps, pos))
    acc = mix_chunk(partner, acc, n_sens, n_dev, True)
    parts = exchange(acc, AXES)
    sens, new, density = finish(
        parts, weights.reshape(n_sens // 128, 128), blk_sensor.reshape(nblk, 1), blk_count, maps, pos, 1.0 / (foot * probe_n)
    )
    return (sens.reshape(SPD), new.reshape(n_sens), density)


def solution(mesh):
    n_gx, n_gy = mesh.devices.shape
    mesh = Mesh(mesh.devices.reshape(n_gx, n_gy // 2, 2), AXES)
    gy = AXES[1:]
    in_specs = (P("gx", gy, None), P(AXES, None), P(AXES), P(AXES), P(AXES, None), P(), P())
    out_specs = (P(AXES), P(), P("gx", gy))
    return jax.shard_map(local, mesh=mesh, in_specs=in_specs, out_specs=out_specs, check_vma=False)
```

```python
import itertools

import jax
import jax.numpy as jnp
from jax import lax
from jax.experimental import pallas as pl
from jax.experimental.pallas import tpu as pltpu
from jax.sharding import Mesh
from jax.sharding import PartitionSpec as P

SPD = 8
AXES = ("y", "x", "z", "core")
ORDERS = (("z", "y", "x"), ("y", "x", "z"), ("x", "z", "y"))
EACH = (5, 5, 6)
PEERS = ((0, 0), (0, 1), (1, 0), (1, 1), (3, 0), (3, 1), (2, 0), (2, 1))
SHIFTS = (0, 1, 3, 2)
SIDE = 8
ROOM = 5
VMEM = 60 * 1024 * 1024
MB = 256
F32 = jnp.float32
BF16 = jnp.bfloat16
I32 = jnp.int32


def member(core_ref, at_ref, shift, flip):
    return ((at_ref[0] + shift) & 3) * 2 + (core_ref[0] + flip) % 2


def gather_flows(probes, rows, coef, sensor, count, core, flows, places):
    n, pn = probes.shape
    nblk, foot = rows.shape
    half = pn // 2
    parts = 8
    step = n // parts
    n_at = len(places)
    n_out = len(flows) * len(PEERS)

    def body(*refs):
        x_hbm, rows_hbm, coef_ref, sensor_ref, count_ref, core_ref = refs[:6]
        at_refs = refs[6 : 6 + n_at]
        outs = refs[6 + n_at : 6 + n_at + n_out]
        idx, idx_v, raw, tab, stage, coef_t, ids, sem, out_sem = refs[6 + n_at + n_out : 6 + n_at + n_out + 9]
        packs = refs[6 + n_at + n_out + 9 :]

        def fetch(i):
            return pltpu.make_async_copy(x_hbm.at[pl.ds(i * step, step), :], raw.at[pl.ds(i * step, step), :], sem.at[i])

        index = pltpu.make_async_copy(rows_hbm, idx_v, sem.at[parts])
        index.start()
        for i in range(parts):
            fetch(i).start()
        index.wait()
        idx_v[...] = idx_v[...] * 2
        doubled = pltpu.make_async_copy(idx_v, idx, sem.at[parts + 1])
        doubled.start()
        alive = lax.broadcasted_iota(I32, (nblk, foot), 0) < count_ref[0]
        coef_t[...] = jnp.where(alive, coef_ref[...].astype(F32), 0.0).T
        high = sensor_ref[...] // MB
        low = sensor_ref[...] - high * MB
        row = lax.broadcasted_iota(I32, (SIDE, nblk), 0)
        ids[...] = jnp.where(row == 1, high, jnp.where(row == 2, low, 0)).astype(F32)
        ch = 512
        for i in range(parts):
            fetch(i).wait()

            def conv(q, c):
                at = i * step + q * ch
                x = raw[pl.ds(at, ch), :].astype(F32)
                tab[pl.ds(at * 2, ch, stride=2), :] = x[:, :half]
                tab[pl.ds(at * 2 + 1, ch, stride=2), :] = x[:, half:]
                return c

            lax.fori_loop(0, step // ch, conv, 0)
        doubled.wait()
        copies = []
        for f, (first, each, axis) in enumerate(flows):
            for p, (shift, flip) in enumerate(PEERS):
                base = first + member(core_ref, at_refs[axis], shift, flip) * each
                pack = packs[f].at[p]

                def channel(i, c):
                    r = base + i
                    for j in range(nblk):
                        at = pl.multiple_of(idx.at[j][r], 2)
                        stage[pl.ds(2 * j, 2), :] = tab[pl.ds(at, 2), :]
                    pack[i, pl.ds(0, nblk), :] = stage[pl.ds(0, nblk, stride=2), :].astype(BF16)
                    pack[i, pl.ds(nblk, nblk), :] = stage[pl.ds(1, nblk, stride=2), :].astype(BF16)
                    tail = jnp.where(row == 0, coef_t[pl.ds(r, 1), :], ids[...])
                    pack[i, pl.ds(2 * nblk, SIDE), :] = tail.astype(BF16)
                    return c

                lax.fori_loop(0, each, channel, 0)
                at = f * len(PEERS) + p
                copies.append(pltpu.make_async_copy(pack, outs[at], out_sem.at[at]))
                copies[-1].start()
        for copy in copies:
            copy.wait()

    hbm = pl.BlockSpec(memory_space=pltpu.HBM)
    smem = pl.BlockSpec(memory_space=pltpu.SMEM)
    vmem = pl.BlockSpec(memory_space=pltpu.VMEM)
    shapes = [(each, 2 * nblk + SIDE, half) for _, each, _ in flows]
    return pl.pallas_call(
        body,
        in_specs=[hbm, hbm, vmem, vmem, smem, smem] + [smem] * n_at,
        out_specs=[hbm] * n_out,
        scratch_shapes=[
            pltpu.SMEM((nblk, foot), I32),
            pltpu.VMEM((nblk, foot), I32),
            pltpu.VMEM((n, pn), BF16),
            pltpu.VMEM((2 * n, half), F32),
            pltpu.VMEM((2 * nblk, half), F32),
            pltpu.VMEM((foot, nblk), F32),
            pltpu.VMEM((SIDE, nblk), F32),
            pltpu.SemaphoreType.DMA((parts + 2,)),
            pltpu.SemaphoreType.DMA((n_out,)),
        ]
        + [pltpu.VMEM((len(PEERS),) + s, BF16) for s in shapes],
        out_shape=[jax.ShapeDtypeStruct(s, BF16) for s in shapes for _ in PEERS],
        compiler_params=pltpu.CompilerParams(vmem_limit_bytes=VMEM),
        name="gather_flows",
    )(probes, rows, coef, sensor, count, core, *places)


def mix_tiles(tiles, at, n_sens):
    each, rows, half = tiles[0].shape
    ns = half
    n = len(tiles)

    def body(at_ref, *refs):
        data, outs = refs[:n], refs[n:]
        x = jnp.concatenate(
            [
                jnp.concatenate([d[0, :ns] for d in data], axis=0),
                jnp.concatenate([d[0, ns : 2 * ns] for d in data], axis=0),
            ],
            axis=1,
        )
        side = [d[0, 2 * ns :].astype(F32) for d in data]
        coef, high, low = (jnp.concatenate([s[i : i + 1] for s in side], axis=1) for i in range(3))
        coef = coef.astype(BF16)
        high = high.astype(I32)
        sub = lax.broadcasted_iota(I32, (MB, n * ns), 0).astype(F32).astype(BF16)
        for out, shift in zip(outs, SHIFTS):
            wanted = jnp.where(high == ((at_ref[0] + shift) & 3), low, -1.0).astype(BF16)
            mixer = jnp.where(sub == wanted, coef, jnp.zeros((), BF16))
            out[0] = jnp.dot(mixer, x, preferred_element_type=F32).astype(BF16)

    shape = (each, n_sens // 4, 2 * half)
    return pl.pallas_call(
        body,
        grid=(each,),
        in_specs=[pl.BlockSpec(memory_space=pltpu.SMEM)] + [pl.BlockSpec((1, rows, half), lambda i: (i, 0, 0))] * n,
        out_specs=[pl.BlockSpec((1,) + shape[1:], lambda i: (i, 0, 0))] * 4,
        out_shape=[jax.ShapeDtypeStruct(shape, BF16)] * 4,
        compiler_params=pltpu.CompilerParams(dimension_semantics=("arbitrary",), vmem_limit_bytes=VMEM),
        name="mix_tiles",
    )(at, *tiles)


def add_quarters(quarters, at):
    each, n_sens, width = quarters[0].shape
    piece = n_sens // 4

    def body(at_ref, *refs):
        for out, shift in zip(refs[4:], SHIFTS):
            rows = pl.ds(pl.multiple_of(((at_ref[0] + shift) & 3) * piece, piece), piece)
            total = refs[0][0, rows, :].astype(F32)
            for r in refs[1:4]:
                total += r[0, rows, :].astype(F32)
            out[0] = total.astype(BF16)

    shape = (each, piece, width)
    return pl.pallas_call(
        body,
        grid=(each,),
        in_specs=[pl.BlockSpec(memory_space=pltpu.SMEM)] + [pl.BlockSpec((1, n_sens, width), lambda i: (i, 0, 0))] * 4,
        out_specs=[pl.BlockSpec((1,) + shape[1:], lambda i: (i, 0, 0))] * 4,
        out_shape=[jax.ShapeDtypeStruct(shape, BF16)] * 4,
        compiler_params=pltpu.CompilerParams(dimension_semantics=("arbitrary",), vmem_limit_bytes=VMEM),
        name="add_quarters",
    )(at, *quarters)


def square_sums(flows, n_dev):
    n = len(flows)
    piece = flows[0][0].shape[1]

    def body(*refs):
        out = refs[-1]
        lanes = []
        for f in range(n):
            four = refs[4 * f : 4 * f + 4]
            total = jnp.zeros((piece, 128), F32)
            for i in range(four[0].shape[0]):
                y = four[0][i].astype(F32) + four[1][i].astype(F32) + four[2][i].astype(F32) + four[3][i].astype(F32)
                y = y * y
                total += y[:, :128] + y[:, 128:]
            total = jnp.concatenate([total, jnp.zeros((128 - piece, 128), F32)], axis=0)
            lanes.append(jnp.sum(total.T, axis=0, keepdims=True))
        out[...] = jnp.broadcast_to(jnp.concatenate(lanes, axis=1)[None], out.shape)

    return pl.pallas_call(
        body,
        out_shape=jax.ShapeDtypeStruct((n_dev, 1, 128 * n), F32),
        compiler_params=pltpu.CompilerParams(vmem_limit_bytes=VMEM),
        name="square_sums",
    )(*[x for four in flows for x in four])


def spread_squares(rows, coef, owner, me, tile_r, tile_c, sb=8):
    nblk, foot = rows.shape
    n_sens = owner.shape[1]

    def body(me_ref, rows_ref, coef_ref, owner_ref, map_ref, pos_ref):
        g = pl.program_id(0)

        @pl.when(g == 0)
        def _():
            mine = owner_ref[...] == me_ref[0]
            flag = jnp.broadcast_to(jnp.where(mine, 1.0, 0.0), (8, n_sens)).astype(BF16)
            row = lax.broadcasted_iota(I32, (n_sens, n_sens), 0)
            col = lax.broadcasted_iota(I32, (n_sens, n_sens), 1)
            before = jnp.where(row < col, 1.0, 0.0).astype(BF16)
            rank = jnp.dot(flag, before, preferred_element_type=F32)[0:1, :]
            pos_ref[...] = jnp.where(mine, rank.astype(I32), -1)

        sub_r = lax.broadcasted_iota(I32, (tile_r, foot), 0)
        sub_c = lax.broadcasted_iota(I32, (tile_c, foot), 0)
        point = rows_ref[...]
        high = point // tile_c
        low = point - high * tile_c
        c = coef_ref[...].astype(F32)
        sq = c * c
        sq_top = sq.astype(BF16).astype(F32)
        sq_rest = sq - sq_top
        for s in range(sb):
            at_r = sub_r == high[s : s + 1, :]
            left = jnp.concatenate(
                [jnp.where(at_r, sq_top[s : s + 1, :], 0.0), jnp.where(at_r, sq_rest[s : s + 1, :], 0.0)], axis=0
            ).astype(BF16)
            right = jnp.where(sub_c == low[s : s + 1, :], 1.0, 0.0).astype(BF16)
            both = lax.dot_general(left, right, (((1,), (1,)), ((), ())), preferred_element_type=F32)
            map_ref[s] = both[:tile_r] + both[tile_r:]

    return pl.pallas_call(
        body,
        grid=(nblk // sb,),
        in_specs=[
            pl.BlockSpec(memory_space=pltpu.SMEM),
            pl.BlockSpec((sb, foot), lambda g: (g, 0)),
            pl.BlockSpec((sb, foot), lambda g: (g, 0)),
            pl.BlockSpec((1, n_sens), lambda g: (0, 0)),
        ],
        out_specs=[
            pl.BlockSpec((sb, tile_r, tile_c), lambda g: (g, 0, 0)),
            pl.BlockSpec((1, n_sens), lambda g: (0, 0)),
        ],
        out_shape=[
            jax.ShapeDtypeStruct((ROOM * nblk, tile_r, tile_c), F32),
            jax.ShapeDtypeStruct((1, n_sens), I32),
        ],
        compiler_params=pltpu.CompilerParams(
            dimension_semantics=("arbitrary",), vmem_limit_bytes=VMEM
        ),
        name="spread_squares",
    )(me, rows, coef, owner)


def finish(parts, weights, sensor, count, maps, pos, scale, sb=32):
    n_sens = pos.shape[1]
    nblk = sensor.shape[0]
    tile_r, tile_c = maps.shape[1:]
    pieces = nblk // sb

    def body(count_ref, parts_ref, weights_ref, sensor_ref, pos_ref, maps_hbm, sens_ref, new_ref, dens_ref, slot_w, maps_ref, sem):
        def fetch(i):
            return pltpu.make_async_copy(maps_hbm.at[pl.ds(i * sb, sb)], maps_ref.at[pl.ds(i * sb, sb)], sem.at[i])

        for i in range(pieces):
            fetch(i).start()
        col = lax.broadcasted_iota(I32, (8, 128), 1)
        place = {"y": col // 32, "x": col // 8 % 4, "z": col // 2 % 4}
        want = lax.broadcasted_iota(I32, (8, 128), 0) * 2
        pair = [jnp.zeros((8, 128), F32), jnp.zeros((8, 128), F32)]
        for f, (_, b, c) in enumerate(ORDERS):
            group = place[b] * 4 + place[c]
            sums = parts_ref[:, 0, pl.ds(128 * f, 128)]
            for odd in range(2):
                pick = jnp.where(group == want + odd, 1.0, 0.0)
                pair[odd] += jnp.dot(pick, sums, precision=lax.Precision.HIGHEST, preferred_element_type=F32)
        h8 = (pair[0] + pltpu.roll(pair[1], 64, 1)) * scale
        gain = weights_ref[...] * jnp.sqrt(1.0 + h8)
        new8 = n_sens * gain / jnp.sum(gain)
        new_ref[...] = new8
        h, new = (jnp.concatenate([v[i : i + 1] for i in range(n_sens // 128)], axis=1) for v in (h8, new8))
        k = lax.broadcasted_iota(I32, (SPD, n_sens), 0)
        own = jnp.sum(jnp.where(pos_ref[...] == k, h, 0.0), axis=1, keepdims=True)
        diag = lax.broadcasted_iota(I32, (SPD, SPD), 0) == lax.broadcasted_iota(I32, (SPD, SPD), 1)
        sens_ref[...] = jnp.sum(jnp.where(diag, own, 0.0), axis=0, keepdims=True)
        which = lax.broadcasted_iota(I32, (nblk, n_sens), 1)
        w = jnp.sum(jnp.where(which == sensor_ref[...], new, 0.0), axis=1, keepdims=True)
        alive = lax.broadcasted_iota(I32, (nblk, 1), 0) < count_ref[0]
        slot_w[...] = jnp.broadcast_to(jnp.where(alive, w, 0.0), (nblk, tile_c))
        dens_ref[...] = jnp.zeros((tile_r, tile_c), F32)
        for i in range(pieces):
            fetch(i).wait()

            def add(q, c):
                total = dens_ref[...]
                for s in range(8):
                    at = i * sb + q * 8 + s
                    total += slot_w[pl.ds(at, 1), :] * maps_ref[at]
                dens_ref[...] = total
                return c

            lax.fori_loop(0, sb // 8, add, 0)

    vmem = pl.BlockSpec(memory_space=pltpu.VMEM)
    return pl.pallas_call(
        body,
        in_specs=[pl.BlockSpec(memory_space=pltpu.SMEM), vmem, vmem, vmem, vmem, pl.BlockSpec(memory_space=pltpu.HBM)],
        out_specs=[vmem, vmem, vmem],
        out_shape=[
            jax.ShapeDtypeStruct((1, SPD), F32),
            jax.ShapeDtypeStruct((n_sens // 128, 128), F32),
            jax.ShapeDtypeStruct((tile_r, tile_c), F32),
        ],
        scratch_shapes=[
            pltpu.VMEM((nblk, tile_c), F32),
            pltpu.VMEM((nblk, tile_r, tile_c), F32),
            pltpu.SemaphoreType.DMA((pieces,)),
        ],
        compiler_params=pltpu.CompilerParams(vmem_limit_bytes=48 * 1024 * 1024),
        name="finish",
    )(count, parts, weights, sensor, pos, maps)


def exchange(x, axes):
    return lax.all_to_all(x, axes, split_axis=0, concat_axis=0, tiled=True)


def shift_to(x, axis, shift, flip):
    if not shift and not flip:
        return x
    sizes = [lax.axis_size(a) for a in AXES]
    where = AXES.index(axis)
    pairs = []
    for i, place in enumerate(itertools.product(*map(range, sizes))):
        to = list(place)
        to[where] = (to[where] + shift) % sizes[where]
        to[3] = (to[3] + flip) % 2
        j = 0
        for p, size in zip(to, sizes):
            j = j * size + p
        pairs.append((i, j))
    return lax.ppermute(x, AXES, pairs)


def local(probes, blk_rows, blk_sensor, blk_count, coef, owner, weights):
    n_dev = lax.axis_size(AXES)
    core = lax.axis_index("core").astype(I32).reshape(1)
    me = lax.axis_index(AXES).astype(I32).reshape(1)
    at = {axis: lax.axis_index(axis).astype(I32).reshape(1) for axis in AXES[:3]}
    tile_r, tile_c, probe_n = probes.shape
    nblk, foot = blk_rows.shape
    n_sens = owner.shape[0]
    flat = probes.reshape(tile_r * tile_c, probe_n)
    tile = (blk_rows, coef, blk_sensor.reshape(1, nblk), blk_count, core)
    maps, pos = spread_squares(blk_rows, coef, owner.reshape(1, n_sens), me, tile_r, tile_c)
    firsts = [8 * sum(EACH[:f]) for f in range(3)]
    sent = gather_flows(flat, *tile, [(firsts[0], EACH[0], 0)], [at["z"]])
    *sent, flat = lax.optimization_barrier((*sent, flat))
    more = gather_flows(flat, *tile, [(firsts[1], EACH[1], 0), (firsts[2], EACH[2], 1)], [at["y"], at["x"]])
    sent = (sent, more[:8], more[8:])
    tiles = [[shift_to(x, a, *peer) for x, peer in zip(sent[f], PEERS)] for f, (a, _, _) in enumerate(ORDERS)]
    flows = []
    for f, (_, b, c) in enumerate(ORDERS):
        quarters = mix_tiles(tiles[f], at[b], n_sens)
        quarters = [shift_to(x, b, s, 0) for x, s in zip(quarters, SHIFTS)]
        pieces = add_quarters(quarters, at[c])
        flows.append([shift_to(x, c, s, 0) for x, s in zip(pieces, SHIFTS)])
    (flows, maps, pos) = lax.optimization_barrier((flows, maps, pos))
    acc = square_sums(flows, n_dev)
    parts = exchange(acc, AXES)
    sens, new, density = finish(
        parts, weights.reshape(n_sens // 128, 128), blk_sensor.reshape(nblk, 1), blk_count, maps, pos, 1.0 / (foot * probe_n)
    )
    return (sens.reshape(SPD), new.reshape(n_sens), density)


def solution(mesh):
    mesh = Mesh(mesh.devices.reshape(4, 4, 4, 2), AXES)
    gx, gy = AXES[:2], AXES[2:]
    in_specs = (P(gx, gy, None), P(AXES, None), P(AXES), P(AXES), P(AXES, None), P(), P())
    out_specs = (P(AXES), P(), P(gx, gy))
    return jax.shard_map(local, mesh=mesh, in_specs=in_specs, out_specs=out_specs, check_vma=False)
```

```python
import itertools

import jax
import jax.numpy as jnp
from jax import lax
from jax.experimental import pallas as pl
from jax.experimental.pallas import tpu as pltpu
from jax.sharding import Mesh
from jax.sharding import PartitionSpec as P

SPD = 8
AXES = ("y", "x", "z", "core")
ORDERS = (("z", "y", "x"), ("y", "x", "z"), ("x", "z", "y"))
EACH = (5, 5, 6)
PEERS = ((0, 0), (0, 1), (1, 0), (1, 1), (3, 0), (3, 1), (2, 0), (2, 1))
SHIFTS = (0, 1, 3, 2)
SIDE = 8
ROOM = 5
VMEM = 60 * 1024 * 1024
MB = 256
F32 = jnp.float32
BF16 = jnp.bfloat16
I32 = jnp.int32


def member(core_ref, at_ref, shift, flip):
    return ((at_ref[0] + shift) & 3) * 2 + (core_ref[0] + flip) % 2


def gather_flows(probes, rows, coef, sensor, count, core, flows, places):
    n, pn = probes.shape
    nblk, foot = rows.shape
    half = pn // 2
    parts = 8
    step = n // parts
    n_at = len(places)
    n_out = len(flows) * len(PEERS)

    def body(*refs):
        x_hbm, rows_hbm, coef_ref, sensor_ref, count_ref, core_ref = refs[:6]
        at_refs = refs[6 : 6 + n_at]
        outs = refs[6 + n_at : 6 + n_at + n_out]
        idx, idx_v, raw, tab, stage, coef_t, ids, sem, out_sem = refs[6 + n_at + n_out : 6 + n_at + n_out + 9]
        packs = refs[6 + n_at + n_out + 9 :]

        def fetch(i):
            return pltpu.make_async_copy(x_hbm.at[pl.ds(i * step, step), :], raw.at[pl.ds(i * step, step), :], sem.at[i])

        index = pltpu.make_async_copy(rows_hbm, idx_v, sem.at[parts])
        index.start()
        for i in range(parts):
            fetch(i).start()
        index.wait()
        idx_v[...] = idx_v[...] * 2
        doubled = pltpu.make_async_copy(idx_v, idx, sem.at[parts + 1])
        doubled.start()
        alive = lax.broadcasted_iota(I32, (nblk, foot), 0) < count_ref[0]
        coef_t[...] = jnp.where(alive, coef_ref[...].astype(F32), 0.0).T
        high = sensor_ref[...] // MB
        low = sensor_ref[...] - high * MB
        row = lax.broadcasted_iota(I32, (SIDE, nblk), 0)
        ids[...] = jnp.where(row == 1, high, jnp.where(row == 2, low, 0)).astype(F32)
        ch = 512
        for i in range(parts):
            fetch(i).wait()

            def conv(q, c):
                at = i * step + q * ch
                x = raw[pl.ds(at, ch), :].astype(F32)
                tab[pl.ds(at * 2, ch, stride=2), :] = x[:, :half]
                tab[pl.ds(at * 2 + 1, ch, stride=2), :] = x[:, half:]
                return c

            lax.fori_loop(0, step // ch, conv, 0)
        doubled.wait()
        copies = []
        for f, (first, each, axis) in enumerate(flows):
            for p, (shift, flip) in enumerate(PEERS):
                base = first + member(core_ref, at_refs[axis], shift, flip) * each
                pack = packs[f].at[p]

                def channel(i, c):
                    r = base + i
                    for j in range(nblk):
                        at = pl.multiple_of(idx.at[j][r], 2)
                        stage[pl.ds(2 * j, 2), :] = tab[pl.ds(at, 2), :]
                    pack[i, pl.ds(0, nblk), :] = stage[pl.ds(0, nblk, stride=2), :].astype(BF16)
                    pack[i, pl.ds(nblk, nblk), :] = stage[pl.ds(1, nblk, stride=2), :].astype(BF16)
                    tail = jnp.where(row == 0, coef_t[pl.ds(r, 1), :], ids[...])
                    pack[i, pl.ds(2 * nblk, SIDE), :] = tail.astype(BF16)
                    return c

                lax.fori_loop(0, each, channel, 0)
                at = f * len(PEERS) + p
                copies.append(pltpu.make_async_copy(pack, outs[at], out_sem.at[at]))
                copies[-1].start()
        for copy in copies:
            copy.wait()

    hbm = pl.BlockSpec(memory_space=pltpu.HBM)
    smem = pl.BlockSpec(memory_space=pltpu.SMEM)
    vmem = pl.BlockSpec(memory_space=pltpu.VMEM)
    shapes = [(each, 2 * nblk + SIDE, half) for _, each, _ in flows]
    return pl.pallas_call(
        body,
        in_specs=[hbm, hbm, vmem, vmem, smem, smem] + [smem] * n_at,
        out_specs=[hbm] * n_out,
        scratch_shapes=[
            pltpu.SMEM((nblk, foot), I32),
            pltpu.VMEM((nblk, foot), I32),
            pltpu.VMEM((n, pn), BF16),
            pltpu.VMEM((2 * n, half), F32),
            pltpu.VMEM((2 * nblk, half), F32),
            pltpu.VMEM((foot, nblk), F32),
            pltpu.VMEM((SIDE, nblk), F32),
            pltpu.SemaphoreType.DMA((parts + 2,)),
            pltpu.SemaphoreType.DMA((n_out,)),
        ]
        + [pltpu.VMEM((len(PEERS),) + s, BF16) for s in shapes],
        out_shape=[jax.ShapeDtypeStruct(s, BF16) for s in shapes for _ in PEERS],
        compiler_params=pltpu.CompilerParams(vmem_limit_bytes=VMEM),
        name="gather_flows",
    )(probes, rows, coef, sensor, count, core, *places)


def mix_tiles(tiles, at, n_sens):
    each, rows, half = tiles[0].shape
    ns = half
    n = len(tiles)

    def body(at_ref, *refs):
        data, outs = refs[:n], refs[n:]
        x = jnp.concatenate(
            [
                jnp.concatenate([d[0, :ns] for d in data], axis=0),
                jnp.concatenate([d[0, ns : 2 * ns] for d in data], axis=0),
            ],
            axis=1,
        )
        side = [d[0, 2 * ns :].astype(F32) for d in data]
        coef, high, low = (jnp.concatenate([s[i : i + 1] for s in side], axis=1) for i in range(3))
        coef = coef.astype(BF16)
        high = high.astype(I32)
        sub = lax.broadcasted_iota(I32, (MB, n * ns), 0).astype(F32).astype(BF16)
        for out, shift in zip(outs, SHIFTS):
            wanted = jnp.where(high == ((at_ref[0] + shift) & 3), low, -1.0).astype(BF16)
            mixer = jnp.where(sub == wanted, coef, jnp.zeros((), BF16))
            out[0] = jnp.dot(mixer, x, preferred_element_type=F32).astype(BF16)

    shape = (each, n_sens // 4, 2 * half)
    return pl.pallas_call(
        body,
        grid=(each,),
        in_specs=[pl.BlockSpec(memory_space=pltpu.SMEM)] + [pl.BlockSpec((1, rows, half), lambda i: (i, 0, 0))] * n,
        out_specs=[pl.BlockSpec((1,) + shape[1:], lambda i: (i, 0, 0))] * 4,
        out_shape=[jax.ShapeDtypeStruct(shape, BF16)] * 4,
        compiler_params=pltpu.CompilerParams(dimension_semantics=("arbitrary",), vmem_limit_bytes=24 * 1024 * 1024),
        name="mix_tiles",
    )(at, *tiles)


def add_quarters(quarters, at):
    each, n_sens, width = quarters[0].shape
    piece = n_sens // 4

    def body(at_ref, *refs):
        for out, shift in zip(refs[4:], SHIFTS):
            rows = pl.ds(pl.multiple_of(((at_ref[0] + shift) & 3) * piece, piece), piece)

            def channel(i, c):
                total = refs[0][i, rows, :].astype(F32)
                for r in refs[1:4]:
                    total += r[i, rows, :].astype(F32)
                out[i] = total.astype(BF16)
                return c

            lax.fori_loop(0, each, channel, 0)

    shape = (each, piece, width)
    vmem = pl.BlockSpec(memory_space=pltpu.VMEM)
    return pl.pallas_call(
        body,
        in_specs=[pl.BlockSpec(memory_space=pltpu.SMEM)] + [vmem] * 4,
        out_specs=[vmem] * 4,
        out_shape=[jax.ShapeDtypeStruct(shape, BF16)] * 4,
        compiler_params=pltpu.CompilerParams(vmem_limit_bytes=24 * 1024 * 1024),
        name="add_quarters",
    )(at, *quarters)


def square_sums(flows, n_dev):
    n = len(flows)
    piece = flows[0][0].shape[1]

    def body(*refs):
        out = refs[-1]
        lanes = []
        for f in range(n):
            four = refs[4 * f : 4 * f + 4]
            total = jnp.zeros((piece, 128), F32)
            for i in range(four[0].shape[0]):
                y = four[0][i].astype(F32) + four[1][i].astype(F32) + four[2][i].astype(F32) + four[3][i].astype(F32)
                y = y * y
                total += y[:, :128] + y[:, 128:]
            total = jnp.concatenate([total, jnp.zeros((128 - piece, 128), F32)], axis=0)
            lanes.append(jnp.sum(total.T, axis=0, keepdims=True))
        out[...] = jnp.broadcast_to(jnp.concatenate(lanes, axis=1)[None], out.shape)

    return pl.pallas_call(
        body,
        out_shape=jax.ShapeDtypeStruct((n_dev, 1, 128 * n), F32),
        compiler_params=pltpu.CompilerParams(vmem_limit_bytes=24 * 1024 * 1024),
        name="square_sums",
    )(*[x for four in flows for x in four])


def spread_squares(rows, coef, owner, me, tile_r, tile_c, sb=8):
    nblk, foot = rows.shape
    n_sens = owner.shape[1]

    def body(me_ref, rows_ref, coef_ref, owner_ref, map_ref, pos_ref):
        g = pl.program_id(0)

        @pl.when(g == 0)
        def _():
            mine = owner_ref[...] == me_ref[0]
            flag = jnp.broadcast_to(jnp.where(mine, 1.0, 0.0), (8, n_sens)).astype(BF16)
            row = lax.broadcasted_iota(I32, (n_sens, n_sens), 0)
            col = lax.broadcasted_iota(I32, (n_sens, n_sens), 1)
            before = jnp.where(row < col, 1.0, 0.0).astype(BF16)
            rank = jnp.dot(flag, before, preferred_element_type=F32)[0:1, :]
            pos_ref[...] = jnp.where(mine, rank.astype(I32), -1)

        sub_r = lax.broadcasted_iota(I32, (tile_r, foot), 0)
        sub_c = lax.broadcasted_iota(I32, (tile_c, foot), 0)
        point = rows_ref[...]
        high = point // tile_c
        low = point - high * tile_c
        c = coef_ref[...].astype(F32)
        sq = c * c
        sq_top = sq.astype(BF16).astype(F32)
        sq_rest = sq - sq_top
        for s in range(sb):
            at_r = sub_r == high[s : s + 1, :]
            left = jnp.concatenate(
                [jnp.where(at_r, sq_top[s : s + 1, :], 0.0), jnp.where(at_r, sq_rest[s : s + 1, :], 0.0)], axis=0
            ).astype(BF16)
            right = jnp.where(sub_c == low[s : s + 1, :], 1.0, 0.0).astype(BF16)
            both = lax.dot_general(left, right, (((1,), (1,)), ((), ())), preferred_element_type=F32)
            map_ref[s] = both[:tile_r] + both[tile_r:]

    return pl.pallas_call(
        body,
        grid=(nblk // sb,),
        in_specs=[
            pl.BlockSpec(memory_space=pltpu.SMEM),
            pl.BlockSpec((sb, foot), lambda g: (g, 0)),
            pl.BlockSpec((sb, foot), lambda g: (g, 0)),
            pl.BlockSpec((1, n_sens), lambda g: (0, 0)),
        ],
        out_specs=[
            pl.BlockSpec((sb, tile_r, tile_c), lambda g: (g, 0, 0)),
            pl.BlockSpec((1, n_sens), lambda g: (0, 0)),
        ],
        out_shape=[
            jax.ShapeDtypeStruct((ROOM * nblk, tile_r, tile_c), F32),
            jax.ShapeDtypeStruct((1, n_sens), I32),
        ],
        compiler_params=pltpu.CompilerParams(
            dimension_semantics=("arbitrary",), vmem_limit_bytes=VMEM
        ),
        name="spread_squares",
    )(me, rows, coef, owner)


def finish(parts, weights, sensor, count, maps, pos, scale, sb=32):
    n_sens = pos.shape[1]
    nblk = sensor.shape[0]
    tile_r, tile_c = maps.shape[1:]
    pieces = nblk // sb

    def body(count_ref, parts_ref, weights_ref, sensor_ref, pos_ref, maps_hbm, sens_ref, new_ref, dens_ref, slot_w, maps_ref, sem):
        def fetch(i):
            return pltpu.make_async_copy(maps_hbm.at[pl.ds(i * sb, sb)], maps_ref.at[pl.ds(i * sb, sb)], sem.at[i])

        for i in range(pieces):
            fetch(i).start()
        col = lax.broadcasted_iota(I32, (8, 128), 1)
        place = {"y": col // 32, "x": col // 8 % 4, "z": col // 2 % 4}
        want = lax.broadcasted_iota(I32, (8, 128), 0) * 2
        pair = [jnp.zeros((8, 128), F32), jnp.zeros((8, 128), F32)]
        for f, (_, b, c) in enumerate(ORDERS):
            group = place[b] * 4 + place[c]
            sums = parts_ref[:, 0, pl.ds(128 * f, 128)]
            for odd in range(2):
                pick = jnp.where(group == want + odd, 1.0, 0.0)
                pair[odd] += jnp.dot(pick, sums, precision=lax.Precision.HIGHEST, preferred_element_type=F32)
        h8 = (pair[0] + pltpu.roll(pair[1], 64, 1)) * scale
        gain = weights_ref[...] * jnp.sqrt(1.0 + h8)
        new8 = n_sens * gain / jnp.sum(gain)
        new_ref[...] = new8
        h, new = (jnp.concatenate([v[i : i + 1] for i in range(n_sens // 128)], axis=1) for v in (h8, new8))
        k = lax.broadcasted_iota(I32, (SPD, n_sens), 0)
        own = jnp.sum(jnp.where(pos_ref[...] == k, h, 0.0), axis=1, keepdims=True)
        diag = lax.broadcasted_iota(I32, (SPD, SPD), 0) == lax.broadcasted_iota(I32, (SPD, SPD), 1)
        sens_ref[...] = jnp.sum(jnp.where(diag, own, 0.0), axis=0, keepdims=True)
        which = lax.broadcasted_iota(I32, (nblk, n_sens), 1)
        w = jnp.sum(jnp.where(which == sensor_ref[...], new, 0.0), axis=1, keepdims=True)
        alive = lax.broadcasted_iota(I32, (nblk, 1), 0) < count_ref[0]
        slot_w[...] = jnp.broadcast_to(jnp.where(alive, w, 0.0), (nblk, tile_c))
        dens_ref[...] = jnp.zeros((tile_r, tile_c), F32)
        for i in range(pieces):
            fetch(i).wait()

            def add(q, c):
                total = dens_ref[...]
                for s in range(8):
                    at = i * sb + q * 8 + s
                    total += slot_w[pl.ds(at, 1), :] * maps_ref[at]
                dens_ref[...] = total
                return c

            lax.fori_loop(0, sb // 8, add, 0)

    vmem = pl.BlockSpec(memory_space=pltpu.VMEM)
    return pl.pallas_call(
        body,
        in_specs=[pl.BlockSpec(memory_space=pltpu.SMEM), vmem, vmem, vmem, vmem, pl.BlockSpec(memory_space=pltpu.HBM)],
        out_specs=[vmem, vmem, vmem],
        out_shape=[
            jax.ShapeDtypeStruct((1, SPD), F32),
            jax.ShapeDtypeStruct((n_sens // 128, 128), F32),
            jax.ShapeDtypeStruct((tile_r, tile_c), F32),
        ],
        scratch_shapes=[
            pltpu.VMEM((nblk, tile_c), F32),
            pltpu.VMEM((nblk, tile_r, tile_c), F32),
            pltpu.SemaphoreType.DMA((pieces,)),
        ],
        compiler_params=pltpu.CompilerParams(vmem_limit_bytes=48 * 1024 * 1024),
        name="finish",
    )(count, parts, weights, sensor, pos, maps)


def exchange(x, axes):
    return lax.all_to_all(x, axes, split_axis=0, concat_axis=0, tiled=True)


def shift_to(x, axis, shift, flip):
    if not shift and not flip:
        return x
    sizes = [lax.axis_size(a) for a in AXES]
    where = AXES.index(axis)
    pairs = []
    for i, place in enumerate(itertools.product(*map(range, sizes))):
        to = list(place)
        to[where] = (to[where] + shift) % sizes[where]
        to[3] = (to[3] + flip) % 2
        j = 0
        for p, size in zip(to, sizes):
            j = j * size + p
        pairs.append((i, j))
    return lax.ppermute(x, AXES, pairs)


def local(probes, blk_rows, blk_sensor, blk_count, coef, owner, weights):
    n_dev = lax.axis_size(AXES)
    core = lax.axis_index("core").astype(I32).reshape(1)
    me = lax.axis_index(AXES).astype(I32).reshape(1)
    at = {axis: lax.axis_index(axis).astype(I32).reshape(1) for axis in AXES[:3]}
    tile_r, tile_c, probe_n = probes.shape
    nblk, foot = blk_rows.shape
    n_sens = owner.shape[0]
    flat = probes.reshape(tile_r * tile_c, probe_n)
    tile = (blk_rows, coef, blk_sensor.reshape(1, nblk), blk_count, core)
    firsts = [8 * sum(EACH[:f]) for f in range(3)]
    packs = [(first, each, f) for f, (first, each) in enumerate(zip(firsts, EACH))]
    sent = gather_flows(flat, *tile, packs, [at[a] for a, _, _ in ORDERS])
    maps, pos = spread_squares(blk_rows, coef, owner.reshape(1, n_sens), me, tile_r, tile_c)
    tiles = []
    for f, (a, _, _) in enumerate(ORDERS):
        tiles.append([shift_to(x, a, *peer) for x, peer in zip(sent[8 * f : 8 * f + 8], PEERS)])
    flows = []
    for f, (_, b, c) in enumerate(ORDERS):
        quarters = mix_tiles(tiles[f], at[b], n_sens)
        quarters = [shift_to(x, b, s, 0) for x, s in zip(quarters, SHIFTS)]
        pieces = add_quarters(quarters, at[c])
        flows.append([shift_to(x, c, s, 0) for x, s in zip(pieces, SHIFTS)])
    (flows, maps, pos) = lax.optimization_barrier((flows, maps, pos))
    acc = square_sums(flows, n_dev)
    parts = exchange(acc, AXES)
    sens, new, density = finish(
        parts, weights.reshape(n_sens // 128, 128), blk_sensor.reshape(nblk, 1), blk_count, maps, pos, 1.0 / (foot * probe_n)
    )
    return (sens.reshape(SPD), new.reshape(n_sens), density)


def solution(mesh):
    mesh = Mesh(mesh.devices.reshape(4, 4, 4, 2), AXES)
    gx, gy = AXES[:2], AXES[2:]
    in_specs = (P(gx, gy, None), P(AXES, None), P(AXES), P(AXES), P(AXES, None), P(), P())
    out_specs = (P(AXES), P(), P(gx, gy))
    return jax.shard_map(local, mesh=mesh, in_specs=in_specs, out_specs=out_specs, check_vma=False)
```

```python
import itertools

import jax
import jax.numpy as jnp
from jax import lax
from jax.experimental import pallas as pl
from jax.experimental.pallas import tpu as pltpu
from jax.sharding import Mesh
from jax.sharding import PartitionSpec as P

SPD = 8
AXES = ("y", "x", "z", "core")
ORDERS = (("z", "y", "x"), ("y", "x", "z"), ("x", "z", "y"))
EACH = (4, 6, 6)
PEERS = ((0, 0), (0, 1), (1, 0), (1, 1), (3, 0), (3, 1), (2, 0), (2, 1))
SHIFTS = (0, 1, 3, 2)
SIDE = 8
ROOM = 5
VMEM = 60 * 1024 * 1024
MB = 256
F32 = jnp.float32
BF16 = jnp.bfloat16
I32 = jnp.int32


def member(core_ref, at_ref, shift, flip):
    return ((at_ref[0] + shift) & 3) * 2 + (core_ref[0] + flip) % 2


def gather_flows(probes, rows, coef, sensor, count, core, flows, places):
    n, pn = probes.shape
    nblk, foot = rows.shape
    half = pn // 2
    parts = 8
    step = n // parts
    n_at = len(places)
    n_out = len(flows) * len(PEERS)

    def body(*refs):
        x_hbm, rows_hbm, coef_ref, sensor_ref, count_ref, core_ref = refs[:6]
        at_refs = refs[6 : 6 + n_at]
        outs = refs[6 + n_at : 6 + n_at + n_out]
        idx, idx_v, raw, tab, stage, coef_t, ids, sem, out_sem = refs[6 + n_at + n_out : 6 + n_at + n_out + 9]
        packs = refs[6 + n_at + n_out + 9 :]

        def fetch(i):
            return pltpu.make_async_copy(x_hbm.at[pl.ds(i * step, step), :], raw.at[pl.ds(i * step, step), :], sem.at[i])

        index = pltpu.make_async_copy(rows_hbm, idx_v, sem.at[parts])
        index.start()
        for i in range(parts):
            fetch(i).start()
        index.wait()
        idx_v[...] = idx_v[...] * 2
        doubled = pltpu.make_async_copy(idx_v, idx, sem.at[parts + 1])
        doubled.start()
        alive = lax.broadcasted_iota(I32, (nblk, foot), 0) < count_ref[0]
        coef_t[...] = jnp.where(alive, coef_ref[...].astype(F32), 0.0).T
        high = sensor_ref[...] // MB
        low = sensor_ref[...] - high * MB
        row = lax.broadcasted_iota(I32, (SIDE, nblk), 0)
        ids[...] = jnp.where(row == 1, high, jnp.where(row == 2, low, 0)).astype(F32)
        ch = 512
        for i in range(parts):
            fetch(i).wait()

            def conv(q, c):
                at = i * step + q * ch
                x = raw[pl.ds(at, ch), :].astype(F32)
                tab[pl.ds(at * 2, ch, stride=2), :] = x[:, :half]
                tab[pl.ds(at * 2 + 1, ch, stride=2), :] = x[:, half:]
                return c

            lax.fori_loop(0, step // ch, conv, 0)
        doubled.wait()
        copies = []
        for f, (first, each, axis) in enumerate(flows):
            for p, (shift, flip) in enumerate(PEERS):
                base = first + member(core_ref, at_refs[axis], shift, flip) * each
                pack = packs[f].at[p]

                def channel(i, c):
                    r = base + i
                    for j in range(nblk):
                        at = pl.multiple_of(idx.at[j][r], 2)
                        stage[pl.ds(2 * j, 2), :] = tab[pl.ds(at, 2), :]
                    pack[i, pl.ds(0, nblk), :] = stage[pl.ds(0, nblk, stride=2), :].astype(BF16)
                    pack[i, pl.ds(nblk, nblk), :] = stage[pl.ds(1, nblk, stride=2), :].astype(BF16)
                    tail = jnp.where(row == 0, coef_t[pl.ds(r, 1), :], ids[...])
                    pack[i, pl.ds(2 * nblk, SIDE), :] = tail.astype(BF16)
                    return c

                lax.fori_loop(0, each, channel, 0)
                at = f * len(PEERS) + p
                copies.append(pltpu.make_async_copy(pack, outs[at], out_sem.at[at]))
                copies[-1].start()
        for copy in copies:
            copy.wait()

    hbm = pl.BlockSpec(memory_space=pltpu.HBM)
    smem = pl.BlockSpec(memory_space=pltpu.SMEM)
    vmem = pl.BlockSpec(memory_space=pltpu.VMEM)
    shapes = [(each, 2 * nblk + SIDE, half) for _, each, _ in flows]
    return pl.pallas_call(
        body,
        in_specs=[hbm, hbm, vmem, vmem, smem, smem] + [smem] * n_at,
        out_specs=[hbm] * n_out,
        scratch_shapes=[
            pltpu.SMEM((nblk, foot), I32),
            pltpu.VMEM((nblk, foot), I32),
            pltpu.VMEM((n, pn), BF16),
            pltpu.VMEM((2 * n, half), F32),
            pltpu.VMEM((2 * nblk, half), F32),
            pltpu.VMEM((foot, nblk), F32),
            pltpu.VMEM((SIDE, nblk), F32),
            pltpu.SemaphoreType.DMA((parts + 2,)),
            pltpu.SemaphoreType.DMA((n_out,)),
        ]
        + [pltpu.VMEM((len(PEERS),) + s, BF16) for s in shapes],
        out_shape=[jax.ShapeDtypeStruct(s, BF16) for s in shapes for _ in PEERS],
        compiler_params=pltpu.CompilerParams(vmem_limit_bytes=VMEM),
        name="gather_flows",
    )(probes, rows, coef, sensor, count, core, *places)


def mix_tiles(tiles, at, n_sens):
    each, rows, half = tiles[0].shape
    ns = half
    n = len(tiles)

    def body(at_ref, *refs):
        data, outs = refs[:n], refs[n:]
        x = jnp.concatenate(
            [
                jnp.concatenate([d[0, :ns] for d in data], axis=0),
                jnp.concatenate([d[0, ns : 2 * ns] for d in data], axis=0),
            ],
            axis=1,
        )
        side = [d[0, 2 * ns :].astype(F32) for d in data]
        coef, high, low = (jnp.concatenate([s[i : i + 1] for s in side], axis=1) for i in range(3))
        coef = coef.astype(BF16)
        high = high.astype(I32)
        sub = lax.broadcasted_iota(I32, (MB, n * ns), 0).astype(F32).astype(BF16)
        for out, shift in zip(outs, SHIFTS):
            wanted = jnp.where(high == ((at_ref[0] + shift) & 3), low, -1.0).astype(BF16)
            mixer = jnp.where(sub == wanted, coef, jnp.zeros((), BF16))
            out[0] = jnp.dot(mixer, x, preferred_element_type=F32).astype(BF16)

    shape = (each, n_sens // 4, 2 * half)
    return pl.pallas_call(
        body,
        grid=(each,),
        in_specs=[pl.BlockSpec(memory_space=pltpu.SMEM)] + [pl.BlockSpec((1, rows, half), lambda i: (i, 0, 0))] * n,
        out_specs=[pl.BlockSpec((1,) + shape[1:], lambda i: (i, 0, 0))] * 4,
        out_shape=[jax.ShapeDtypeStruct(shape, BF16)] * 4,
        compiler_params=pltpu.CompilerParams(dimension_semantics=("arbitrary",), vmem_limit_bytes=24 * 1024 * 1024),
        name="mix_tiles",
    )(at, *tiles)


def add_quarters(quarters, at):
    each, n_sens, width = quarters[0].shape
    piece = n_sens // 4

    def body(at_ref, *refs):
        for out, shift in zip(refs[4:], SHIFTS):
            rows = pl.ds(pl.multiple_of(((at_ref[0] + shift) & 3) * piece, piece), piece)

            def channel(i, c):
                total = refs[0][i, rows, :].astype(F32)
                for r in refs[1:4]:
                    total += r[i, rows, :].astype(F32)
                out[i] = total.astype(BF16)
                return c

            lax.fori_loop(0, each, channel, 0)

    shape = (each, piece, width)
    vmem = pl.BlockSpec(memory_space=pltpu.VMEM)
    return pl.pallas_call(
        body,
        in_specs=[pl.BlockSpec(memory_space=pltpu.SMEM)] + [vmem] * 4,
        out_specs=[vmem] * 4,
        out_shape=[jax.ShapeDtypeStruct(shape, BF16)] * 4,
        compiler_params=pltpu.CompilerParams(vmem_limit_bytes=24 * 1024 * 1024),
        name="add_quarters",
    )(at, *quarters)


def square_sums(flows, n_dev):
    n = len(flows)
    piece = flows[0][0].shape[1]

    def body(*refs):
        out = refs[-1]
        lanes = []
        for f in range(n):
            four = refs[4 * f : 4 * f + 4]
            total = jnp.zeros((piece, 128), F32)
            for i in range(four[0].shape[0]):
                y = four[0][i].astype(F32) + four[1][i].astype(F32) + four[2][i].astype(F32) + four[3][i].astype(F32)
                y = y * y
                total += y[:, :128] + y[:, 128:]
            total = jnp.concatenate([total, jnp.zeros((128 - piece, 128), F32)], axis=0)
            lanes.append(jnp.sum(total.T, axis=0, keepdims=True))
        out[...] = jnp.broadcast_to(jnp.concatenate(lanes, axis=1)[None], out.shape)

    return pl.pallas_call(
        body,
        out_shape=jax.ShapeDtypeStruct((n_dev, 1, 128 * n), F32),
        compiler_params=pltpu.CompilerParams(vmem_limit_bytes=24 * 1024 * 1024),
        name="square_sums",
    )(*[x for four in flows for x in four])


def spread_squares(rows, coef, owner, me, tile_r, tile_c, sb=8):
    nblk, foot = rows.shape
    n_sens = owner.shape[1]

    def body(me_ref, rows_ref, coef_ref, owner_ref, map_ref, pos_ref):
        g = pl.program_id(0)

        @pl.when(g == 0)
        def _():
            mine = owner_ref[...] == me_ref[0]
            flag = jnp.broadcast_to(jnp.where(mine, 1.0, 0.0), (8, n_sens)).astype(BF16)
            row = lax.broadcasted_iota(I32, (n_sens, n_sens), 0)
            col = lax.broadcasted_iota(I32, (n_sens, n_sens), 1)
            before = jnp.where(row < col, 1.0, 0.0).astype(BF16)
            rank = jnp.dot(flag, before, preferred_element_type=F32)[0:1, :]
            pos_ref[...] = jnp.where(mine, rank.astype(I32), -1)

        sub_r = lax.broadcasted_iota(I32, (tile_r, foot), 0)
        sub_c = lax.broadcasted_iota(I32, (tile_c, foot), 0)
        point = rows_ref[...]
        high = point // tile_c
        low = point - high * tile_c
        c = coef_ref[...].astype(F32)
        sq = c * c
        sq_top = sq.astype(BF16).astype(F32)
        sq_rest = sq - sq_top
        for s in range(sb):
            at_r = sub_r == high[s : s + 1, :]
            left = jnp.concatenate(
                [jnp.where(at_r, sq_top[s : s + 1, :], 0.0), jnp.where(at_r, sq_rest[s : s + 1, :], 0.0)], axis=0
            ).astype(BF16)
            right = jnp.where(sub_c == low[s : s + 1, :], 1.0, 0.0).astype(BF16)
            both = lax.dot_general(left, right, (((1,), (1,)), ((), ())), preferred_element_type=F32)
            map_ref[s] = both[:tile_r] + both[tile_r:]

    return pl.pallas_call(
        body,
        grid=(nblk // sb,),
        in_specs=[
            pl.BlockSpec(memory_space=pltpu.SMEM),
            pl.BlockSpec((sb, foot), lambda g: (g, 0)),
            pl.BlockSpec((sb, foot), lambda g: (g, 0)),
            pl.BlockSpec((1, n_sens), lambda g: (0, 0)),
        ],
        out_specs=[
            pl.BlockSpec((sb, tile_r, tile_c), lambda g: (g, 0, 0)),
            pl.BlockSpec((1, n_sens), lambda g: (0, 0)),
        ],
        out_shape=[
            jax.ShapeDtypeStruct((ROOM * nblk, tile_r, tile_c), F32),
            jax.ShapeDtypeStruct((1, n_sens), I32),
        ],
        compiler_params=pltpu.CompilerParams(
            dimension_semantics=("arbitrary",), vmem_limit_bytes=VMEM
        ),
        name="spread_squares",
    )(me, rows, coef, owner)


def finish(parts, weights, sensor, count, maps, pos, scale, sb=32):
    n_sens = pos.shape[1]
    nblk = sensor.shape[0]
    tile_r, tile_c = maps.shape[1:]
    pieces = nblk // sb

    def body(count_ref, parts_ref, weights_ref, sensor_ref, pos_ref, maps_hbm, sens_ref, new_ref, dens_ref, slot_w, maps_ref, sem):
        def fetch(i):
            return pltpu.make_async_copy(maps_hbm.at[pl.ds(i * sb, sb)], maps_ref.at[pl.ds(i * sb, sb)], sem.at[i])

        for i in range(pieces):
            fetch(i).start()
        col = lax.broadcasted_iota(I32, (8, 128), 1)
        place = {"y": col // 32, "x": col // 8 % 4, "z": col // 2 % 4}
        want = lax.broadcasted_iota(I32, (8, 128), 0) * 2
        pair = [jnp.zeros((8, 128), F32), jnp.zeros((8, 128), F32)]
        for f, (_, b, c) in enumerate(ORDERS):
            group = place[b] * 4 + place[c]
            sums = parts_ref[:, 0, pl.ds(128 * f, 128)]
            for odd in range(2):
                pick = jnp.where(group == want + odd, 1.0, 0.0)
                pair[odd] += jnp.dot(pick, sums, precision=lax.Precision.HIGHEST, preferred_element_type=F32)
        h8 = (pair[0] + pltpu.roll(pair[1], 64, 1)) * scale
        gain = weights_ref[...] * jnp.sqrt(1.0 + h8)
        new8 = n_sens * gain / jnp.sum(gain)
        new_ref[...] = new8
        h, new = (jnp.concatenate([v[i : i + 1] for i in range(n_sens // 128)], axis=1) for v in (h8, new8))
        k = lax.broadcasted_iota(I32, (SPD, n_sens), 0)
        own = jnp.sum(jnp.where(pos_ref[...] == k, h, 0.0), axis=1, keepdims=True)
        diag = lax.broadcasted_iota(I32, (SPD, SPD), 0) == lax.broadcasted_iota(I32, (SPD, SPD), 1)
        sens_ref[...] = jnp.sum(jnp.where(diag, own, 0.0), axis=0, keepdims=True)
        which = lax.broadcasted_iota(I32, (nblk, n_sens), 1)
        w = jnp.sum(jnp.where(which == sensor_ref[...], new, 0.0), axis=1, keepdims=True)
        alive = lax.broadcasted_iota(I32, (nblk, 1), 0) < count_ref[0]
        slot_w[...] = jnp.broadcast_to(jnp.where(alive, w, 0.0), (nblk, tile_c))
        dens_ref[...] = jnp.zeros((tile_r, tile_c), F32)
        for i in range(pieces):
            fetch(i).wait()

            def add(q, c):
                total = dens_ref[...]
                for s in range(8):
                    at = i * sb + q * 8 + s
                    total += slot_w[pl.ds(at, 1), :] * maps_ref[at]
                dens_ref[...] = total
                return c

            lax.fori_loop(0, sb // 8, add, 0)

    vmem = pl.BlockSpec(memory_space=pltpu.VMEM)
    return pl.pallas_call(
        body,
        in_specs=[pl.BlockSpec(memory_space=pltpu.SMEM), vmem, vmem, vmem, vmem, pl.BlockSpec(memory_space=pltpu.HBM)],
        out_specs=[vmem, vmem, vmem],
        out_shape=[
            jax.ShapeDtypeStruct((1, SPD), F32),
            jax.ShapeDtypeStruct((n_sens // 128, 128), F32),
            jax.ShapeDtypeStruct((tile_r, tile_c), F32),
        ],
        scratch_shapes=[
            pltpu.VMEM((nblk, tile_c), F32),
            pltpu.VMEM((nblk, tile_r, tile_c), F32),
            pltpu.SemaphoreType.DMA((pieces,)),
        ],
        compiler_params=pltpu.CompilerParams(vmem_limit_bytes=48 * 1024 * 1024),
        name="finish",
    )(count, parts, weights, sensor, pos, maps)


def exchange(x, axes):
    return lax.all_to_all(x, axes, split_axis=0, concat_axis=0, tiled=True)


def shift_to(x, axis, shift, flip):
    if not shift and not flip:
        return x
    sizes = [lax.axis_size(a) for a in AXES]
    where = AXES.index(axis)
    pairs = []
    for i, place in enumerate(itertools.product(*map(range, sizes))):
        to = list(place)
        to[where] = (to[where] + shift) % sizes[where]
        to[3] = (to[3] + flip) % 2
        j = 0
        for p, size in zip(to, sizes):
            j = j * size + p
        pairs.append((i, j))
    return lax.ppermute(x, AXES, pairs)


def local(probes, blk_rows, blk_sensor, blk_count, coef, owner, weights):
    n_dev = lax.axis_size(AXES)
    core = lax.axis_index("core").astype(I32).reshape(1)
    me = lax.axis_index(AXES).astype(I32).reshape(1)
    at = {axis: lax.axis_index(axis).astype(I32).reshape(1) for axis in AXES[:3]}
    tile_r, tile_c, probe_n = probes.shape
    nblk, foot = blk_rows.shape
    n_sens = owner.shape[0]
    flat = probes.reshape(tile_r * tile_c, probe_n)
    tile = (blk_rows, coef, blk_sensor.reshape(1, nblk), blk_count, core)
    firsts = [8 * sum(EACH[:f]) for f in range(3)]
    tiles = [None] * 3
    flows = [None] * 3
    maps, pos = spread_squares(blk_rows, coef, owner.reshape(1, n_sens), me, tile_r, tile_c)
    for group in ((2,), (0, 1)):
        packs = [(firsts[f], EACH[f], i) for i, f in enumerate(group)]
        sent = gather_flows(flat, *tile, packs, [at[ORDERS[f][0]] for f in group])
        for i, f in enumerate(group):
            tiles[f] = [shift_to(x, ORDERS[f][0], *peer) for x, peer in zip(sent[8 * i : 8 * i + 8], PEERS)]
    for f, (_, b, c) in enumerate(ORDERS):
        quarters = mix_tiles(tiles[f], at[b], n_sens)
        quarters = [shift_to(x, b, s, 0) for x, s in zip(quarters, SHIFTS)]
        pieces = add_quarters(quarters, at[c])
        flows[f] = [shift_to(x, c, s, 0) for x, s in zip(pieces, SHIFTS)]
    (flows, maps, pos) = lax.optimization_barrier((flows, maps, pos))
    acc = square_sums(flows, n_dev)
    parts = exchange(acc, AXES)
    sens, new, density = finish(
        parts, weights.reshape(n_sens // 128, 128), blk_sensor.reshape(nblk, 1), blk_count, maps, pos, 1.0 / (foot * probe_n)
    )
    return (sens.reshape(SPD), new.reshape(n_sens), density)


def solution(mesh):
    mesh = Mesh(mesh.devices.reshape(4, 4, 4, 2), AXES)
    gx, gy = AXES[:2], AXES[2:]
    in_specs = (P(gx, gy, None), P(AXES, None), P(AXES), P(AXES), P(AXES, None), P(), P())
    out_specs = (P(AXES), P(), P(gx, gy))
    return jax.shard_map(local, mesh=mesh, in_specs=in_specs, out_specs=out_specs, check_vma=False)
```

```python
import itertools

import jax
import jax.numpy as jnp
from jax import lax
from jax.experimental import pallas as pl
from jax.experimental.pallas import tpu as pltpu
from jax.sharding import Mesh
from jax.sharding import PartitionSpec as P

SPD = 8
AXES = ("y", "x", "z", "core")
ORDERS = (("z", "y", "x"), ("y", "x", "z"), ("x", "z", "y"))
EACH = (5, 5, 6)
PEERS = ((0, 0), (0, 1), (1, 0), (1, 1), (3, 0), (3, 1), (2, 0), (2, 1))
SHIFTS = (0, 1, 3, 2)
SIDE = 8
ROOM = 5
VMEM = 60 * 1024 * 1024
MB = 256
F32 = jnp.float32
BF16 = jnp.bfloat16
I32 = jnp.int32


def member(core_ref, at_ref, shift, flip):
    return ((at_ref[0] + shift) & 3) * 2 + (core_ref[0] + flip) % 2


def gather_flows(probes, rows, coef, sensor, count, core, flows, places):
    n, pn = probes.shape
    nblk, foot = rows.shape
    half = pn // 2
    parts = 8
    step = n // parts
    n_at = len(places)
    n_out = sum(1 if axis is None else len(PEERS) for _, _, axis in flows)
    n_copy = len(flows) * len(PEERS)

    def body(*refs):
        x_hbm, rows_hbm, coef_ref, sensor_ref, count_ref, core_ref = refs[:6]
        at_refs = refs[6 : 6 + n_at]
        outs = refs[6 + n_at : 6 + n_at + n_out]
        idx, idx_v, raw, tab, stage, coef_t, ids, sem, out_sem = refs[6 + n_at + n_out : 6 + n_at + n_out + 9]
        packs = refs[6 + n_at + n_out + 9 :]

        def fetch(i):
            return pltpu.make_async_copy(x_hbm.at[pl.ds(i * step, step), :], raw.at[pl.ds(i * step, step), :], sem.at[i])

        index = pltpu.make_async_copy(rows_hbm, idx_v, sem.at[parts])
        index.start()
        for i in range(parts):
            fetch(i).start()
        index.wait()
        idx_v[...] = idx_v[...] * 2
        doubled = pltpu.make_async_copy(idx_v, idx, sem.at[parts + 1])
        doubled.start()
        alive = lax.broadcasted_iota(I32, (nblk, foot), 0) < count_ref[0]
        coef_t[...] = jnp.where(alive, coef_ref[...].astype(F32), 0.0).T
        high = sensor_ref[...] // MB
        low = sensor_ref[...] - high * MB
        row = lax.broadcasted_iota(I32, (SIDE, nblk), 0)
        ids[...] = jnp.where(row == 1, high, jnp.where(row == 2, low, 0)).astype(F32)
        ch = 512
        for i in range(parts):
            fetch(i).wait()

            def conv(q, c):
                at = i * step + q * ch
                x = raw[pl.ds(at, ch), :].astype(F32)
                tab[pl.ds(at * 2, ch, stride=2), :] = x[:, :half]
                tab[pl.ds(at * 2 + 1, ch, stride=2), :] = x[:, half:]
                return c

            lax.fori_loop(0, step // ch, conv, 0)
        doubled.wait()
        copies = []
        free = list(outs)
        for f, (first, each, axis) in enumerate(flows):
            taken = [free.pop(0) for _ in range(1 if axis is None else len(PEERS))]
            for p, (shift, flip) in enumerate(PEERS):
                if axis is None:
                    base, to = first + p * each, taken[0].at[p]
                else:
                    base, to = first + member(core_ref, at_refs[axis], shift, flip) * each, taken[p]
                pack = packs[f].at[p]

                def channel(i, c):
                    r = base + i
                    for j in range(nblk):
                        at = pl.multiple_of(idx.at[j][r], 2)
                        stage[pl.ds(2 * j, 2), :] = tab[pl.ds(at, 2), :]
                    pack[i, pl.ds(0, nblk), :] = stage[pl.ds(0, nblk, stride=2), :].astype(BF16)
                    pack[i, pl.ds(nblk, nblk), :] = stage[pl.ds(1, nblk, stride=2), :].astype(BF16)
                    tail = jnp.where(row == 0, coef_t[pl.ds(r, 1), :], ids[...])
                    pack[i, pl.ds(2 * nblk, SIDE), :] = tail.astype(BF16)
                    return c

                lax.fori_loop(0, each, channel, 0)
                copies.append(pltpu.make_async_copy(pack, to, out_sem.at[len(copies)]))
                copies[-1].start()
        for copy in copies:
            copy.wait()

    hbm = pl.BlockSpec(memory_space=pltpu.HBM)
    smem = pl.BlockSpec(memory_space=pltpu.SMEM)
    vmem = pl.BlockSpec(memory_space=pltpu.VMEM)
    shapes = [(each, 2 * nblk + SIDE, half) for _, each, _ in flows]
    return pl.pallas_call(
        body,
        in_specs=[hbm, hbm, vmem, vmem, smem, smem] + [smem] * n_at,
        out_specs=[hbm] * n_out,
        scratch_shapes=[
            pltpu.SMEM((nblk, foot), I32),
            pltpu.VMEM((nblk, foot), I32),
            pltpu.VMEM((n, pn), BF16),
            pltpu.VMEM((2 * n, half), F32),
            pltpu.VMEM((2 * nblk, half), F32),
            pltpu.VMEM((foot, nblk), F32),
            pltpu.VMEM((SIDE, nblk), F32),
            pltpu.SemaphoreType.DMA((parts + 2,)),
            pltpu.SemaphoreType.DMA((n_copy,)),
        ]
        + [pltpu.VMEM((len(PEERS),) + s, BF16) for s in shapes],
        out_shape=[
            jax.ShapeDtypeStruct(s, BF16)
            for shape, (_, _, axis) in zip(shapes, flows)
            for s in ([(len(PEERS),) + shape] if axis is None else [shape] * len(PEERS))
        ],
        compiler_params=pltpu.CompilerParams(vmem_limit_bytes=VMEM),
        name="gather_flows",
    )(probes, rows, coef, sensor, count, core, *places)


def mix_tiles(tiles, at, n_sens):
    each, rows, half = tiles[0].shape
    ns = half
    n = len(tiles)

    def body(at_ref, *refs):
        data, outs = refs[:n], refs[n:]
        x = jnp.concatenate(
            [
                jnp.concatenate([d[0, :ns] for d in data], axis=0),
                jnp.concatenate([d[0, ns : 2 * ns] for d in data], axis=0),
            ],
            axis=1,
        )
        side = [d[0, 2 * ns :].astype(F32) for d in data]
        coef, high, low = (jnp.concatenate([s[i : i + 1] for s in side], axis=1) for i in range(3))
        coef = coef.astype(BF16)
        high = high.astype(I32)
        sub = lax.broadcasted_iota(I32, (MB, n * ns), 0).astype(F32).astype(BF16)
        for out, shift in zip(outs, SHIFTS):
            wanted = jnp.where(high == ((at_ref[0] + shift) & 3), low, -1.0).astype(BF16)
            mixer = jnp.where(sub == wanted, coef, jnp.zeros((), BF16))
            out[0] = jnp.dot(mixer, x, preferred_element_type=F32).astype(BF16)

    shape = (each, n_sens // 4, 2 * half)
    return pl.pallas_call(
        body,
        grid=(each,),
        in_specs=[pl.BlockSpec(memory_space=pltpu.SMEM)] + [pl.BlockSpec((1, rows, half), lambda i: (i, 0, 0))] * n,
        out_specs=[pl.BlockSpec((1,) + shape[1:], lambda i: (i, 0, 0))] * 4,
        out_shape=[jax.ShapeDtypeStruct(shape, BF16)] * 4,
        compiler_params=pltpu.CompilerParams(dimension_semantics=("arbitrary",), vmem_limit_bytes=24 * 1024 * 1024),
        name="mix_tiles",
    )(at, *tiles)


def mix_members(tiles, n_sens):
    n, each, rows, half = tiles.shape
    ns = half

    def body(data, out):
        x = jnp.concatenate(
            [
                jnp.concatenate([data[t, 0, :ns] for t in range(n)], axis=0),
                jnp.concatenate([data[t, 0, ns : 2 * ns] for t in range(n)], axis=0),
            ],
            axis=1,
        )
        side = [data[t, 0, 2 * ns :].astype(F32) for t in range(n)]
        coef, high, low = (jnp.concatenate([s[i : i + 1] for s in side], axis=1) for i in range(3))
        coef = coef.astype(BF16)
        sub = lax.broadcasted_iota(I32, (MB, n * ns), 0).astype(F32).astype(BF16)
        for q in range(4):
            wanted = jnp.where(high == q, low, -1.0).astype(BF16)
            mixer = jnp.where(sub == wanted, coef, jnp.zeros((), BF16))
            out[q, 0] = jnp.dot(mixer, x, preferred_element_type=F32).astype(BF16)

    shape = (4, each, n_sens // 4, 2 * half)
    return pl.pallas_call(
        body,
        grid=(each,),
        in_specs=[pl.BlockSpec((n, 1, rows, half), lambda i: (0, i, 0, 0))],
        out_specs=pl.BlockSpec((4, 1) + shape[2:], lambda i: (0, i, 0, 0)),
        out_shape=jax.ShapeDtypeStruct(shape, BF16),
        compiler_params=pltpu.CompilerParams(
            dimension_semantics=("arbitrary",), vmem_limit_bytes=24 * 1024 * 1024
        ),
        name="mix_members",
    )(tiles)


def add_members(quarters):
    n, each, n_sens, width = quarters.shape
    piece = n_sens // 4

    def body(data, out):
        def channel(i, c):
            total = data[0, i].astype(F32)
            for t in range(1, n):
                total += data[t, i].astype(F32)
            total = total.astype(BF16)
            for q in range(4):
                out[q, i] = total[q * piece : (q + 1) * piece]
            return c

        lax.fori_loop(0, each, channel, 0)

    vmem = pl.BlockSpec(memory_space=pltpu.VMEM)
    return pl.pallas_call(
        body,
        in_specs=[vmem],
        out_specs=vmem,
        out_shape=jax.ShapeDtypeStruct((4, each, piece, width), BF16),
        compiler_params=pltpu.CompilerParams(vmem_limit_bytes=24 * 1024 * 1024),
        name="add_members",
    )(quarters)


def add_quarters(quarters, at):
    each, n_sens, width = quarters[0].shape
    piece = n_sens // 4

    def body(at_ref, *refs):
        for out, shift in zip(refs[4:], SHIFTS):
            rows = pl.ds(pl.multiple_of(((at_ref[0] + shift) & 3) * piece, piece), piece)

            def channel(i, c):
                total = refs[0][i, rows, :].astype(F32)
                for r in refs[1:4]:
                    total += r[i, rows, :].astype(F32)
                out[i] = total.astype(BF16)
                return c

            lax.fori_loop(0, each, channel, 0)

    shape = (each, piece, width)
    vmem = pl.BlockSpec(memory_space=pltpu.VMEM)
    return pl.pallas_call(
        body,
        in_specs=[pl.BlockSpec(memory_space=pltpu.SMEM)] + [vmem] * 4,
        out_specs=[vmem] * 4,
        out_shape=[jax.ShapeDtypeStruct(shape, BF16)] * 4,
        compiler_params=pltpu.CompilerParams(vmem_limit_bytes=24 * 1024 * 1024),
        name="add_quarters",
    )(at, *quarters)


def square_sums(flows, n_dev):
    counts = [len(four) if isinstance(four, list) else 1 for four in flows]
    args = [x for four in flows for x in (four if isinstance(four, list) else [four])]
    piece = args[0].shape[-2]

    def body(*refs):
        out = refs[-1]
        free = list(refs[:-1])
        lanes = []
        for count in counts:
            four = [free.pop(0) for _ in range(count)]
            if count == 1:
                four = [four[0].at[t] for t in range(4)]
            total = jnp.zeros((piece, 128), F32)
            for i in range(four[0].shape[0]):
                y = four[0][i].astype(F32) + four[1][i].astype(F32) + four[2][i].astype(F32) + four[3][i].astype(F32)
                y = y * y
                total += y[:, :128] + y[:, 128:]
            total = jnp.concatenate([total, jnp.zeros((128 - piece, 128), F32)], axis=0)
            lanes.append(jnp.sum(total.T, axis=0, keepdims=True))
        out[...] = jnp.broadcast_to(jnp.concatenate(lanes, axis=1)[None], out.shape)

    return pl.pallas_call(
        body,
        out_shape=jax.ShapeDtypeStruct((n_dev, 1, 128 * len(flows)), F32),
        compiler_params=pltpu.CompilerParams(vmem_limit_bytes=24 * 1024 * 1024),
        name="square_sums",
    )(*args)


def spread_squares(rows, coef, owner, me, tile_r, tile_c, sb=8):
    nblk, foot = rows.shape
    n_sens = owner.shape[1]

    def body(me_ref, rows_ref, coef_ref, owner_ref, map_ref, pos_ref):
        g = pl.program_id(0)

        @pl.when(g == 0)
        def _():
            mine = owner_ref[...] == me_ref[0]
            flag = jnp.broadcast_to(jnp.where(mine, 1.0, 0.0), (8, n_sens)).astype(BF16)
            row = lax.broadcasted_iota(I32, (n_sens, n_sens), 0)
            col = lax.broadcasted_iota(I32, (n_sens, n_sens), 1)
            before = jnp.where(row < col, 1.0, 0.0).astype(BF16)
            rank = jnp.dot(flag, before, preferred_element_type=F32)[0:1, :]
            pos_ref[...] = jnp.where(mine, rank.astype(I32), -1)

        sub_r = lax.broadcasted_iota(I32, (tile_r, foot), 0)
        sub_c = lax.broadcasted_iota(I32, (tile_c, foot), 0)
        point = rows_ref[...]
        high = point // tile_c
        low = point - high * tile_c
        c = coef_ref[...].astype(F32)
        sq = c * c
        sq_top = sq.astype(BF16).astype(F32)
        sq_rest = sq - sq_top
        for s in range(sb):
            at_r = sub_r == high[s : s + 1, :]
            left = jnp.concatenate(
                [jnp.where(at_r, sq_top[s : s + 1, :], 0.0), jnp.where(at_r, sq_rest[s : s + 1, :], 0.0)], axis=0
            ).astype(BF16)
            right = jnp.where(sub_c == low[s : s + 1, :], 1.0, 0.0).astype(BF16)
            both = lax.dot_general(left, right, (((1,), (1,)), ((), ())), preferred_element_type=F32)
            map_ref[s] = both[:tile_r] + both[tile_r:]

    return pl.pallas_call(
        body,
        grid=(nblk // sb,),
        in_specs=[
            pl.BlockSpec(memory_space=pltpu.SMEM),
            pl.BlockSpec((sb, foot), lambda g: (g, 0)),
            pl.BlockSpec((sb, foot), lambda g: (g, 0)),
            pl.BlockSpec((1, n_sens), lambda g: (0, 0)),
        ],
        out_specs=[
            pl.BlockSpec((sb, tile_r, tile_c), lambda g: (g, 0, 0)),
            pl.BlockSpec((1, n_sens), lambda g: (0, 0)),
        ],
        out_shape=[
            jax.ShapeDtypeStruct((ROOM * nblk, tile_r, tile_c), F32),
            jax.ShapeDtypeStruct((1, n_sens), I32),
        ],
        compiler_params=pltpu.CompilerParams(
            dimension_semantics=("arbitrary",), vmem_limit_bytes=VMEM
        ),
        name="spread_squares",
    )(me, rows, coef, owner)


def finish(parts, weights, sensor, count, maps, pos, scale, sb=32):
    n_sens = pos.shape[1]
    nblk = sensor.shape[0]
    tile_r, tile_c = maps.shape[1:]
    pieces = nblk // sb

    def body(count_ref, parts_ref, weights_ref, sensor_ref, pos_ref, maps_hbm, sens_ref, new_ref, dens_ref, slot_w, maps_ref, sem):
        def fetch(i):
            return pltpu.make_async_copy(maps_hbm.at[pl.ds(i * sb, sb)], maps_ref.at[pl.ds(i * sb, sb)], sem.at[i])

        for i in range(pieces):
            fetch(i).start()
        col = lax.broadcasted_iota(I32, (8, 128), 1)
        place = {"y": col // 32, "x": col // 8 % 4, "z": col // 2 % 4}
        want = lax.broadcasted_iota(I32, (8, 128), 0) * 2
        pair = [jnp.zeros((8, 128), F32), jnp.zeros((8, 128), F32)]
        for f, (_, b, c) in enumerate(ORDERS):
            group = place[b] * 4 + place[c]
            sums = parts_ref[:, 0, pl.ds(128 * f, 128)]
            for odd in range(2):
                pick = jnp.where(group == want + odd, 1.0, 0.0)
                pair[odd] += jnp.dot(pick, sums, precision=lax.Precision.HIGHEST, preferred_element_type=F32)
        h8 = (pair[0] + pltpu.roll(pair[1], 64, 1)) * scale
        gain = weights_ref[...] * jnp.sqrt(1.0 + h8)
        new8 = n_sens * gain / jnp.sum(gain)
        new_ref[...] = new8
        h, new = (jnp.concatenate([v[i : i + 1] for i in range(n_sens // 128)], axis=1) for v in (h8, new8))
        k = lax.broadcasted_iota(I32, (SPD, n_sens), 0)
        own = jnp.sum(jnp.where(pos_ref[...] == k, h, 0.0), axis=1, keepdims=True)
        diag = lax.broadcasted_iota(I32, (SPD, SPD), 0) == lax.broadcasted_iota(I32, (SPD, SPD), 1)
        sens_ref[...] = jnp.sum(jnp.where(diag, own, 0.0), axis=0, keepdims=True)
        which = lax.broadcasted_iota(I32, (nblk, n_sens), 1)
        w = jnp.sum(jnp.where(which == sensor_ref[...], new, 0.0), axis=1, keepdims=True)
        alive = lax.broadcasted_iota(I32, (nblk, 1), 0) < count_ref[0]
        slot_w[...] = jnp.broadcast_to(jnp.where(alive, w, 0.0), (nblk, tile_c))
        dens_ref[...] = jnp.zeros((tile_r, tile_c), F32)
        for i in range(pieces):
            fetch(i).wait()

            def add(q, c):
                total = dens_ref[...]
                for s in range(8):
                    at = i * sb + q * 8 + s
                    total += slot_w[pl.ds(at, 1), :] * maps_ref[at]
                dens_ref[...] = total
                return c

            lax.fori_loop(0, sb // 8, add, 0)

    vmem = pl.BlockSpec(memory_space=pltpu.VMEM)
    return pl.pallas_call(
        body,
        in_specs=[pl.BlockSpec(memory_space=pltpu.SMEM), vmem, vmem, vmem, vmem, pl.BlockSpec(memory_space=pltpu.HBM)],
        out_specs=[vmem, vmem, vmem],
        out_shape=[
            jax.ShapeDtypeStruct((1, SPD), F32),
            jax.ShapeDtypeStruct((n_sens // 128, 128), F32),
            jax.ShapeDtypeStruct((tile_r, tile_c), F32),
        ],
        scratch_shapes=[
            pltpu.VMEM((nblk, tile_c), F32),
            pltpu.VMEM((nblk, tile_r, tile_c), F32),
            pltpu.SemaphoreType.DMA((pieces,)),
        ],
        compiler_params=pltpu.CompilerParams(vmem_limit_bytes=48 * 1024 * 1024),
        name="finish",
    )(count, parts, weights, sensor, pos, maps)


def exchange(x, axes):
    return lax.all_to_all(x, axes, split_axis=0, concat_axis=0, tiled=True)


def shift_to(x, axis, shift, flip):
    if not shift and not flip:
        return x
    sizes = [lax.axis_size(a) for a in AXES]
    where = AXES.index(axis)
    pairs = []
    for i, place in enumerate(itertools.product(*map(range, sizes))):
        to = list(place)
        to[where] = (to[where] + shift) % sizes[where]
        to[3] = (to[3] + flip) % 2
        j = 0
        for p, size in zip(to, sizes):
            j = j * size + p
        pairs.append((i, j))
    return lax.ppermute(x, AXES, pairs)


def local(probes, blk_rows, blk_sensor, blk_count, coef, owner, weights):
    n_dev = lax.axis_size(AXES)
    core = lax.axis_index("core").astype(I32).reshape(1)
    me = lax.axis_index(AXES).astype(I32).reshape(1)
    at = {axis: lax.axis_index(axis).astype(I32).reshape(1) for axis in AXES[:3]}
    tile_r, tile_c, probe_n = probes.shape
    nblk, foot = blk_rows.shape
    n_sens = owner.shape[0]
    flat = probes.reshape(tile_r * tile_c, probe_n)
    tile = (blk_rows, coef, blk_sensor.reshape(1, nblk), blk_count, core)
    firsts = [8 * sum(EACH[:f]) for f in range(3)]
    tiles = [None] * 3
    flows = [None] * 3
    packs = [(firsts[f], EACH[f], i) for i, f in enumerate((2, 1))] + [(firsts[0], EACH[0], None)]
    sent = gather_flows(flat, *tile, packs, [at[ORDERS[f][0]] for f in (2, 1)])
    maps, pos = spread_squares(blk_rows, coef, owner.reshape(1, n_sens), me, tile_r, tile_c)
    for f, (a, b, c) in enumerate(ORDERS):
        if f == 0:
            tiles = exchange(sent[-1], (a, "core"))
            quarters = mix_members(tiles, n_sens)
            quarters = exchange(quarters, b)
            pieces = add_members(quarters)
            flows[f] = exchange(pieces, c)
            continue
        tiles = [shift_to(x, a, *peer) for x, peer in zip(sent[8 * (2 - f) :], PEERS)]
        quarters = mix_tiles(tiles, at[b], n_sens)
        quarters = [shift_to(x, b, s, 0) for x, s in zip(quarters, SHIFTS)]
        pieces = add_quarters(quarters, at[c])
        flows[f] = [shift_to(x, c, s, 0) for x, s in zip(pieces, SHIFTS)]
    (flows, maps, pos) = lax.optimization_barrier((flows, maps, pos))
    acc = square_sums(flows, n_dev)
    parts = exchange(acc, AXES)
    sens, new, density = finish(
        parts, weights.reshape(n_sens // 128, 128), blk_sensor.reshape(nblk, 1), blk_count, maps, pos, 1.0 / (foot * probe_n)
    )
    return (sens.reshape(SPD), new.reshape(n_sens), density)


def solution(mesh):
    mesh = Mesh(mesh.devices.reshape(4, 4, 4, 2), AXES)
    gx, gy = AXES[:2], AXES[2:]
    in_specs = (P(gx, gy, None), P(AXES, None), P(AXES), P(AXES), P(AXES, None), P(), P())
    out_specs = (P(AXES), P(), P(gx, gy))
    return jax.shard_map(local, mesh=mesh, in_specs=in_specs, out_specs=out_specs, check_vma=False)
```

```python
import itertools

import jax
import jax.numpy as jnp
from jax import lax
from jax.experimental import pallas as pl
from jax.experimental.pallas import tpu as pltpu
from jax.sharding import Mesh
from jax.sharding import PartitionSpec as P

SPD = 8
AXES = ("y", "x", "z", "core")
ORDERS = (("z", "y", "x"), ("y", "x", "z"), ("x", "z", "y"))
EACH = (5, 6, 5)
PEERS = ((0, 0), (0, 1), (1, 0), (1, 1), (3, 0), (3, 1), (2, 0), (2, 1))
SHIFTS = (0, 1, 3, 2)
SIDE = 8
ROOM = 5
VMEM = 60 * 1024 * 1024
MB = 256
F32 = jnp.float32
BF16 = jnp.bfloat16
I32 = jnp.int32


def member(core_ref, at_ref, shift, flip):
    return ((at_ref[0] + shift) & 3) * 2 + (core_ref[0] + flip) % 2


def gather_flows(probes, rows, coef, sensor, count, core, flows, places):
    n, pn = probes.shape
    nblk, foot = rows.shape
    half = pn // 2
    parts = 8
    step = n // parts
    n_at = len(places)
    n_out = len(flows) * len(PEERS)

    def body(*refs):
        x_hbm, rows_hbm, coef_ref, sensor_ref, count_ref, core_ref = refs[:6]
        at_refs = refs[6 : 6 + n_at]
        outs = refs[6 + n_at : 6 + n_at + n_out]
        idx, idx_v, raw, tab, stage, coef_t, ids, sem, out_sem = refs[6 + n_at + n_out : 6 + n_at + n_out + 9]
        packs = refs[6 + n_at + n_out + 9 :]

        def fetch(i):
            return pltpu.make_async_copy(x_hbm.at[pl.ds(i * step, step), :], raw.at[pl.ds(i * step, step), :], sem.at[i])

        index = pltpu.make_async_copy(rows_hbm, idx_v, sem.at[parts])
        index.start()
        for i in range(parts):
            fetch(i).start()
        index.wait()
        idx_v[...] = idx_v[...] * 2
        doubled = pltpu.make_async_copy(idx_v, idx, sem.at[parts + 1])
        doubled.start()
        alive = lax.broadcasted_iota(I32, (nblk, foot), 0) < count_ref[0]
        coef_t[...] = jnp.where(alive, coef_ref[...].astype(F32), 0.0).T
        high = sensor_ref[...] // MB
        low = sensor_ref[...] - high * MB
        row = lax.broadcasted_iota(I32, (SIDE, nblk), 0)
        ids[...] = jnp.where(row == 1, high, jnp.where(row == 2, low, 0)).astype(F32)
        ch = 512
        for i in range(parts):
            fetch(i).wait()

            def conv(q, c):
                at = i * step + q * ch
                x = raw[pl.ds(at, ch), :].astype(F32)
                tab[pl.ds(at * 2, ch, stride=2), :] = x[:, :half]
                tab[pl.ds(at * 2 + 1, ch, stride=2), :] = x[:, half:]
                return c

            lax.fori_loop(0, step // ch, conv, 0)
        doubled.wait()
        copies = []
        for f, (first, each, axis) in enumerate(flows):
            for p, (shift, flip) in enumerate(PEERS):
                base = first + member(core_ref, at_refs[axis], shift, flip) * each
                pack = packs[f].at[p]

                def channel(i, c):
                    r = base + i
                    for j in range(nblk):
                        at = pl.multiple_of(idx.at[j][r], 2)
                        stage[pl.ds(2 * j, 2), :] = tab[pl.ds(at, 2), :]
                    pack[i, pl.ds(0, nblk), :] = stage[pl.ds(0, nblk, stride=2), :].astype(BF16)
                    pack[i, pl.ds(nblk, nblk), :] = stage[pl.ds(1, nblk, stride=2), :].astype(BF16)
                    tail = jnp.where(row == 0, coef_t[pl.ds(r, 1), :], ids[...])
                    pack[i, pl.ds(2 * nblk, SIDE), :] = tail.astype(BF16)
                    return c

                lax.fori_loop(0, each, channel, 0)
                at = f * len(PEERS) + p
                copies.append(pltpu.make_async_copy(pack, outs[at], out_sem.at[at]))
                copies[-1].start()
        for copy in copies:
            copy.wait()

    hbm = pl.BlockSpec(memory_space=pltpu.HBM)
    smem = pl.BlockSpec(memory_space=pltpu.SMEM)
    vmem = pl.BlockSpec(memory_space=pltpu.VMEM)
    shapes = [(each, 2 * nblk + SIDE, half) for _, each, _ in flows]
    return pl.pallas_call(
        body,
        in_specs=[hbm, hbm, vmem, vmem, smem, smem] + [smem] * n_at,
        out_specs=[hbm] * n_out,
        scratch_shapes=[
            pltpu.SMEM((nblk, foot), I32),
            pltpu.VMEM((nblk, foot), I32),
            pltpu.VMEM((n, pn), BF16),
            pltpu.VMEM((2 * n, half), F32),
            pltpu.VMEM((2 * nblk, half), F32),
            pltpu.VMEM((foot, nblk), F32),
            pltpu.VMEM((SIDE, nblk), F32),
            pltpu.SemaphoreType.DMA((parts + 2,)),
            pltpu.SemaphoreType.DMA((n_out,)),
        ]
        + [pltpu.VMEM((len(PEERS),) + s, BF16) for s in shapes],
        out_shape=[jax.ShapeDtypeStruct(s, BF16) for s in shapes for _ in PEERS],
        compiler_params=pltpu.CompilerParams(vmem_limit_bytes=VMEM),
        name="gather_flows",
    )(probes, rows, coef, sensor, count, core, *places)


def mix_tiles(tiles, at, n_sens):
    each, rows, half = tiles[0].shape
    ns = half
    n = len(tiles)

    def body(at_ref, *refs):
        data, outs = refs[:n], refs[n:]
        x = jnp.concatenate(
            [
                jnp.concatenate([d[0, :ns] for d in data], axis=0),
                jnp.concatenate([d[0, ns : 2 * ns] for d in data], axis=0),
            ],
            axis=1,
        )
        side = [d[0, 2 * ns :].astype(F32) for d in data]
        coef, high, low = (jnp.concatenate([s[i : i + 1] for s in side], axis=1) for i in range(3))
        coef = coef.astype(BF16)
        high = high.astype(I32)
        sub = lax.broadcasted_iota(I32, (MB, n * ns), 0).astype(F32).astype(BF16)
        for out, shift in zip(outs, SHIFTS):
            wanted = jnp.where(high == ((at_ref[0] + shift) & 3), low, -1.0).astype(BF16)
            mixer = jnp.where(sub == wanted, coef, jnp.zeros((), BF16))
            out[0] = jnp.dot(mixer, x, preferred_element_type=F32).astype(BF16)

    shape = (each, n_sens // 4, 2 * half)
    return pl.pallas_call(
        body,
        grid=(each,),
        in_specs=[pl.BlockSpec(memory_space=pltpu.SMEM)] + [pl.BlockSpec((1, rows, half), lambda i: (i, 0, 0))] * n,
        out_specs=[pl.BlockSpec((1,) + shape[1:], lambda i: (i, 0, 0))] * 4,
        out_shape=[jax.ShapeDtypeStruct(shape, BF16)] * 4,
        compiler_params=pltpu.CompilerParams(dimension_semantics=("arbitrary",), vmem_limit_bytes=24 * 1024 * 1024),
        name="mix_tiles",
    )(at, *tiles)


def add_quarters(quarters, at):
    each, n_sens, width = quarters[0].shape
    piece = n_sens // 4

    def body(at_ref, *refs):
        for out, shift in zip(refs[4:], SHIFTS):
            rows = pl.ds(pl.multiple_of(((at_ref[0] + shift) & 3) * piece, piece), piece)

            def channel(i, c):
                total = refs[0][i, rows, :].astype(F32)
                for r in refs[1:4]:
                    total += r[i, rows, :].astype(F32)
                out[i] = total.astype(BF16)
                return c

            lax.fori_loop(0, each, channel, 0)

    shape = (each, piece, width)
    vmem = pl.BlockSpec(memory_space=pltpu.VMEM)
    return pl.pallas_call(
        body,
        in_specs=[pl.BlockSpec(memory_space=pltpu.SMEM)] + [vmem] * 4,
        out_specs=[vmem] * 4,
        out_shape=[jax.ShapeDtypeStruct(shape, BF16)] * 4,
        compiler_params=pltpu.CompilerParams(vmem_limit_bytes=24 * 1024 * 1024),
        name="add_quarters",
    )(at, *quarters)


def square_sums(flows, n_dev):
    n = len(flows)
    piece = flows[0][0].shape[1]

    def body(*refs):
        out = refs[-1]
        lanes = []
        for f in range(n):
            four = refs[4 * f : 4 * f + 4]
            total = jnp.zeros((piece, 128), F32)
            for i in range(four[0].shape[0]):
                y = four[0][i].astype(F32) + four[1][i].astype(F32) + four[2][i].astype(F32) + four[3][i].astype(F32)
                y = y * y
                total += y[:, :128] + y[:, 128:]
            total = jnp.concatenate([total, jnp.zeros((128 - piece, 128), F32)], axis=0)
            lanes.append(jnp.sum(total.T, axis=0, keepdims=True))
        out[...] = jnp.broadcast_to(jnp.concatenate(lanes, axis=1)[None], out.shape)

    return pl.pallas_call(
        body,
        out_shape=jax.ShapeDtypeStruct((n_dev, 1, 128 * n), F32),
        compiler_params=pltpu.CompilerParams(vmem_limit_bytes=24 * 1024 * 1024),
        name="square_sums",
    )(*[x for four in flows for x in four])


def spread_squares(rows, coef, owner, me, tile_r, tile_c, sb=8):
    nblk, foot = rows.shape
    n_sens = owner.shape[1]

    steps = nblk // sb

    def body(me_ref, rows_ref, coef_ref, owner_ref, map_ref):
        g = pl.program_id(0)

        @pl.when(g == steps)
        def _():
            mine = owner_ref[...] == me_ref[0]
            flag = jnp.broadcast_to(jnp.where(mine, 1.0, 0.0), (8, n_sens)).astype(BF16)
            row = lax.broadcasted_iota(I32, (n_sens, n_sens), 0)
            col = lax.broadcasted_iota(I32, (n_sens, n_sens), 1)
            before = jnp.where(row < col, 1.0, 0.0).astype(BF16)
            rank = jnp.dot(flag, before, preferred_element_type=F32)[0:1, :]
            place = jnp.where(mine, rank, -1.0)
            for i in range(n_sens // 128):
                map_ref[0, i : i + 1, :128] = place[:, i * 128 : (i + 1) * 128]

        @pl.when(g < steps)
        def _():
            spread(rows_ref, coef_ref, map_ref)

    def spread(rows_ref, coef_ref, map_ref):
        sub_r = lax.broadcasted_iota(I32, (tile_r, foot), 0)
        sub_c = lax.broadcasted_iota(I32, (tile_c, foot), 0)
        point = rows_ref[...]
        high = point // tile_c
        low = point - high * tile_c
        c = coef_ref[...].astype(F32)
        sq = c * c
        sq_top = sq.astype(BF16).astype(F32)
        sq_rest = sq - sq_top
        for s in range(sb):
            at_r = sub_r == high[s : s + 1, :]
            left = jnp.concatenate(
                [jnp.where(at_r, sq_top[s : s + 1, :], 0.0), jnp.where(at_r, sq_rest[s : s + 1, :], 0.0)], axis=0
            ).astype(BF16)
            right = jnp.where(sub_c == low[s : s + 1, :], 1.0, 0.0).astype(BF16)
            both = lax.dot_general(left, right, (((1,), (1,)), ((), ())), preferred_element_type=F32)
            map_ref[s] = both[:tile_r] + both[tile_r:]

    return pl.pallas_call(
        body,
        grid=(steps + 1,),
        in_specs=[
            pl.BlockSpec(memory_space=pltpu.SMEM),
            pl.BlockSpec((sb, foot), lambda g: (jnp.minimum(g, steps - 1), 0)),
            pl.BlockSpec((sb, foot), lambda g: (jnp.minimum(g, steps - 1), 0)),
            pl.BlockSpec((1, n_sens), lambda g: (0, 0)),
        ],
        out_specs=pl.BlockSpec((sb, tile_r, tile_c), lambda g: (g, 0, 0)),
        out_shape=jax.ShapeDtypeStruct((ROOM * nblk, tile_r, tile_c), F32),
        compiler_params=pltpu.CompilerParams(
            dimension_semantics=("arbitrary",), vmem_limit_bytes=VMEM
        ),
        name="spread_squares",
    )(me, rows, coef, owner)


def finish(parts, weights, sensor, count, maps, scale, sb=32):
    n_sens = weights.size
    nblk = sensor.shape[0]
    tile_r, tile_c = maps.shape[1:]
    pieces = nblk // sb

    def body(count_ref, parts_ref, weights_ref, sensor_ref, maps_hbm, sens_ref, new_ref, dens_ref, slot_w, maps_ref, place_ref, sem):
        def fetch(i):
            return pltpu.make_async_copy(maps_hbm.at[pl.ds(i * sb, sb)], maps_ref.at[pl.ds(i * sb, sb)], sem.at[i])

        places = pltpu.make_async_copy(maps_hbm.at[nblk], place_ref, sem.at[pieces])
        places.start()
        for i in range(pieces):
            fetch(i).start()
        col = lax.broadcasted_iota(I32, (8, 128), 1)
        place = {"y": col // 32, "x": col // 8 % 4, "z": col // 2 % 4}
        want = lax.broadcasted_iota(I32, (8, 128), 0) * 2
        pair = [jnp.zeros((8, 128), F32), jnp.zeros((8, 128), F32)]
        for f, (_, b, c) in enumerate(ORDERS):
            group = place[b] * 4 + place[c]
            sums = parts_ref[:, 0, pl.ds(128 * f, 128)]
            for odd in range(2):
                pick = jnp.where(group == want + odd, 1.0, 0.0)
                pair[odd] += jnp.dot(pick, sums, precision=lax.Precision.HIGHEST, preferred_element_type=F32)
        h8 = (pair[0] + pltpu.roll(pair[1], 64, 1)) * scale
        gain = weights_ref[...] * jnp.sqrt(1.0 + h8)
        new8 = n_sens * gain / jnp.sum(gain)
        new_ref[...] = new8
        new = jnp.concatenate([new8[i : i + 1] for i in range(n_sens // 128)], axis=1)
        places.wait()
        mine = place_ref[: n_sens // 128, :128]
        lane = lax.broadcasted_iota(I32, (1, SPD), 1)
        own = jnp.zeros((1, SPD), F32)
        for k in range(SPD):
            own = jnp.where(lane == k, jnp.sum(jnp.where(mine == k, h8, 0.0)), own)
        sens_ref[...] = own
        which = lax.broadcasted_iota(I32, (nblk, n_sens), 1)
        w = jnp.sum(jnp.where(which == sensor_ref[...], new, 0.0), axis=1, keepdims=True)
        alive = lax.broadcasted_iota(I32, (nblk, 1), 0) < count_ref[0]
        slot_w[...] = jnp.broadcast_to(jnp.where(alive, w, 0.0), (nblk, tile_c))
        dens_ref[...] = jnp.zeros((tile_r, tile_c), F32)
        for i in range(pieces):
            fetch(i).wait()

            def add(q, c):
                total = dens_ref[...]
                for s in range(8):
                    at = i * sb + q * 8 + s
                    total += slot_w[pl.ds(at, 1), :] * maps_ref[at]
                dens_ref[...] = total
                return c

            lax.fori_loop(0, sb // 8, add, 0)

    vmem = pl.BlockSpec(memory_space=pltpu.VMEM)
    return pl.pallas_call(
        body,
        in_specs=[pl.BlockSpec(memory_space=pltpu.SMEM), vmem, vmem, vmem, pl.BlockSpec(memory_space=pltpu.HBM)],
        out_specs=[vmem, vmem, vmem],
        out_shape=[
            jax.ShapeDtypeStruct((1, SPD), F32),
            jax.ShapeDtypeStruct((n_sens // 128, 128), F32),
            jax.ShapeDtypeStruct((tile_r, tile_c), F32),
        ],
        scratch_shapes=[
            pltpu.VMEM((nblk, tile_c), F32),
            pltpu.VMEM((nblk, tile_r, tile_c), F32),
            pltpu.VMEM((tile_r, tile_c), F32),
            pltpu.SemaphoreType.DMA((pieces + 1,)),
        ],
        compiler_params=pltpu.CompilerParams(vmem_limit_bytes=48 * 1024 * 1024),
        name="finish",
    )(count, parts, weights, sensor, maps)


def exchange(x, axes):
    return lax.all_to_all(x, axes, split_axis=0, concat_axis=0, tiled=True)


def shift_to(x, axis, shift, flip):
    if not shift and not flip:
        return x
    sizes = [lax.axis_size(a) for a in AXES]
    where = AXES.index(axis)
    pairs = []
    for i, place in enumerate(itertools.product(*map(range, sizes))):
        to = list(place)
        to[where] = (to[where] + shift) % sizes[where]
        to[3] = (to[3] + flip) % 2
        j = 0
        for p, size in zip(to, sizes):
            j = j * size + p
        pairs.append((i, j))
    return lax.ppermute(x, AXES, pairs)


def local(probes, blk_rows, blk_sensor, blk_count, coef, owner, weights):
    n_dev = lax.axis_size(AXES)
    core = lax.axis_index("core").astype(I32).reshape(1)
    me = lax.axis_index(AXES).astype(I32).reshape(1)
    at = {axis: lax.axis_index(axis).astype(I32).reshape(1) for axis in AXES[:3]}
    tile_r, tile_c, probe_n = probes.shape
    nblk, foot = blk_rows.shape
    n_sens = owner.shape[0]
    flat = probes.reshape(tile_r * tile_c, probe_n)
    tile = (blk_rows, coef, blk_sensor.reshape(1, nblk), blk_count, core)
    firsts = [8 * sum(EACH[:f]) for f in range(3)]
    packs = [(first, each, f) for f, (first, each) in enumerate(zip(firsts, EACH))]
    sent = gather_flows(flat, *tile, packs, [at[a] for a, _, _ in ORDERS])
    maps = spread_squares(blk_rows, coef, owner.reshape(1, n_sens), me, tile_r, tile_c)
    tiles = [None] * 3
    flows = [None] * 3
    for f, (a, _, _) in enumerate(ORDERS):
        tiles[f] = [shift_to(x, a, *peer) for x, peer in zip(sent[8 * f : 8 * f + 8], PEERS)]
    for f, (_, b, c) in enumerate(ORDERS):
        quarters = mix_tiles(tiles[f], at[b], n_sens)
        quarters = [shift_to(x, b, s, 0) for x, s in zip(quarters, SHIFTS)]
        pieces = add_quarters(quarters, at[c])
        flows[f] = [shift_to(x, c, s, 0) for x, s in zip(pieces, SHIFTS)]
    (flows, maps) = lax.optimization_barrier((flows, maps))
    acc = square_sums(flows, n_dev)
    parts = exchange(acc, AXES)
    sens, new, density = finish(
        parts, weights.reshape(n_sens // 128, 128), blk_sensor.reshape(nblk, 1), blk_count, maps, 1.0 / (foot * probe_n)
    )
    return (sens.reshape(SPD), new.reshape(n_sens), density)


def solution(mesh):
    mesh = Mesh(mesh.devices.reshape(4, 4, 4, 2), AXES)
    gx, gy = AXES[:2], AXES[2:]
    in_specs = (P(gx, gy, None), P(AXES, None), P(AXES), P(AXES), P(AXES, None), P(), P())
    out_specs = (P(AXES), P(), P(gx, gy))
    return jax.shard_map(local, mesh=mesh, in_specs=in_specs, out_specs=out_specs, check_vma=False)
```

```python
import itertools

import jax
import jax.numpy as jnp
from jax import lax
from jax.experimental import pallas as pl
from jax.experimental.pallas import tpu as pltpu
from jax.sharding import Mesh
from jax.sharding import PartitionSpec as P

SPD = 8
AXES = ("y", "x", "z", "core")
ORDERS = (("z", "y", "x"), ("y", "x", "z"), ("x", "z", "y"))
EACH = (5, 6, 5)
PEERS = ((0, 0), (0, 1), (1, 0), (1, 1), (3, 0), (3, 1), (2, 0), (2, 1))
SHIFTS = (0, 1, 3, 2)
SIDE = 8
ROOM = 5
VMEM = 60 * 1024 * 1024
MB = 256
F32 = jnp.float32
BF16 = jnp.bfloat16
I32 = jnp.int32


def member(core_ref, at_ref, shift, flip):
    return ((at_ref[0] + shift) & 3) * 2 + (core_ref[0] + flip) % 2


def gather_flows(probes, rows, coef, sensor, count, core, flows, places):
    n, pn = probes.shape
    nblk, foot = rows.shape
    half = pn // 2
    parts = 8
    step = n // parts
    n_at = len(places)
    n_out = len(flows) * len(PEERS)

    def body(*refs):
        x_hbm, rows_hbm, coef_ref, sensor_ref, count_ref, core_ref = refs[:6]
        at_refs = refs[6 : 6 + n_at]
        outs = refs[6 + n_at : 6 + n_at + n_out]
        idx, idx_v, raw, tab, stage, coef_t, ids, sem, out_sem = refs[6 + n_at + n_out : 6 + n_at + n_out + 9]
        packs = refs[6 + n_at + n_out + 9 :]

        def fetch(i):
            return pltpu.make_async_copy(x_hbm.at[pl.ds(i * step, step), :], raw.at[pl.ds(i * step, step), :], sem.at[i])

        index = pltpu.make_async_copy(rows_hbm, idx_v, sem.at[parts])
        index.start()
        for i in range(parts):
            fetch(i).start()
        index.wait()
        idx_v[...] = idx_v[...] * 2
        doubled = pltpu.make_async_copy(idx_v, idx, sem.at[parts + 1])
        doubled.start()
        alive = lax.broadcasted_iota(I32, (nblk, foot), 0) < count_ref[0]
        coef_t[...] = jnp.where(alive, coef_ref[...].astype(F32), 0.0).T
        high = sensor_ref[...] // MB
        low = sensor_ref[...] - high * MB
        row = lax.broadcasted_iota(I32, (SIDE, nblk), 0)
        ids[...] = jnp.where(row == 1, high, jnp.where(row == 2, low, 0)).astype(F32)
        ch = 512
        for i in range(parts):
            fetch(i).wait()

            def conv(q, c):
                at = i * step + q * ch
                x = raw[pl.ds(at, ch), :].astype(F32)
                tab[pl.ds(at * 2, ch, stride=2), :] = x[:, :half]
                tab[pl.ds(at * 2 + 1, ch, stride=2), :] = x[:, half:]
                return c

            lax.fori_loop(0, step // ch, conv, 0)
        doubled.wait()
        copies = []
        for f, (first, each, axis) in enumerate(flows):
            for p, (shift, flip) in enumerate(PEERS):
                base = first + member(core_ref, at_refs[axis], shift, flip) * each
                pack = packs[f].at[p]

                def channel(i, c):
                    r = base + i
                    for j in range(nblk):
                        at = pl.multiple_of(idx.at[j][r], 2)
                        stage[pl.ds(2 * j, 2), :] = tab[pl.ds(at, 2), :]
                    pack[i, pl.ds(0, nblk), :] = stage[pl.ds(0, nblk, stride=2), :].astype(BF16)
                    pack[i, pl.ds(nblk, nblk), :] = stage[pl.ds(1, nblk, stride=2), :].astype(BF16)
                    tail = jnp.where(row == 0, coef_t[pl.ds(r, 1), :], ids[...])
                    pack[i, pl.ds(2 * nblk, SIDE), :] = tail.astype(BF16)
                    return c

                lax.fori_loop(0, each, channel, 0)
                at = f * len(PEERS) + p
                copies.append(pltpu.make_async_copy(pack, outs[at], out_sem.at[at]))
                copies[-1].start()
        for copy in copies:
            copy.wait()

    hbm = pl.BlockSpec(memory_space=pltpu.HBM)
    smem = pl.BlockSpec(memory_space=pltpu.SMEM)
    vmem = pl.BlockSpec(memory_space=pltpu.VMEM)
    shapes = [(each, 2 * nblk + SIDE, half) for _, each, _ in flows]
    return pl.pallas_call(
        body,
        in_specs=[hbm, hbm, vmem, vmem, smem, smem] + [smem] * n_at,
        out_specs=[hbm] * n_out,
        scratch_shapes=[
            pltpu.SMEM((nblk, foot), I32),
            pltpu.VMEM((nblk, foot), I32),
            pltpu.VMEM((n, pn), BF16),
            pltpu.VMEM((2 * n, half), F32),
            pltpu.VMEM((2 * nblk, half), F32),
            pltpu.VMEM((foot, nblk), F32),
            pltpu.VMEM((SIDE, nblk), F32),
            pltpu.SemaphoreType.DMA((parts + 2,)),
            pltpu.SemaphoreType.DMA((n_out,)),
        ]
        + [pltpu.VMEM((len(PEERS),) + s, BF16) for s in shapes],
        out_shape=[jax.ShapeDtypeStruct(s, BF16) for s in shapes for _ in PEERS],
        compiler_params=pltpu.CompilerParams(vmem_limit_bytes=VMEM),
        name="gather_flows",
    )(probes, rows, coef, sensor, count, core, *places)


def mix_tiles(tiles, at, n_sens):
    each, rows, half = tiles[0].shape
    ns = half
    n = len(tiles)

    def body(at_ref, *refs):
        data, outs = refs[:n], refs[n:]
        x = jnp.concatenate(
            [
                jnp.concatenate([d[0, :ns] for d in data], axis=0),
                jnp.concatenate([d[0, ns : 2 * ns] for d in data], axis=0),
            ],
            axis=1,
        )
        side = [d[0, 2 * ns :].astype(F32) for d in data]
        coef, high, low = (jnp.concatenate([s[i : i + 1] for s in side], axis=1) for i in range(3))
        coef = coef.astype(BF16)
        high = high.astype(I32)
        sub = lax.broadcasted_iota(I32, (MB, n * ns), 0).astype(F32).astype(BF16)
        for out, shift in zip(outs, SHIFTS):
            wanted = jnp.where(high == ((at_ref[0] + shift) & 3), low, -1.0).astype(BF16)
            mixer = jnp.where(sub == wanted, coef, jnp.zeros((), BF16))
            out[0] = jnp.dot(mixer, x, preferred_element_type=F32).astype(BF16)

    shape = (each, n_sens // 4, 2 * half)
    return pl.pallas_call(
        body,
        grid=(each,),
        in_specs=[pl.BlockSpec(memory_space=pltpu.SMEM)] + [pl.BlockSpec((1, rows, half), lambda i: (i, 0, 0))] * n,
        out_specs=[pl.BlockSpec((1,) + shape[1:], lambda i: (i, 0, 0))] * 4,
        out_shape=[jax.ShapeDtypeStruct(shape, BF16)] * 4,
        compiler_params=pltpu.CompilerParams(dimension_semantics=("arbitrary",), vmem_limit_bytes=24 * 1024 * 1024),
        name="mix_tiles",
    )(at, *tiles)


def add_quarters(quarters, at):
    each, n_sens, width = quarters[0].shape
    piece = n_sens // 4

    def body(at_ref, *refs):
        for out, shift in zip(refs[4:], SHIFTS):
            rows = pl.ds(pl.multiple_of(((at_ref[0] + shift) & 3) * piece, piece), piece)

            def channel(i, c):
                total = refs[0][i, rows, :].astype(F32)
                for r in refs[1:4]:
                    total += r[i, rows, :].astype(F32)
                out[i] = total.astype(BF16)
                return c

            lax.fori_loop(0, each, channel, 0)

    shape = (each, piece, width)
    vmem = pl.BlockSpec(memory_space=pltpu.VMEM)
    return pl.pallas_call(
        body,
        in_specs=[pl.BlockSpec(memory_space=pltpu.SMEM)] + [vmem] * 4,
        out_specs=[vmem] * 4,
        out_shape=[jax.ShapeDtypeStruct(shape, BF16)] * 4,
        compiler_params=pltpu.CompilerParams(vmem_limit_bytes=24 * 1024 * 1024),
        name="add_quarters",
    )(at, *quarters)


def square_sums(flows, n_dev):
    n = len(flows)
    piece = flows[0][0].shape[1]

    def body(*refs):
        out = refs[-1]
        lanes = []
        for f in range(n):
            four = refs[4 * f : 4 * f + 4]
            total = jnp.zeros((piece, 128), F32)
            for i in range(four[0].shape[0]):
                y = four[0][i].astype(F32) + four[1][i].astype(F32) + four[2][i].astype(F32) + four[3][i].astype(F32)
                y = y * y
                total += y[:, :128] + y[:, 128:]
            total = jnp.concatenate([total, jnp.zeros((128 - piece, 128), F32)], axis=0)
            lanes.append(jnp.sum(total.T, axis=0, keepdims=True))
        out[...] = jnp.broadcast_to(jnp.concatenate(lanes, axis=1)[None], out.shape)

    return pl.pallas_call(
        body,
        out_shape=jax.ShapeDtypeStruct((n_dev, 1, 128 * n), F32),
        compiler_params=pltpu.CompilerParams(vmem_limit_bytes=24 * 1024 * 1024),
        name="square_sums",
    )(*[x for four in flows for x in four])


def spread_squares(rows, coef, owner, me, tile_r, tile_c, sb=16):
    nblk, foot = rows.shape
    n_sens = owner.shape[1]

    steps = nblk // sb

    def body(me_ref, rows_ref, coef_ref, owner_ref, map_ref):
        g = pl.program_id(0)

        @pl.when(g == steps)
        def _():
            mine = owner_ref[...] == me_ref[0]
            flag = jnp.broadcast_to(jnp.where(mine, 1.0, 0.0), (8, n_sens)).astype(BF16)
            row = lax.broadcasted_iota(I32, (n_sens, n_sens), 0)
            col = lax.broadcasted_iota(I32, (n_sens, n_sens), 1)
            before = jnp.where(row < col, 1.0, 0.0).astype(BF16)
            rank = jnp.dot(flag, before, preferred_element_type=F32)[0:1, :]
            place = jnp.where(mine, rank, -1.0)
            for i in range(n_sens // 128):
                map_ref[0, i : i + 1, :128] = place[:, i * 128 : (i + 1) * 128]

        @pl.when(g < steps)
        def _():
            at = pl.ds(pl.multiple_of(g * sb, sb), sb)
            spread(rows_ref[at, :], coef_ref[at, :], map_ref)

    def spread(point, c, map_ref):
        sub_r = lax.broadcasted_iota(I32, (tile_r, foot), 0)
        sub_c = lax.broadcasted_iota(I32, (tile_c, foot), 0)
        high = point // tile_c
        low = point - high * tile_c
        c = c.astype(F32)
        sq = c * c
        sq_top = sq.astype(BF16).astype(F32)
        sq_rest = sq - sq_top
        for s in range(sb):
            at_r = sub_r == high[s : s + 1, :]
            left = jnp.concatenate(
                [jnp.where(at_r, sq_top[s : s + 1, :], 0.0), jnp.where(at_r, sq_rest[s : s + 1, :], 0.0)], axis=0
            ).astype(BF16)
            right = jnp.where(sub_c == low[s : s + 1, :], 1.0, 0.0).astype(BF16)
            both = lax.dot_general(left, right, (((1,), (1,)), ((), ())), preferred_element_type=F32)
            map_ref[s] = both[:tile_r] + both[tile_r:]

    return pl.pallas_call(
        body,
        grid=(steps + 1,),
        in_specs=[
            pl.BlockSpec(memory_space=pltpu.SMEM),
            pl.BlockSpec((nblk, foot), lambda g: (0, 0)),
            pl.BlockSpec((nblk, foot), lambda g: (0, 0)),
            pl.BlockSpec((1, n_sens), lambda g: (0, 0)),
        ],
        out_specs=pl.BlockSpec((sb, tile_r, tile_c), lambda g: (g, 0, 0)),
        out_shape=jax.ShapeDtypeStruct((ROOM * nblk, tile_r, tile_c), F32),
        compiler_params=pltpu.CompilerParams(
            dimension_semantics=("arbitrary",), vmem_limit_bytes=VMEM
        ),
        name="spread_squares",
    )(me, rows, coef, owner)


def finish(parts, weights, sensor, count, maps, scale, sb=32):
    n_sens = weights.size
    nblk = sensor.shape[0]
    tile_r, tile_c = maps.shape[1:]
    pieces = nblk // sb

    def body(count_ref, parts_ref, weights_ref, sensor_ref, maps_hbm, sens_ref, new_ref, dens_ref, slot_w, maps_ref, place_ref, sem):
        def fetch(i):
            return pltpu.make_async_copy(maps_hbm.at[pl.ds(i * sb, sb)], maps_ref.at[pl.ds(i * sb, sb)], sem.at[i])

        places = pltpu.make_async_copy(maps_hbm.at[nblk], place_ref, sem.at[pieces])
        places.start()
        for i in range(pieces):
            fetch(i).start()
        col = lax.broadcasted_iota(I32, (8, 128), 1)
        place = {"y": col // 32, "x": col // 8 % 4, "z": col // 2 % 4}
        want = lax.broadcasted_iota(I32, (8, 128), 0) * 2
        pair = [jnp.zeros((8, 128), F32), jnp.zeros((8, 128), F32)]
        for f, (_, b, c) in enumerate(ORDERS):
            group = place[b] * 4 + place[c]
            sums = parts_ref[:, 0, pl.ds(128 * f, 128)]
            for odd in range(2):
                pick = jnp.where(group == want + odd, 1.0, 0.0)
                pair[odd] += jnp.dot(pick, sums, precision=lax.Precision.HIGHEST, preferred_element_type=F32)
        h8 = (pair[0] + pltpu.roll(pair[1], 64, 1)) * scale
        gain = weights_ref[...] * jnp.sqrt(1.0 + h8)
        new8 = n_sens * gain / jnp.sum(gain)
        new_ref[...] = new8
        new = jnp.concatenate([new8[i : i + 1] for i in range(n_sens // 128)], axis=1)
        places.wait()
        mine = place_ref[: n_sens // 128, :128]
        lane = lax.broadcasted_iota(I32, (1, SPD), 1)
        own = jnp.zeros((1, SPD), F32)
        for k in range(SPD):
            own = jnp.where(lane == k, jnp.sum(jnp.where(mine == k, h8, 0.0)), own)
        sens_ref[...] = own
        which = lax.broadcasted_iota(I32, (nblk, n_sens), 1)
        w = jnp.sum(jnp.where(which == sensor_ref[...], new, 0.0), axis=1, keepdims=True)
        alive = lax.broadcasted_iota(I32, (nblk, 1), 0) < count_ref[0]
        slot_w[...] = jnp.broadcast_to(jnp.where(alive, w, 0.0), (nblk, tile_c))
        dens_ref[...] = jnp.zeros((tile_r, tile_c), F32)
        for i in range(pieces):
            fetch(i).wait()

            def add(q, c):
                total = dens_ref[...]
                for s in range(8):
                    at = i * sb + q * 8 + s
                    total += slot_w[pl.ds(at, 1), :] * maps_ref[at]
                dens_ref[...] = total
                return c

            lax.fori_loop(0, sb // 8, add, 0)

    vmem = pl.BlockSpec(memory_space=pltpu.VMEM)
    return pl.pallas_call(
        body,
        in_specs=[pl.BlockSpec(memory_space=pltpu.SMEM), vmem, vmem, vmem, pl.BlockSpec(memory_space=pltpu.HBM)],
        out_specs=[vmem, vmem, vmem],
        out_shape=[
            jax.ShapeDtypeStruct((1, SPD), F32),
            jax.ShapeDtypeStruct((n_sens // 128, 128), F32),
            jax.ShapeDtypeStruct((tile_r, tile_c), F32),
        ],
        scratch_shapes=[
            pltpu.VMEM((nblk, tile_c), F32),
            pltpu.VMEM((nblk, tile_r, tile_c), F32),
            pltpu.VMEM((tile_r, tile_c), F32),
            pltpu.SemaphoreType.DMA((pieces + 1,)),
        ],
        compiler_params=pltpu.CompilerParams(vmem_limit_bytes=48 * 1024 * 1024),
        name="finish",
    )(count, parts, weights, sensor, maps)


def exchange(x, axes):
    return lax.all_to_all(x, axes, split_axis=0, concat_axis=0, tiled=True)


def shift_to(x, axis, shift, flip):
    if not shift and not flip:
        return x
    sizes = [lax.axis_size(a) for a in AXES]
    where = AXES.index(axis)
    pairs = []
    for i, place in enumerate(itertools.product(*map(range, sizes))):
        to = list(place)
        to[where] = (to[where] + shift) % sizes[where]
        to[3] = (to[3] + flip) % 2
        j = 0
        for p, size in zip(to, sizes):
            j = j * size + p
        pairs.append((i, j))
    return lax.ppermute(x, AXES, pairs)


def local(probes, blk_rows, blk_sensor, blk_count, coef, owner, weights):
    n_dev = lax.axis_size(AXES)
    core = lax.axis_index("core").astype(I32).reshape(1)
    me = lax.axis_index(AXES).astype(I32).reshape(1)
    at = {axis: lax.axis_index(axis).astype(I32).reshape(1) for axis in AXES[:3]}
    tile_r, tile_c, probe_n = probes.shape
    nblk, foot = blk_rows.shape
    n_sens = owner.shape[0]
    flat = probes.reshape(tile_r * tile_c, probe_n)
    tile = (blk_rows, coef, blk_sensor.reshape(1, nblk), blk_count, core)
    firsts = [8 * sum(EACH[:f]) for f in range(3)]
    packs = [(first, each, f) for f, (first, each) in enumerate(zip(firsts, EACH))]
    sent = gather_flows(flat, *tile, packs, [at[a] for a, _, _ in ORDERS])
    maps = spread_squares(blk_rows, coef, owner.reshape(1, n_sens), me, tile_r, tile_c)
    tiles = [None] * 3
    flows = [None] * 3
    for f, (a, _, _) in enumerate(ORDERS):
        tiles[f] = [shift_to(x, a, *peer) for x, peer in zip(sent[8 * f : 8 * f + 8], PEERS)]
    for f, (_, b, c) in enumerate(ORDERS):
        quarters = mix_tiles(tiles[f], at[b], n_sens)
        quarters = [shift_to(x, b, s, 0) for x, s in zip(quarters, SHIFTS)]
        pieces = add_quarters(quarters, at[c])
        flows[f] = [shift_to(x, c, s, 0) for x, s in zip(pieces, SHIFTS)]
    (flows, maps) = lax.optimization_barrier((flows, maps))
    acc = square_sums(flows, n_dev)
    parts = exchange(acc, AXES)
    sens, new, density = finish(
        parts, weights.reshape(n_sens // 128, 128), blk_sensor.reshape(nblk, 1), blk_count, maps, 1.0 / (foot * probe_n)
    )
    return (sens.reshape(SPD), new.reshape(n_sens), density)


def solution(mesh):
    mesh = Mesh(mesh.devices.reshape(4, 4, 4, 2), AXES)
    gx, gy = AXES[:2], AXES[2:]
    in_specs = (P(gx, gy, None), P(AXES, None), P(AXES), P(AXES), P(AXES, None), P(), P())
    out_specs = (P(AXES), P(), P(gx, gy))
    return jax.shard_map(local, mesh=mesh, in_specs=in_specs, out_specs=out_specs, check_vma=False)
```
